256 devices in a mesh: dp: 64 (over y, z, core), member: 4 (over x).
Axes of the slice: x: 4, y: 4, z: 8, core: 2. Of those that a mesh axis runs over, the one named last changes fastest.
Arguments:
- features: bfloat16 [32768, 256], P('dp'), may hold values from -6 to 6
- next_features: bfloat16 [32768, 256], P('dp'), may hold values from -6 to 6
- rewards: bfloat16 [32768], P('dp'), may hold values from -6 to 6
- next_logp: bfloat16 [32768], P('dp'), may hold values from -8 to 8
- terminal: int32 [32768], P('dp'), may hold values 0 or 1
- source_ids: int32 [32768], P('dp'), may hold values from 0 to 7
- source_weight: bfloat16 [8], replicated, may hold values from 0.29882812 to 3
- subset: int32 [32768, 2], P('dp'), may hold values from 0 to 7, all different within a row
- destination: int32 [32768], P('dp'), may hold values from 0 to 63, as said below
- critic_w1: float32 [8, 2048, 256], P('member'), may hold values from -0.375 to 0.375
- critic_shift: float32 [8, 2048], P('member'), may hold values from -3 to 3
- critic_head: float32 [8, 2048], P('member'), may hold values from -0.125 to 0.125
- target_w1: bfloat16 [8, 2048, 256], P('member'), may hold values from -0.375 to 0.375
- target_mean: float32 [8, 2048], P('member'), may hold values from -2 to 2
- target_scale: float32 [8, 2048], P('member'), may hold values from 0.5 to 2
- target_shift: float32 [8, 2048], P('member'), may hold values from -3 to 3
- target_head: float32 [8, 2048], P('member'), may hold values from -0.125 to 0.125
Outputs:
- step_w1: float32 [8, 2048, 256], P('member')
- step_shift: float32 [8, 2048], P('member')
- step_head: float32 [8, 2048], P('member')
The draws below stay inside these ranges and needn't reach their ends.
Inputs may be any that keep to these rules, and one draw needn't show every extreme that they name: `destination`: in the 512 transitions that start on one index of dp, every shard is named at least 512 // 128 times and at most 16 times, and some shard exactly 16 times. `subset`: the entries of a row differ.
All inputs are finite; a program needn't handle non-finite values. No bound on the sum of `terminal` on one device may be relied on, other than what follows from the above.
Results may differ from the reference program's by a relative error of at most 0.003.
The reference program's roundings to bfloat16 on the way count: a program that leaves them out, or rounds other values in their place, can miss the bound.
Values may be sent and summed in bfloat16 or wider, within the bound.
A program may use at most 128 MiB of HBM per device.

```python
import math
import jax
import jax.numpy as jnp
from jax import lax

IN = 256
HIDDEN_SIZE = 2048
SOURCES = 8
TARGET_SUB = 2
TOK_DEV = 512
CRITICS = 8
TOKENS = 32768
CAP = 16
N_DP = 64


def draw_destination(key, part):
    base = TOK_DEV // (2 * N_DP)
    spare = CAP - base
    needed = TOK_DEV - N_DP * base

    def single(block):
        block_key = jax.random.fold_in(jax.random.fold_in(key, 7331), block)
        key_favor, key_score, key_order = jax.random.split(block_key, 3)
        steady = (jnp.arange(N_DP * base, dtype=jnp.int32) // base).astype(jnp.int32)
        favored = jax.random.randint(key_favor, (), 0, N_DP, dtype=jnp.int32)
        slot_ids = jnp.arange(N_DP * spare, dtype=jnp.int32)
        owners = (slot_ids // spare).astype(jnp.int32)
        scores = jax.random.randint(key_score, (N_DP * spare,), 0, 1048576, dtype=jnp.int32)
        scores = jnp.where(owners == favored, -1 - slot_ids, scores)
        order = jnp.argsort(scores, stable=True)
        chosen = owners[order[:needed]]
        rows = jnp.concatenate([steady, chosen]).astype(jnp.int32)
        shuffle = jax.random.permutation(key_order, TOK_DEV)
        return rows[shuffle]
    return jax.vmap(single)(jnp.arange(N_DP, dtype=jnp.int32)).reshape(TOKENS).astype(jnp.int32)


def with_ends(drawn, key, smallest, top_value):
    dims = drawn.shape
    spot = [jax.random.randint(jax.random.fold_in(key, axis), (), 0, dims[axis]) for axis in range(len(dims))]
    drawn = drawn.at[tuple(spot)].set(smallest)
    longest = dims.index(max(dims))
    spot[longest] = (spot[longest] + 1) % dims[longest]
    return drawn.at[tuple(spot)].set(top_value)


def levels(own_key, extent, cuts, smallest, high):
    loudness, own = 1.0, jax.random.fold_in(own_key, 6)
    for position, blocks in cuts:
        steps = jnp.exp(jax.random.uniform(jax.random.fold_in(own, position), (blocks,), jnp.float32, smallest / len(cuts), high / len(cuts)))
        loudness = loudness * jnp.repeat(steps, extent[position] // blocks).reshape([-1 if axis == position else 1 for axis in range(len(extent))])
    return loudness


def distinct(rng, rows, number_of, top, lift):
    sequence = jax.random.permutation(jax.random.fold_in(rng, 1), number_of)
    boost = sequence
    for power in range(3):
        boost = boost * boost // number_of
    boost = boost * lift // number_of
    lots = jax.random.randint(jax.random.fold_in(rng, 2), (rows, number_of), 0, 4096) + boost
    sure = jax.random.permutation(jax.random.fold_in(rng, 3), rows)[jnp.arange(number_of) % rows]
    lots = jnp.where(jnp.arange(rows)[:, None] == sure[None, :], 1 << 14, lots)
    score = lots * number_of + jnp.arange(number_of)
    return lax.top_k(score.astype(jnp.int32), top)[1].astype(jnp.int32)


def normal_values(stream_key, extent, deviation, reach, cuts=(), held_as=jnp.bfloat16):
    level = levels(stream_key, extent, cuts, -0.22, 0.18) if cuts else 1.0
    result = jax.random.normal(stream_key, extent, jnp.float32) * deviation * level
    return jnp.minimum(jnp.maximum(result, -reach), reach).astype(held_as)


def setup_inputs(seed: int = 0) -> dict:
    streams_of = jax.random.split(jax.random.key(seed), 18)
    features = normal_values(streams_of[0], (TOKENS, IN), 1.0, 6.0, ((0, 64),))
    next_features = normal_values(streams_of[1], (TOKENS, IN), 1.0, 6.0, ((0, 64),))
    rewards = normal_values(streams_of[2], (TOKENS,), 1.0, 6.0, ((0, 64),))
    next_logp = normal_values(streams_of[3], (TOKENS,), 2.0, 8.0, ((0, 64),))
    terminal = with_ends((jax.random.randint(streams_of[4], (TOKENS,), 0, 8) < 1).astype(jnp.int32), jax.random.fold_in(streams_of[4], 1), 0, 1)
    source_ids = with_ends(jax.random.randint(streams_of[5], (TOKENS,), 0, SOURCES), jax.random.fold_in(streams_of[5], 1), 0, SOURCES - 1).astype(jnp.int32)
    source_weight = jnp.clip(jnp.exp(jax.random.uniform(streams_of[6], (SOURCES,), jnp.float32, math.log(0.29882812), math.log(3.0))), 0.29882812, 3.0).astype(jnp.bfloat16)
    subset = distinct(streams_of[7], TOKENS, CRITICS, TARGET_SUB, 0)
    destination = draw_destination(jax.random.fold_in(streams_of[17], 71), 0)
    critic_w1 = normal_values(streams_of[9], (CRITICS, HIDDEN_SIZE, IN), IN ** -0.5, 0.375, ((0, 4),), jnp.float32)
    critic_shift = normal_values(streams_of[10], (CRITICS, HIDDEN_SIZE), 0.5, 3.0, ((0, 4),), jnp.float32)
    critic_head = normal_values(streams_of[11], (CRITICS, HIDDEN_SIZE), HIDDEN_SIZE ** -0.5, 0.125, ((0, 4),), jnp.float32)
    target_w1 = normal_values(streams_of[12], (CRITICS, HIDDEN_SIZE, IN), IN ** -0.5, 0.375, ((0, 4),))
    target_mean = normal_values(streams_of[13], (CRITICS, HIDDEN_SIZE), 0.3, 2.0, ((0, 4),), jnp.float32)
    target_scale = jnp.clip(jnp.exp(math.log(2.0) - 1.3862944 * jax.random.uniform(streams_of[14], (CRITICS, HIDDEN_SIZE), jnp.float32) ** levels(streams_of[14], (CRITICS, HIDDEN_SIZE), ((0, 4),), -0.2, 0.2)), 0.5, 2.0)
    target_shift = normal_values(streams_of[15], (CRITICS, HIDDEN_SIZE), 0.5, 3.0, ((0, 4),), jnp.float32)
    target_head = normal_values(streams_of[16], (CRITICS, HIDDEN_SIZE), HIDDEN_SIZE ** -0.5, 0.125, ((0, 4),), jnp.float32)
    return {"features": features, "next_features": next_features, "rewards": rewards, "next_logp": next_logp, "terminal": terminal, "source_ids": source_ids, "source_weight": source_weight, "subset": subset, "destination": destination, "critic_w1": critic_w1, "critic_shift": critic_shift, "critic_head": critic_head, "target_w1": target_w1, "target_mean": target_mean, "target_scale": target_scale, "target_shift": target_shift, "target_head": target_head}


GAMMA = 0.99
ALPHA = 0.2
EPS = 1e-05
HIGH = lax.Precision.HIGHEST

def target_values(next_features, target_w1, target_mean, target_scale, target_shift, target_head):

    def single(params):
        weights, center, spread, offset, output = params
        pre_act = jnp.dot(next_features, weights.T, preferred_element_type=jnp.float32)
        active = jnp.maximum((pre_act - center[None]) * spread[None] + offset[None], 0.0)
        return lax.optimization_barrier(jnp.sum(active * output[None], axis=1))
    values = lax.map(single, (target_w1, target_mean, target_scale, target_shift, target_head))
    return values.T

def reference(features, next_features, rewards, next_logp, terminal, source_ids, source_weight, subset, destination, critic_w1, critic_shift, critic_head, target_w1, target_mean, target_scale, target_shift, target_head):
    values = target_values(next_features, target_w1, target_mean, target_scale, target_shift, target_head)
    critic_iota = jnp.arange(CRITICS, dtype=jnp.int32)
    first = lax.optimization_barrier(jnp.sum(jnp.where(subset[:, 0:1] == critic_iota[None], values, 0.0), axis=1))
    second = lax.optimization_barrier(jnp.sum(jnp.where(subset[:, 1:2] == critic_iota[None], values, 0.0), axis=1))
    lowest = jnp.minimum(first, second)
    carry_on = 1.0 - terminal.astype(jnp.float32)
    target = rewards.astype(jnp.float32) + GAMMA * carry_on * (lowest - ALPHA * next_logp.astype(jnp.float32))
    target = lax.optimization_barrier(target.astype(jnp.bfloat16)).astype(jnp.float32)
    source_iota = jnp.arange(SOURCES, dtype=jnp.int32)
    weight = lax.optimization_barrier(jnp.sum(jnp.where(source_ids[:, None] == source_iota[None], source_weight.astype(jnp.float32)[None], 0.0), axis=1))
    shard_iota = jnp.arange(N_DP, dtype=jnp.int32)
    group = (destination[:, None] == shard_iota[None]).astype(jnp.float32)
    members = lax.optimization_barrier(jnp.sum(group, axis=0))[:, None]

    def spread_rows(table):
        return jnp.dot(group, table, precision=HIGH)

    def shard_mean(table):
        return jnp.dot(group.T, table, precision=HIGH) / members

    def critic(params):
        weights, offset, output = params
        pre_act = jnp.dot(features, weights.astype(jnp.bfloat16).T, preferred_element_type=jnp.float32)
        centred = pre_act - spread_rows(shard_mean(pre_act))
        inverse = spread_rows(1.0 / jnp.sqrt(shard_mean(centred * centred) + EPS))
        normed = centred * inverse
        before = normed + offset[None]
        active = jnp.maximum(before, 0.0)
        value = lax.optimization_barrier(jnp.sum(active * output[None], axis=1))
        slope = weight * (value - target)
        grad_head = jnp.dot(slope, active, precision=HIGH)
        grad_unit = jnp.where(before > 0, slope[:, None] * output[None], 0.0)
        grad_shift = lax.optimization_barrier(jnp.sum(grad_unit, axis=0))
        grad_pre = inverse * (grad_unit - spread_rows(shard_mean(grad_unit)) - normed * spread_rows(shard_mean(grad_unit * normed)))
        grad_w1 = jnp.dot(grad_pre.astype(jnp.bfloat16).T, features, preferred_element_type=jnp.float32)
        return (grad_w1, grad_shift, grad_head)
    grad_w1, grad_shift, grad_head = lax.map(critic, (critic_w1, critic_shift, critic_head))
    squares = jnp.sum(grad_w1 * grad_w1) + jnp.sum(grad_shift * grad_shift) + jnp.sum(grad_head * grad_head)
    norm = jnp.sqrt(squares)
    root = jnp.float32(math.sqrt(CRITICS * HIDDEN_SIZE * (IN + 2)))
    factor = root / jnp.maximum(norm, root)
    return (grad_w1 * factor, grad_shift * factor, grad_head * factor)
```

```python
import functools
import math

import jax
import jax.numpy as jnp
from jax import lax
from jax.experimental import pallas as pl
from jax.experimental.pallas import tpu as pltpu
from jax.sharding import PartitionSpec as P

GAMMA = 0.99
ALPHA = 0.2
EPS = 1e-05
NZ = 8
MESH = pl.DeviceIdType.MESH


def far_first(i, nz):
    half = nz // 2
    return half + ((i + 1) // 2) * (2 * ((i + 1) % 2) - 1)


def near_first(i, nz):
    return far_first(nz - 2 - i, nz)


def reduce_kernel(
    ny,
    nz,
    nx,
    h,
    hs,
    full,
    small,
    total,
    y_in,
    z_out,
    z_in,
    ys_in,
    zs_out,
    zs_in,
    x_out,
    x_in,
    y_sems,
    z_sems,
    gz_sems,
    gy_sems,
    pair_sems,
    ys_sems,
    zs_sems,
    gzs_sems,
    gys_sems,
    pair_small,
    x_sems,
):
    me = lax.axis_index("dp")
    mx = lax.axis_index("member")
    c = lax.rem(me, 2)
    z = lax.rem(me // 2, nz)
    y = me // (2 * nz)
    partner = me + 1 - 2 * c

    def dp_of(yy, zz):
        return (yy * nz + zz) * 2 + c

    def yo(o):
        return lax.rem(y + o, ny)

    def zo(o):
        return lax.rem(z + o, nz)

    def copy(src, dst, sems, index, dp):
        return pltpu.make_async_remote_copy(
            src_ref=src,
            dst_ref=dst,
            send_sem=sems.at[(0,) + index],
            recv_sem=sems.at[(1,) + index],
            device_id={"dp": dp},
            device_id_type=MESH,
        )

    barrier = pltpu.get_barrier_semaphore()
    for o in range(1, ny):
        pl.semaphore_signal(barrier, inc=1, device_id={"dp": dp_of(yo(o), z)}, device_id_type=MESH)
    for o in range(1, nz):
        pl.semaphore_signal(barrier, inc=1, device_id={"dp": dp_of(y, zo(o))}, device_id_type=MESH)
    pl.semaphore_signal(barrier, inc=1, device_id={"dp": partner}, device_id_type=MESH)
    for o in range(1, nx):
        pl.semaphore_signal(
            barrier, inc=1, device_id={"member": lax.rem(mx + o, nx)}, device_id_type=MESH
        )
    pl.semaphore_wait(barrier, ny + nz + nx - 2)

    def y_small(o):
        return copy(hs.at[yo(o)], ys_in.at[o - 1], ys_sems, (o - 1,), dp_of(yo(o), z))

    def y_block(o, oz):
        return copy(
            h.at[yo(o), zo(oz)],
            y_in.at[o - 1, oz],
            y_sems,
            (o - 1, oz),
            dp_of(yo(o), z),
        )

    for o in range(1, ny):
        y_small(o).start()

    def send_y(i, _):
        oz = lax.rem(far_first(i, nz), nz)
        for o in range(1, ny):
            y_block(o, oz).start()
        return 0

    lax.fori_loop(0, nz - 1, send_y, 0)
    for o in range(1, ny):
        y_block(o, 0).start()

    def z_small(o):
        return copy(zs_out.at[zo(o)], zs_in.at[o - 1], zs_sems, (o - 1,), dp_of(y, zo(o)))

    def z_block(o):
        return copy(z_out.at[o], z_in.at[o], z_sems, (o,), dp_of(y, zo(o)))

    for o in range(1, ny):
        y_small(o).wait_recv()
    zs_out[...] = hs[y] + sum(ys_in[o - 1] for o in range(1, ny))
    for o in range(1, nz):
        z_small(o).start()

    def y_sum(oz):
        for o in range(1, ny):
            y_block(o, oz).wait_recv()
        value = h[y, zo(oz)].astype(jnp.float32)
        for o in range(1, ny):
            value = value + y_in[o - 1, oz].astype(jnp.float32)
        z_out[oz] = value

    def send_z(i, _):
        oz = lax.rem(far_first(i, nz), nz)
        y_sum(oz)
        z_block(oz).start()
        return 0

    lax.fori_loop(0, nz - 1, send_z, 0)
    y_sum(0)

    for o in range(1, nz):
        z_small(o).wait_recv()
    mine_small = zs_out[z] + sum(zs_in[o - 1] for o in range(1, nz))

    def add_z(i, value):
        oz = near_first(i, nz)
        z_block(oz).wait_recv()
        return value + z_in[oz]

    z_out[0] = lax.fori_loop(0, nz - 1, add_z, z_out[0])
    mine = z_out[0]
    squares = jnp.sum(mine * mine) + jnp.sum(mine_small * mine_small)
    small[c, y, z, :, 0:128] = mine_small
    small[c, y, z, :, 128:256] = jnp.full((1, 128), squares, jnp.float32)
    full[c, y, z] = mine.astype(jnp.bfloat16)

    def gz_small(o):
        ref = small.at[c, y, z]
        return copy(ref, ref, gzs_sems, (o - 1,), dp_of(y, zo(o)))

    def gz_block(o):
        ref = full.at[c, y, z]
        return copy(ref, ref, gz_sems, (o,), dp_of(y, zo(o)))

    def gy_small(o):
        ref = small.at[c, y]
        return copy(ref, ref, gys_sems, (o - 1,), dp_of(yo(o), z))

    def gy_block(o, oz):
        ref = full.at[c, y, zo(nz - oz)]
        return copy(ref, ref, gy_sems, (o - 1, oz), dp_of(yo(o), z))

    def pair_block(oy, oz):
        ref = full.at[c, yo(ny - oy), zo(nz - oz)]
        return copy(ref, ref, pair_sems, (oy, oz), partner)

    for o in range(1, nz):
        gz_small(o).start()

    def send_gz(i, _):
        gz_block(far_first(i, nz)).start()
        return 0

    lax.fori_loop(0, nz - 1, send_gz, 0)
    for o in range(1, ny):
        gy_block(o, 0).start()
    pair_block(0, 0).start()

    for o in range(1, nz):
        gz_small(o).wait_recv()
    for o in range(1, ny):
        gy_small(o).start()

    def relay_z(i, _):
        oz = near_first(i, nz)
        gz_block(oz).wait_recv()
        for o in range(1, ny):
            gy_block(o, oz).start()
        pair_block(0, oz).start()
        return 0

    lax.fori_loop(0, nz - 1, relay_z, 0)

    for o in range(1, ny):
        gy_small(o).wait_recv()
    pair_s = copy(small.at[c], small.at[c], pair_small, (0,), partner)
    pair_s.start()

    def relay_y(i, _):
        oz = lax.rem(near_first(lax.rem(i + nz - 2, nz - 1), nz) * lax.min(i, 1), nz)
        for o in range(1, ny):
            gy_block(o, oz).wait_recv()
            pair_block(o, oz).start()
        return 0

    half = nz // 2
    lax.fori_loop(0, half, relay_y, 0)
    pair_s.wait_recv()
    x_out[...] = jnp.sum(small[:, :, :, :, 128:256], axis=(0, 1, 2))

    def x_copy(o):
        return pltpu.make_async_remote_copy(
            src_ref=x_out,
            dst_ref=x_in.at[o - 1],
            send_sem=x_sems.at[0, o - 1],
            recv_sem=x_sems.at[1, o - 1],
            device_id={"member": lax.rem(mx + o, nx)},
            device_id_type=MESH,
        )

    for o in range(1, nx):
        x_copy(o).start()
    lax.fori_loop(half, nz, relay_y, 0)
    for o in range(1, nx):
        x_copy(o).wait_recv()
    total[...] = x_out[...] + sum(x_in[o - 1] for o in range(1, nx))

    def wait_pair(i, _):
        for o in range(ny):
            pair_block(o, i).wait_recv()
        return 0

    lax.fori_loop(0, nz, wait_pair, 0)

    def drain_y(i, _):
        for o in range(1, ny):
            y_block(o, i).wait_send()
            gy_block(o, i).wait_send()
        for o in range(ny):
            pair_block(o, i).wait_send()
        return 0

    lax.fori_loop(0, nz, drain_y, 0)

    def drain_z(i, _):
        z_block(i).wait_send()
        gz_block(i).wait_send()
        return 0

    lax.fori_loop(1, nz, drain_z, 0)
    for o in range(1, ny):
        y_small(o).wait_send()
        gy_small(o).wait_send()
    for o in range(1, nz):
        z_small(o).wait_send()
        gz_small(o).wait_send()
    for o in range(1, nx):
        x_copy(o).wait_send()
    pair_s.wait_send()


def reduce_all(h, hs, ny, nz, nx):
    rows, width = h.shape[2:]
    f32, bf16 = jnp.float32, jnp.bfloat16
    vmem = pl.BlockSpec(memory_space=pltpu.VMEM)
    dma = pltpu.SemaphoreType.DMA
    return pl.pallas_call(
        functools.partial(reduce_kernel, ny, nz, nx),
        out_shape=(
            jax.ShapeDtypeStruct((2, ny, nz, rows, width), bf16),
            jax.ShapeDtypeStruct((2, ny, nz, 1, 256), f32),
            jax.ShapeDtypeStruct((1, 128), f32),
        ),
        in_specs=[vmem] * 2,
        out_specs=[vmem] * 3,
        scratch_shapes=[
            pltpu.VMEM((ny - 1, nz, rows, width), bf16),
            pltpu.VMEM((nz, rows, width), f32),
            pltpu.VMEM((nz, rows, width), f32),
            pltpu.VMEM((ny - 1, nz, 1, 128), f32),
            pltpu.VMEM((nz, 1, 128), f32),
            pltpu.VMEM((nz - 1, 1, 128), f32),
            pltpu.VMEM((1, 128), f32),
            pltpu.VMEM((nx - 1, 1, 128), f32),
            dma((2, ny - 1, nz)),
            dma((2, nz)),
            dma((2, nz)),
            dma((2, ny - 1, nz)),
            dma((2, ny, nz)),
            dma((2, ny - 1)),
            dma((2, nz - 1)),
            dma((2, nz - 1)),
            dma((2, ny - 1)),
            dma((2, 1)),
            dma((2, nx - 1)),
        ],
        compiler_params=pltpu.CompilerParams(collective_id=0, has_side_effects=True),
        cost_estimate=pl.CostEstimate(flops=10**7, bytes_accessed=4 * 10**6, transcendentals=0),
        name="gradient_sum",
    )(h, hs)


def per_device(
    features,
    next_features,
    rewards,
    next_logp,
    terminal,
    source_ids,
    source_weight,
    subset,
    destination,
    critic_w1,
    critic_shift,
    critic_head,
    target_w1,
    target_mean,
    target_scale,
    target_shift,
    target_head,
):
    shards = lax.axis_size("dp")
    members = lax.axis_size("member")
    local_rows = features.shape[0]
    width = features.shape[1]
    local_critics = critic_w1.shape[0]
    total_critics = local_critics * members
    capacity = 2 * local_rows // shards
    slot_total = shards * capacity
    shard_iota = jnp.arange(shards, dtype=jnp.int32)
    picked = (destination[:, None] == shard_iota[None]).astype(jnp.int32)
    earlier = jnp.cumsum(picked, axis=0) - picked
    rank = jnp.sum(earlier * picked, axis=1)
    position = destination * capacity + rank

    def place(values):
        empty = jnp.zeros((slot_total,) + values.shape[1:], values.dtype)
        return empty.at[position].set(values).reshape((shards, capacity) + values.shape[1:])

    source_iota = jnp.arange(source_weight.shape[0], dtype=jnp.int32)
    weight_rows = jnp.sum(
        jnp.where(
            source_ids[:, None] == source_iota[None], source_weight.astype(jnp.float32)[None], 0.0
        ),
        axis=1,
    ).astype(jnp.bfloat16)
    carry_rows = (1 - terminal).astype(jnp.bfloat16)
    pre_act = jnp.einsum(
        "si,cfi->csf", next_features, target_w1, preferred_element_type=jnp.float32
    )
    active = jnp.maximum(
        (pre_act - target_mean[:, None]) * target_scale[:, None] + target_shift[:, None], 0.0
    )
    mine = jnp.sum(active * target_head[:, None], axis=2).T
    everyone = lax.all_gather(mine, "member", axis=1, tiled=True)
    critic_iota = jnp.arange(total_critics, dtype=jnp.int32)
    first = jnp.sum(jnp.where(subset[:, 0][:, None] == critic_iota[None], everyone, 0.0), axis=1)
    second = jnp.sum(jnp.where(subset[:, 1][:, None] == critic_iota[None], everyone, 0.0), axis=1)
    lowest = jnp.minimum(first, second)
    value = rewards.astype(jnp.float32) + GAMMA * carry_rows.astype(jnp.float32) * (
        lowest - ALPHA * next_logp.astype(jnp.float32)
    )
    value = value.astype(jnp.bfloat16)
    received, weight_slots, target_slots = (
        lax.all_to_all(place(features), "dp", split_axis=0, concat_axis=0, tiled=True),
        lax.all_to_all(place(weight_rows), "dp", split_axis=0, concat_axis=0, tiled=True),
        lax.all_to_all(place(value), "dp", split_axis=0, concat_axis=0, tiled=True),
    )
    rows_in = received.reshape(slot_total, width)
    weight = weight_slots.reshape(slot_total).astype(jnp.float32)
    target = target_slots.reshape(slot_total).astype(jnp.float32)
    live = (weight > 0).astype(jnp.float32)
    live_count = jnp.sum(live)
    live_col = live[:, None]

    def critic(params):
        weights, offset, output = params
        pre_act = jnp.dot(
            rows_in, weights.astype(jnp.bfloat16).T, preferred_element_type=jnp.float32
        )
        centred = pre_act - jnp.sum(pre_act * live_col, axis=0, keepdims=True) / live_count
        inverse = 1.0 / jnp.sqrt(
            jnp.sum(centred * centred * live_col, axis=0, keepdims=True) / live_count + EPS
        )
        normed = centred * inverse
        before = normed + offset[None]
        active = jnp.maximum(before, 0.0)
        value_now = jnp.sum(active * output[None], axis=1)
        slope = weight * (value_now - target)
        grad_head = jnp.dot(slope, active)
        grad_unit = jnp.where(before > 0, slope[:, None] * output[None], 0.0)
        grad_shift = jnp.sum(grad_unit, axis=0)
        unit_mean = jnp.sum(grad_unit * live_col, axis=0, keepdims=True) / live_count
        cross_mean = jnp.sum(grad_unit * normed * live_col, axis=0, keepdims=True) / live_count
        grad_pre = (inverse * (grad_unit - unit_mean - normed * cross_mean) * live_col).astype(
            jnp.bfloat16
        )
        grad_w1 = jnp.dot(grad_pre.T, rows_in, preferred_element_type=jnp.float32)
        return (grad_w1, grad_shift, grad_head)

    grad_w1, grad_shift, grad_head = lax.map(critic, (critic_w1, critic_shift, critic_head))
    hidden = critic_w1.shape[1]
    root = jnp.float32(math.sqrt(total_critics * hidden * (width + 2)))
    nz = NZ
    ny = shards // (2 * nz)
    blocks = ny * nz
    core = lax.rem(lax.axis_index("dp"), 2)
    pairs = [(i, i ^ 1) for i in range(shards)]

    def half_sum(a):
        keep = lax.dynamic_index_in_dim(a, core, 0, keepdims=False)
        give = lax.dynamic_index_in_dim(a, 1 - core, 0, keepdims=False)
        return keep + lax.ppermute(give, "dp", pairs)

    h = half_sum(grad_w1).astype(jnp.bfloat16).reshape(ny, nz, hidden // blocks, width)
    vectors = jnp.concatenate(
        [
            grad_shift.reshape(2, blocks, hidden // blocks),
            grad_head.reshape(2, blocks, hidden // blocks),
        ],
        axis=2,
    )
    hs = half_sum(vectors).reshape(ny, nz, 1, 2 * hidden // blocks)
    full, small, squares = reduce_all(h, hs, ny, nz, members)
    norm = jnp.sqrt(squares[0, 0])
    factor = root / jnp.maximum(norm, root)
    step_w1 = full.reshape(2, hidden, width).astype(jnp.float32) * factor
    per = hidden // blocks
    step_shift = small[..., 0, 0:per].reshape(2, hidden) * factor
    step_head = small[..., 0, per : 2 * per].reshape(2, hidden) * factor
    return (step_w1, step_shift, step_head)


def solution(mesh):
    in_specs = (
        P("dp", None),
        P("dp", None),
        P("dp"),
        P("dp"),
        P("dp"),
        P("dp"),
        P(),
        P("dp", None),
        P("dp"),
        P("member", None, None),
        P("member", None),
        P("member", None),
        P("member", None, None),
        P("member", None),
        P("member", None),
        P("member", None),
        P("member", None),
    )
    out_specs = (P("member", None, None), P("member", None), P("member", None))
    return jax.shard_map(
        per_device, mesh=mesh, in_specs=in_specs, out_specs=out_specs, check_vma=False
    )
```

```python
import functools
import math

import jax
import jax.numpy as jnp
from jax import lax
from jax.experimental import pallas as pl
from jax.experimental.pallas import tpu as pltpu
from jax.sharding import PartitionSpec as P

GAMMA = 0.99
ALPHA = 0.2
EPS = 1e-05
NZ = 8
MESH = pl.DeviceIdType.MESH


def far_first(i, nz):
    half = nz // 2
    return half + ((i + 1) // 2) * (2 * ((i + 1) % 2) - 1)


def near_first(i, nz):
    return far_first(nz - 2 - i, nz)


def reduce_kernel(
    ny,
    nz,
    nx,
    h,
    hs,
    full,
    small,
    total,
    y_in,
    z_out,
    z_in,
    ys_in,
    zs_out,
    zs_in,
    x_out,
    x_in,
    y_sems,
    z_sems,
    gz_sems,
    gy_sems,
    pair_sems,
    ys_sems,
    zs_sems,
    gzs_sems,
    gys_sems,
    pair_small,
    x_sems,
):
    me = lax.axis_index("dp")
    mx = lax.axis_index("member")
    c = lax.rem(me, 2)
    z = lax.rem(me // 2, nz)
    y = me // (2 * nz)
    partner = me + 1 - 2 * c

    def dp_of(yy, zz):
        return (yy * nz + zz) * 2 + c

    def yo(o):
        return lax.rem(y + o, ny)

    def zo(o):
        return lax.rem(z + o, nz)

    def copy(src, dst, sems, index, dp):
        return pltpu.make_async_remote_copy(
            src_ref=src,
            dst_ref=dst,
            send_sem=sems.at[(0,) + index],
            recv_sem=sems.at[(1,) + index],
            device_id={"dp": dp},
            device_id_type=MESH,
        )

    def block_of(yy, zz):
        return full.at[c, yy * (nz // 2) + zz // 2, :, pl.ds(pl.multiple_of(lax.rem(zz, 2) * 128, 128), 128)]

    barrier = pltpu.get_barrier_semaphore()
    for o in range(1, ny):
        pl.semaphore_signal(barrier, inc=1, device_id={"dp": dp_of(yo(o), z)}, device_id_type=MESH)
    for o in range(1, nz):
        pl.semaphore_signal(barrier, inc=1, device_id={"dp": dp_of(y, zo(o))}, device_id_type=MESH)
    pl.semaphore_signal(barrier, inc=1, device_id={"dp": partner}, device_id_type=MESH)
    for o in range(1, nx):
        pl.semaphore_signal(
            barrier, inc=1, device_id={"member": lax.rem(mx + o, nx)}, device_id_type=MESH
        )
    pl.semaphore_wait(barrier, ny + nz + nx - 2)

    def y_small(o):
        return copy(hs.at[yo(o)], ys_in.at[o - 1], ys_sems, (o - 1,), dp_of(yo(o), z))

    def y_block(o, oz):
        return copy(
            h.at[yo(o), zo(oz)],
            y_in.at[o - 1, oz],
            y_sems,
            (o - 1, oz),
            dp_of(yo(o), z),
        )

    for o in range(1, ny):
        y_small(o).start()

    def send_y(i, _):
        oz = lax.rem(far_first(i, nz), nz)
        for o in range(1, ny):
            y_block(o, oz).start()
        return 0

    lax.fori_loop(0, nz - 1, send_y, 0)
    for o in range(1, ny):
        y_block(o, 0).start()

    def z_small(o):
        return copy(zs_out.at[zo(o)], zs_in.at[o - 1], zs_sems, (o - 1,), dp_of(y, zo(o)))

    def z_block(o):
        return copy(z_out.at[o], z_in.at[o], z_sems, (o,), dp_of(y, zo(o)))

    for o in range(1, ny):
        y_small(o).wait_recv()
    zs_out[...] = hs[y] + sum(ys_in[o - 1] for o in range(1, ny))
    for o in range(1, nz):
        z_small(o).start()

    def y_sum(oz):
        for o in range(1, ny):
            y_block(o, oz).wait_recv()
        value = h[y, zo(oz)].astype(jnp.float32)
        for o in range(1, ny):
            value = value + y_in[o - 1, oz].astype(jnp.float32)
        z_out[oz] = value

    def send_z(i, _):
        oz = lax.rem(far_first(i, nz), nz)
        y_sum(oz)
        z_block(oz).start()
        return 0

    lax.fori_loop(0, nz - 1, send_z, 0)
    y_sum(0)

    for o in range(1, nz):
        z_small(o).wait_recv()
    mine_small = zs_out[z] + sum(zs_in[o - 1] for o in range(1, nz))

    def add_z(i, value):
        oz = near_first(i, nz)
        z_block(oz).wait_recv()
        return value + z_in[oz]

    z_out[0] = lax.fori_loop(0, nz - 1, add_z, z_out[0])
    mine = z_out[0]
    squares = jnp.sum(mine * mine) + jnp.sum(mine_small * mine_small)
    small[c, y, z, :, 0:128] = mine_small
    small[c, y, z, :, 128:256] = jnp.full((1, 128), squares, jnp.float32)
    mine_ref = block_of(y, z)
    mine_ref[...] = mine.T.astype(jnp.bfloat16)

    def gz_small(o):
        ref = small.at[c, y, z]
        return copy(ref, ref, gzs_sems, (o - 1,), dp_of(y, zo(o)))

    def gz_block(o):
        ref = block_of(y, z)
        return copy(ref, ref, gz_sems, (o,), dp_of(y, zo(o)))

    def gy_small(o):
        ref = small.at[c, y]
        return copy(ref, ref, gys_sems, (o - 1,), dp_of(yo(o), z))

    def gy_block(o, oz):
        ref = block_of(y, zo(nz - oz))
        return copy(ref, ref, gy_sems, (o - 1, oz), dp_of(yo(o), z))

    def pair_block(oy, oz):
        ref = block_of(yo(ny - oy), zo(nz - oz))
        return copy(ref, ref, pair_sems, (oy, oz), partner)

    for o in range(1, nz):
        gz_small(o).start()

    def send_gz(i, _):
        gz_block(far_first(i, nz)).start()
        return 0

    lax.fori_loop(0, nz - 1, send_gz, 0)
    for o in range(1, ny):
        gy_block(o, 0).start()
    pair_block(0, 0).start()

    for o in range(1, nz):
        gz_small(o).wait_recv()
    for o in range(1, ny):
        gy_small(o).start()

    def relay_z(i, _):
        oz = near_first(i, nz)
        gz_block(oz).wait_recv()
        for o in range(1, ny):
            gy_block(o, oz).start()
        pair_block(0, oz).start()
        return 0

    lax.fori_loop(0, nz - 1, relay_z, 0)

    for o in range(1, ny):
        gy_small(o).wait_recv()
    pair_s = copy(small.at[c], small.at[c], pair_small, (0,), partner)
    pair_s.start()

    def relay_y(i, _):
        oz = lax.rem(near_first(lax.rem(i + nz - 2, nz - 1), nz) * lax.min(i, 1), nz)
        for o in range(1, ny):
            gy_block(o, oz).wait_recv()
            pair_block(o, oz).start()
        return 0

    half = nz // 2
    lax.fori_loop(0, half, relay_y, 0)
    pair_s.wait_recv()
    x_out[...] = jnp.sum(small[:, :, :, :, 128:256], axis=(0, 1, 2))

    def x_copy(o):
        return pltpu.make_async_remote_copy(
            src_ref=x_out,
            dst_ref=x_in.at[o - 1],
            send_sem=x_sems.at[0, o - 1],
            recv_sem=x_sems.at[1, o - 1],
            device_id={"member": lax.rem(mx + o, nx)},
            device_id_type=MESH,
        )

    for o in range(1, nx):
        x_copy(o).start()
    lax.fori_loop(half, nz, relay_y, 0)
    for o in range(1, nx):
        x_copy(o).wait_recv()
    total[...] = x_out[...] + sum(x_in[o - 1] for o in range(1, nx))

    def wait_pair(i, _):
        for o in range(ny):
            pair_block(o, i).wait_recv()
        return 0

    lax.fori_loop(0, nz, wait_pair, 0)

    def drain_y(i, _):
        for o in range(1, ny):
            y_block(o, i).wait_send()
            gy_block(o, i).wait_send()
        for o in range(ny):
            pair_block(o, i).wait_send()
        return 0

    lax.fori_loop(0, nz, drain_y, 0)

    def drain_z(i, _):
        z_block(i).wait_send()
        gz_block(i).wait_send()
        return 0

    lax.fori_loop(1, nz, drain_z, 0)
    for o in range(1, ny):
        y_small(o).wait_send()
        gy_small(o).wait_send()
    for o in range(1, nz):
        z_small(o).wait_send()
        gz_small(o).wait_send()
    for o in range(1, nx):
        x_copy(o).wait_send()
    pair_s.wait_send()


def reduce_all(h, hs, ny, nz, nx):
    rows, width = h.shape[2:]
    f32, bf16 = jnp.float32, jnp.bfloat16
    vmem = pl.BlockSpec(memory_space=pltpu.VMEM)
    dma = pltpu.SemaphoreType.DMA
    return pl.pallas_call(
        functools.partial(reduce_kernel, ny, nz, nx),
        out_shape=(
            jax.ShapeDtypeStruct((2, ny * nz // 2, 128, 256), bf16),
            jax.ShapeDtypeStruct((2, ny, nz, 1, 256), f32),
            jax.ShapeDtypeStruct((1, 128), f32),
        ),
        in_specs=[vmem] * 2,
        out_specs=[vmem] * 3,
        scratch_shapes=[
            pltpu.VMEM((ny - 1, nz, rows, width), bf16),
            pltpu.VMEM((nz, rows, width), f32),
            pltpu.VMEM((nz, rows, width), f32),
            pltpu.VMEM((ny - 1, nz, 1, 128), f32),
            pltpu.VMEM((nz, 1, 128), f32),
            pltpu.VMEM((nz - 1, 1, 128), f32),
            pltpu.VMEM((1, 128), f32),
            pltpu.VMEM((nx - 1, 1, 128), f32),
            dma((2, ny - 1, nz)),
            dma((2, nz)),
            dma((2, nz)),
            dma((2, ny - 1, nz)),
            dma((2, ny, nz)),
            dma((2, ny - 1)),
            dma((2, nz - 1)),
            dma((2, nz - 1)),
            dma((2, ny - 1)),
            dma((2, 1)),
            dma((2, nx - 1)),
        ],
        compiler_params=pltpu.CompilerParams(collective_id=0, has_side_effects=True),
        cost_estimate=pl.CostEstimate(flops=10**7, bytes_accessed=4 * 10**6, transcendentals=0),
        name="gradient_sum",
    )(h, hs)


def dot_nt(a, b):
    return lax.dot_general(a, b, (((1,), (1,)), ((), ())), preferred_element_type=jnp.float32)


def dot_nn(a, b):
    return lax.dot_general(a, b, (((1,), (0,)), ((), ())), preferred_element_type=jnp.float32)


def dot_tn(a, b):
    return lax.dot_general(a, b, (((0,), (0,)), ((), ())), preferred_element_type=jnp.float32)


def iota(shape, axis):
    return lax.broadcasted_iota(jnp.int32, shape, axis)


def ones_where(mask):
    return jnp.where(mask, 1.0, 0.0).astype(jnp.bfloat16)


def dispatch_kernel(
    ny,
    nz,
    nx,
    cap,
    features,
    next_features,
    ints,
    reals,
    source_weight,
    target_w1,
    target_mean,
    target_scale,
    target_shift,
    target_head,
    rows,
    notes,
    sent,
    sent_notes,
    q_all,
    acc,
    row_sems,
    note_sems,
    pair_sems,
    pair_note,
    q_sems,
):
    f32, bf16 = jnp.float32, jnp.bfloat16
    shards = 2 * ny * nz
    tokens = features.shape[0]
    me = lax.axis_index("dp")
    mx = lax.axis_index("member")
    c = lax.rem(me, 2)
    z = lax.rem(me // 2, nz)
    y = me // (2 * nz)
    partner = me + 1 - 2 * c

    def peer(i, sign):
        oc = lax.rem(i, 2)
        oz = lax.rem(far_first(lax.rem(i // 2, nz), nz), nz)
        oy = i // (2 * nz)
        yy = lax.rem(y + ny + sign * oy, ny)
        zz = lax.rem(z + nz + sign * oz, nz)
        return (yy * nz + zz) * 2 + lax.rem(c + oc, 2)

    last = 2 * nz - 2

    def step_of(i):
        return i + jnp.where(i >= last, 1, 0)

    def remote(src, dst, send, recv, device):
        return pltpu.make_async_remote_copy(
            src_ref=src, dst_ref=dst, send_sem=send, recv_sem=recv, device_id=device, device_id_type=MESH
        )

    barrier = pltpu.get_barrier_semaphore()

    def greet(i, _):
        pl.semaphore_signal(
            barrier, inc=1, device_id={"dp": peer(step_of(i), 1)}, device_id_type=MESH
        )
        return 0

    lax.fori_loop(0, shards - 1, greet, 0)
    for o in range(1, nx):
        pl.semaphore_signal(
            barrier, inc=1, device_id={"member": lax.rem(mx + o, nx)}, device_id_type=MESH
        )

    dest = ints[4:5, :]
    to_shard = dest == iota((shards, tokens), 0)
    chosen = ones_where(to_shard)
    before = ones_where(iota((tokens, tokens), 0) < iota((tokens, tokens), 1))
    rank = jnp.sum(jnp.where(to_shard, dot_nn(chosen, before), 0.0), axis=0, keepdims=True)
    rank = rank.astype(jnp.int32)
    slot = dest * cap + rank
    chunk = min(16, shards) * cap
    per = min(16, shards)

    def place(i, _):
        pick = ones_where(iota((chunk, tokens), 0) + i * chunk == slot)
        block = dot_nn(pick, features[...]).astype(bf16)
        sent[pl.ds(i * per, per)] = block.reshape(per, cap, features.shape[1])
        return 0

    lax.fori_loop(0, shards // per, place, 0)
    weight = jnp.zeros((1, tokens), f32)
    for k in range(source_weight.shape[0]):
        weight = jnp.where(ints[1:2, :] == k, source_weight[k], weight)

    pl.semaphore_wait(barrier, shards + nx - 2)

    def row_copy(i):
        to = peer(i, 1)
        return remote(
            sent.at[to], rows.at[lax.rem(to, 2), me], row_sems.at[0, i], row_sems.at[1, i], {"dp": to}
        )

    def row_landed(i):
        ref = rows.at[c, peer(i, -1)]
        return remote(ref, ref, row_sems.at[0, i], row_sems.at[1, i], {"dp": peer(i, 1)})

    def send_rows(i, _):
        row_copy(step_of(i)).start()
        return 0

    lax.fori_loop(0, shards - 1, send_rows, 0)
    rows[c, me] = sent[me]

    hidden = target_w1.shape[1]
    wide = min(256, hidden)
    tall = 128 if tokens % 128 == 0 else tokens
    acc[...] = jnp.zeros(acc.shape, f32)
    for k in range(2):

        def block(i, _, k=k):
            units = pl.ds(pl.multiple_of(i * wide, wide), wide)
            scale = target_scale[k : k + 1, units]
            shift = target_shift[k : k + 1, units] - target_mean[k : k + 1, units] * scale
            head = target_head[k : k + 1, units]
            w = target_w1[k, units, :]
            for t in range(tokens // tall):
                pre = dot_nt(next_features[t * tall : (t + 1) * tall, :], w)
                term = jnp.maximum(pre * scale + shift, 0.0) * head
                total = term[:, 0:128]
                for part in range(1, wide // 128):
                    total = total + term[:, part * 128 : (part + 1) * 128]
                acc[k, t * tall : (t + 1) * tall, :] += total
            return 0

        lax.fori_loop(0, hidden // wide, block, 0)
    for k in range(2):
        q_all[mx, k] = jnp.sum(acc[k].T, axis=0, keepdims=True)

    def q_copy(o):
        ref = q_all.at[mx]
        return remote(ref, ref, q_sems.at[0, o - 1], q_sems.at[1, o - 1], {"member": lax.rem(mx + o, nx)})

    for o in range(1, nx):
        q_copy(o).start()
    for o in range(1, nx):
        q_copy(o).wait_recv()
    first = jnp.zeros((1, tokens), f32)
    second = first
    for k in range(2 * nx):
        value = q_all[k // 2, k % 2]
        first = jnp.where(ints[2:3, :] == k, value, first)
        second = jnp.where(ints[3:4, :] == k, value, second)
    lowest = jnp.minimum(first, second)
    carry = 1.0 - ints[0:1, :].astype(f32)
    target = reals[0:1, :] + GAMMA * carry * (lowest - ALPHA * reals[1:2, :])

    lane = iota((128, tokens), 0)
    spread = jnp.where(to_shard, target, 0.0).astype(bf16)
    spread_w = jnp.where(to_shard, weight, 0.0).astype(bf16)
    note = dot_nt(spread, ones_where(lane == rank)) + dot_nt(
        spread_w, ones_where(lane == rank + cap)
    )
    sent_notes[...] = note.reshape(shards, 1, 128)

    def note_copy(i):
        to = peer(i, 1)
        return remote(
            sent_notes.at[to],
            notes.at[lax.rem(to, 2), me],
            note_sems.at[0, i],
            note_sems.at[1, i],
            {"dp": to},
        )

    def note_landed(i):
        ref = notes.at[c, peer(i, -1)]
        return remote(ref, ref, note_sems.at[0, i], note_sems.at[1, i], {"dp": peer(i, 1)})

    def send_notes(i, _):
        note_copy(step_of(i)).start()
        return 0

    lax.fori_loop(0, shards - 1, send_notes, 0)
    notes[c, me] = sent_notes[me]

    def pair_copy(i):
        ref = rows.at[c, peer(i, -1)]
        return remote(ref, ref, pair_sems.at[0, i], pair_sems.at[1, i], {"dp": partner})

    pair_copy(last).start()

    def relay(i, _):
        step = step_of(shards - 2 - i)
        row_landed(step).wait_recv()
        pair_copy(step).start()
        return 0

    lax.fori_loop(0, shards - 1, relay, 0)

    def note_wait(i, _):
        note_landed(step_of(i)).wait_recv()
        return 0

    lax.fori_loop(0, shards - 1, note_wait, 0)
    pair_n = remote(notes.at[c], notes.at[c], pair_note.at[0], pair_note.at[1], {"dp": partner})
    pair_n.start()

    def drain(i, _):
        row_copy(step_of(i)).wait_send()
        note_copy(step_of(i)).wait_send()
        return 0

    lax.fori_loop(0, shards - 1, drain, 0)

    def pair_wait(i, _):
        pair_copy(i).wait()
        return 0

    lax.fori_loop(0, shards, pair_wait, 0)
    for o in range(1, nx):
        q_copy(o).wait_send()
    pair_n.wait()


def dispatch(features, next_features, ints, reals, source_weight, targets, ny, nz, nx):
    tokens, width = features.shape
    shards = 2 * ny * nz
    cap = 2 * tokens // shards
    f32, bf16 = jnp.float32, jnp.bfloat16
    vmem = pl.BlockSpec(memory_space=pltpu.VMEM)
    dma = pltpu.SemaphoreType.DMA
    return pl.pallas_call(
        functools.partial(dispatch_kernel, ny, nz, nx, cap),
        out_shape=(
            jax.ShapeDtypeStruct((2, shards, cap, width), bf16),
            jax.ShapeDtypeStruct((2, shards, 1, 128), f32),
        ),
        in_specs=[vmem] * 4 + [pl.BlockSpec(memory_space=pltpu.SMEM)] + [vmem] * 5,
        out_specs=[vmem] * 2,
        scratch_shapes=[
            pltpu.VMEM((shards, cap, width), bf16),
            pltpu.VMEM((shards, 1, 128), f32),
            pltpu.VMEM((nx, 2, 1, tokens), f32),
            pltpu.VMEM((2, tokens, 128), f32),
            dma((2, shards)),
            dma((2, shards)),
            dma((2, shards)),
            dma((2,)),
            dma((2, nx - 1)),
        ],
        compiler_params=pltpu.CompilerParams(collective_id=1, has_side_effects=True),
        cost_estimate=pl.CostEstimate(flops=10**9, bytes_accessed=4 * 10**6, transcendentals=0),
        name="dispatch",
    )(features, next_features, ints, reals, source_weight, *targets)


def critic_kernel(
    cap,
    tile,
    rows,
    notes,
    shift_all,
    head_all,
    w_hbm,
    h,
    hs,
    w_wide,
    w,
    xc,
    targets,
    weights,
    zbuf,
    gbuf,
    gz,
    gt,
    sq,
    s0,
    s1,
    sem,
):
    f32, bf16 = jnp.float32, jnp.bfloat16
    slots, width = rows.shape[1:]
    hidden = w.shape[0]
    shards = slots // cap
    pieces = slots // 128
    few, many = 3, 6
    wide = min(256, hidden)
    lanes = hidden // 128
    c = lax.rem(lax.axis_index("dp"), 2)
    fetch = pltpu.make_async_copy(w_hbm.at[c], w_wide, sem)
    fetch.start()
    shift = shift_all[pl.ds(c, 1), :]
    head = head_all[pl.ds(c, 1), :]

    owner = ones_where(iota((shards, slots), 1) // cap == iota((shards, slots), 0))
    my_slot = lax.rem(iota((cap, slots), 1), cap) == iota((cap, slots), 0)
    upto = ones_where(iota((128, 128), 0) <= iota((128, 128), 1))
    counts = []
    for s in range(2):
        by_slot = notes[s, :, 0, :].T[0 : 2 * cap].astype(bf16)
        spread = dot_nn(by_slot, owner)
        y_row = jnp.sum(jnp.where(my_slot, spread[0:cap], 0.0), axis=0, keepdims=True)
        w_row = jnp.sum(jnp.where(my_slot, spread[cap : 2 * cap], 0.0), axis=0, keepdims=True)
        alive = jnp.where(w_row > 0, 1.0, 0.0)
        stacked = jnp.concatenate(
            [alive[:, p * 128 : (p + 1) * 128] for p in range(pieces)]
            + [jnp.zeros((8, 128), f32)] * (1 if pieces < 8 else 0),
            axis=0,
        )
        running = dot_nn(stacked.astype(bf16), upto)
        place = []
        start = jnp.zeros((1, 1), f32)
        for p in range(pieces):
            position = running[p : p + 1] - 1.0 + start
            position = jnp.where(stacked[p : p + 1] > 0, position, -1.0)
            place.append(position.astype(jnp.int32))
            start = start + running[p : p + 1, 127:128]
        number = jnp.sum(alive)
        counts.append(number)
        y_wide = jnp.broadcast_to(y_row, (128, slots)).astype(bf16)
        w_wide_row = jnp.broadcast_to(w_row, (128, slots)).astype(bf16)
        trips = jnp.where(number <= few * tile, few, many)

        def compact(i, _, s=s, place=place, y_wide=y_wide, w_wide_row=w_wide_row):
            at = pl.ds(pl.multiple_of(i * tile, tile), tile)
            row = iota((tile, 128), 0) + i * tile
            pick = jnp.concatenate([ones_where(row == p) for p in place], axis=1)
            xc[s, at, :] = dot_nn(pick, rows[s]).astype(bf16)
            targets[s, at, :] = dot_nt(pick, y_wide)
            weights[s, at, :] = dot_nt(pick, w_wide_row)
            return 0

        lax.fori_loop(0, trips, compact, 0)

    fetch.wait()
    w[...] = w_wide[...].astype(bf16)
    total0 = jnp.zeros((1, hidden), f32)
    total1 = jnp.zeros((1, hidden), f32)
    groups = tile // 8
    for s in range(2):
        number = counts[s]
        whole = jnp.full((1, 1), number, f32)
        trips = jnp.where(number <= few * tile, few, many)
        middle = jnp.sum(rows[s].astype(f32), axis=0, keepdims=True) / whole
        one = middle.astype(bf16)
        rest = middle - one.astype(f32)
        two = rest.astype(bf16)
        three = (rest - two.astype(f32)).astype(bf16)
        parts = jnp.concatenate(
            [one.astype(f32), two.astype(f32), three.astype(f32), jnp.zeros((13, width), f32)], axis=0
        ).astype(bf16)
        mu = jnp.sum(dot_nt(parts, w[...]), axis=0, keepdims=True)
        sq[...] = jnp.zeros(sq.shape, f32)
        s0[...] = jnp.zeros(s0.shape, f32)
        s1[...] = jnp.zeros(s1.shape, f32)

        def forward(i, _, s=s, mu=mu, number=number):
            at = pl.ds(pl.multiple_of(i * tile, tile), tile)
            row = iota((tile, 128), 0) + i * tile
            alive = jnp.where(row < number.astype(jnp.int32), 1.0, 0.0)
            x = xc[s, at, :]
            for j in range(hidden // wide):
                pre = dot_nt(x, w[j * wide : (j + 1) * wide, :])
                for k in range(wide // 128):
                    lo = j * wide + k * 128
                    zc = (pre[:, k * 128 : (k + 1) * 128] - mu[:, lo : lo + 128]) * alive
                    zbuf[at, lo : lo + 128] = zc
                    sq[:, lo : lo + 128] += jnp.sum((zc * zc).reshape(groups, 8, 128), axis=0)
            return 0

        lax.fori_loop(0, trips, forward, 0)
        var = jnp.sum(sq[...], axis=0, keepdims=True) / whole
        inv = 1.0 / jnp.sqrt(var + EPS)

        def slopes(i, _, s=s, inv=inv):
            at = pl.ds(pl.multiple_of(i * tile, tile), tile)
            acc = jnp.zeros((tile, 128), f32)
            for j in range(lanes):
                cut = slice(j * 128, (j + 1) * 128)
                zh = zbuf[at, cut] * inv[:, cut]
                zbuf[at, cut] = zh
                acc = acc + jnp.maximum(zh + shift[:, cut], 0.0) * head[:, cut]
            q = jnp.sum(acc, axis=1, keepdims=True)
            dq = weights[s, at, :] * (q - targets[s, at, :])
            for j in range(lanes):
                cut = slice(j * 128, (j + 1) * 128)
                zh = zbuf[at, cut]
                g = jnp.where(zh > -shift[:, cut], dq, 0.0)
                gbuf[at, cut] = g
                s0[:, cut] += jnp.sum(g.reshape(groups, 8, 128), axis=0)
                s1[:, cut] += jnp.sum((g * zh).reshape(groups, 8, 128), axis=0)
            return 0

        lax.fori_loop(0, trips, slopes, 0)
        sum0 = jnp.sum(s0[...], axis=0, keepdims=True)
        sum1 = jnp.sum(s1[...], axis=0, keepdims=True)
        total0 = total0 + sum0
        total1 = total1 + sum1
        scale = inv * head
        base = -scale * (sum0 / whole)
        tilt = -scale * (sum1 / whole)

        def backward(i, _, scale=scale, base=base, tilt=tilt):
            at = pl.ds(pl.multiple_of(i * tile, tile), tile)
            for j in range(lanes):
                cut = slice(j * 128, (j + 1) * 128)
                value = gbuf[at, cut] * scale[:, cut] + (zbuf[at, cut] * tilt[:, cut] + base[:, cut])
                gz[at, cut] = value.astype(bf16)
            return 0

        lax.fori_loop(0, trips, backward, 0)

        def product(depth, s=s):
            x = xc[s, 0:depth, :]
            for j in range(hidden // wide):
                cut = slice(j * wide, (j + 1) * wide)
                out = dot_tn(x, gz[0:depth, cut])
                gt[:, cut] = out if s == 0 else gt[:, cut] + out

        @pl.when(trips == few)
        def _():
            product(few * tile)

        @pl.when(trips != few)
        def _():
            product(many * tile)

    g_shift = head * total0
    g_head = shift * total0 + total1
    for u in range(lanes):
        cut = slice(u * 128, (u + 1) * 128)
        h[2 * u] = gt[0:128, cut].astype(bf16)
        h[2 * u + 1] = gt[128:256, cut].astype(bf16)
        hs[2 * u] = g_shift[:, cut]
        hs[2 * u + 1] = g_head[:, cut]


def critic_sums(rows, notes, shift, head, w1, cap):
    f32, bf16 = jnp.float32, jnp.bfloat16
    slots, width = rows.shape[1:]
    hidden = w1.shape[1]
    tile = slots * 3 // 16
    tall = 6 * tile
    vmem = pl.BlockSpec(memory_space=pltpu.VMEM)
    blocks = hidden // 128 * (width // 128)
    return pl.pallas_call(
        functools.partial(critic_kernel, cap, tile),
        out_shape=(
            jax.ShapeDtypeStruct((blocks, 128, 128), bf16),
            jax.ShapeDtypeStruct((blocks, 1, 128), f32),
        ),
        in_specs=[vmem] * 4 + [pl.BlockSpec(memory_space=pl.ANY)],
        out_specs=[vmem] * 2,
        scratch_shapes=[
            pltpu.VMEM((hidden, width), f32),
            pltpu.VMEM((hidden, width), bf16),
            pltpu.VMEM((2, tall, width), bf16),
            pltpu.VMEM((2, tall, 128), f32),
            pltpu.VMEM((2, tall, 128), f32),
            pltpu.VMEM((tall, hidden), f32),
            pltpu.VMEM((tall, hidden), f32),
            pltpu.VMEM((tall, hidden), bf16),
            pltpu.VMEM((width, hidden), f32),
            pltpu.VMEM((8, hidden), f32),
            pltpu.VMEM((8, hidden), f32),
            pltpu.VMEM((8, hidden), f32),
            pltpu.SemaphoreType.DMA,
        ],
        compiler_params=pltpu.CompilerParams(vmem_limit_bytes=60 * 2**20),
        cost_estimate=pl.CostEstimate(
            flops=8 * slots * hidden * width, bytes_accessed=4 * 10**6, transcendentals=0
        ),
        name="critic_sums",
    )(rows, notes, shift, head, w1)


def per_device(
    features,
    next_features,
    rewards,
    next_logp,
    terminal,
    source_ids,
    source_weight,
    subset,
    destination,
    critic_w1,
    critic_shift,
    critic_head,
    target_w1,
    target_mean,
    target_scale,
    target_shift,
    target_head,
):
    f32 = jnp.float32
    shards = lax.axis_size("dp")
    nx = lax.axis_size("member")
    nz = NZ
    ny = shards // (2 * nz)
    tokens, width = features.shape
    critics, hidden = critic_w1.shape[:2]
    cap = 2 * tokens // shards
    zero = jnp.zeros_like(terminal)
    ints = jnp.stack(
        [terminal, source_ids, subset[:, 0], subset[:, 1], destination, zero, zero, zero]
    )
    reals = jnp.stack([rewards, next_logp]).astype(f32)
    rows, notes = dispatch(
        features,
        next_features,
        ints,
        reals,
        source_weight.astype(f32),
        (target_w1, target_mean, target_scale, target_shift, target_head),
        ny,
        nz,
        nx,
    )
    h, hs = critic_sums(
        rows.reshape(2, shards * cap, width), notes, critic_shift, critic_head, critic_w1, cap
    )
    h = h.reshape(ny, nz, 128, 128)
    hs = hs.reshape(ny, nz, 1, 128)
    full, small, squares = reduce_all(h, hs, ny, nz, nx)
    root = jnp.float32(math.sqrt(critics * nx * hidden * (width + 2)))
    norm = jnp.sqrt(squares[0, 0])
    factor = root / jnp.maximum(norm, root)
    step_w1 = full.reshape(critics, hidden, width).astype(f32) * factor
    small = small[..., 0, 0:128].reshape(critics, hidden // 128, 2, 128)
    step_shift = small[:, :, 0, :].reshape(critics, hidden) * factor
    step_head = small[:, :, 1, :].reshape(critics, hidden) * factor
    return (step_w1, step_shift, step_head)


def solution(mesh):
    in_specs = (
        P("dp", None),
        P("dp", None),
        P("dp"),
        P("dp"),
        P("dp"),
        P("dp"),
        P(),
        P("dp", None),
        P("dp"),
        P("member", None, None),
        P("member", None),
        P("member", None),
        P("member", None, None),
        P("member", None),
        P("member", None),
        P("member", None),
        P("member", None),
    )
    out_specs = (P("member", None, None), P("member", None), P("member", None))
    return jax.shard_map(
        per_device, mesh=mesh, in_specs=in_specs, out_specs=out_specs, check_vma=False
    )
```

```python
import functools
import math

import jax
import jax.numpy as jnp
from jax import lax
from jax.experimental import pallas as pl
from jax.experimental.pallas import tpu as pltpu
from jax.sharding import PartitionSpec as P

GAMMA = 0.99
ALPHA = 0.2
EPS = 1e-05
NZ = 8
MESH = pl.DeviceIdType.MESH


def far_first(i, nz):
    half = nz // 2
    return half + ((i + 1) // 2) * (2 * ((i + 1) % 2) - 1)


def reduce_kernel(
    ny,
    nz,
    nx,
    h,
    hs,
    full,
    shift_out,
    head_out,
    factor_out,
    t_in,
    m_out,
    n_in,
    r_out,
    r_in,
    small,
    ys_in,
    zs_out,
    zs_in,
    x_out,
    x_in,
    t_sems,
    u_sems,
    m_sems,
    r_sems,
    gz_sems,
    tie_sems,
    gy_sems,
    go_sems,
    pair_sems,
    ys_sems,
    zs_sems,
    gzs_sems,
    gys_sems,
    pair_small,
    x_sems,
):
    f32, bf16 = jnp.float32, jnp.bfloat16
    me = lax.axis_index("dp")
    mx = lax.axis_index("member")
    c = lax.rem(me, 2)
    z = lax.rem(me // 2, nz)
    y = me // (2 * nz)
    partner = me + 1 - 2 * c
    half = nz // 2
    started = []

    def dp_of(yy, zz):
        return (yy * nz + zz) * 2 + c

    def yo(o):
        return lax.rem(y + (o % ny), ny)

    def zo(o):
        return lax.rem(z + (o % nz), nz)

    up, down, over = yo(1), yo(-1), yo(2)

    def copy(src, dst, sems, index, device):
        return pltpu.make_async_remote_copy(
            src_ref=src,
            dst_ref=dst,
            send_sem=sems.at[(0,) + index],
            recv_sem=sems.at[(1,) + index],
            device_id=device,
            device_id_type=MESH,
        )

    def send(*args):
        c = copy(*args)
        c.start()
        started.append(c)

    def landed(ref, sems, index):
        copy(ref, ref, sems, index, {"dp": partner}).wait_recv()

    def to_y(yy):
        return {"dp": dp_of(yy, z)}

    def to_z(zz):
        return {"dp": dp_of(y, zz)}

    def block_of(yy, zz):
        return full.at[
            c, yy * (nz // 2) + zz // 2, :, pl.ds(pl.multiple_of(lax.rem(zz, 2) * 128, 128), 128)
        ]

    def half_of(yy, zz, part):
        return full.at[
            c,
            yy * (nz // 2) + zz // 2,
            pl.ds(part * 64, 64),
            pl.ds(pl.multiple_of(lax.rem(zz, 2) * 128, 128), 128),
        ]

    barrier = pltpu.get_barrier_semaphore()
    for o in range(1, ny):
        pl.semaphore_signal(barrier, inc=1, device_id=to_y(yo(o)), device_id_type=MESH)
    for o in range(1, nz):
        pl.semaphore_signal(barrier, inc=1, device_id=to_z(zo(o)), device_id_type=MESH)
    pl.semaphore_signal(barrier, inc=1, device_id={"dp": partner}, device_id_type=MESH)
    for o in range(1, nx):
        pl.semaphore_signal(
            barrier, inc=1, device_id={"member": lax.rem(mx + o, nx)}, device_id_type=MESH
        )
    pl.semaphore_wait(barrier, ny + nz + nx - 2)

    first, second = pl.ds(0, 64), pl.ds(64, 64)
    order = [half]
    for k in range(half - 1, 0, -1):
        order += [nz - k, k]
    order.append(0)

    for o in range(1, ny):
        send(hs.at[yo(o)], ys_in.at[o - 1], ys_sems, (o - 1,), to_y(yo(o)))
    for o in order:
        send(h.at[over, zo(o), first], t_in.at[0, o], t_sems, (0, o), to_y(up))
        send(h.at[over, zo(o), second], t_in.at[1, o], t_sems, (1, o), to_y(down))
    for o in order:
        landed(t_in.at[0, o], t_sems, (0, o))
        m_out[0, o] = (h[up, zo(o), 0:64].astype(f32) + t_in[0, o].astype(f32)).astype(bf16)
        send(m_out.at[0, o], n_in.at[0, o, first], m_sems, (0, o), to_y(up))
        send(h.at[up, zo(o), second], n_in.at[0, o, second], u_sems, (0, o), to_y(up))
        landed(t_in.at[1, o], t_sems, (1, o))
        m_out[1, o] = (h[down, zo(o), 64:128].astype(f32) + t_in[1, o].astype(f32)).astype(bf16)
        send(m_out.at[1, o], n_in.at[1, o, second], m_sems, (1, o), to_y(down))
        send(h.at[down, zo(o), first], n_in.at[1, o, first], u_sems, (1, o), to_y(down))
    for o in range(1, ny):
        landed(ys_in.at[o - 1], ys_sems, (o - 1,))
    zs_out[...] = hs[y] + sum(ys_in[o - 1] for o in range(1, ny))
    for o in range(1, nz):
        send(zs_out.at[zo(o)], zs_in.at[o - 1], zs_sems, (o - 1,), to_z(zo(o)))

    for o in order:
        landed(n_in.at[0, o, first], m_sems, (0, o))
        landed(n_in.at[0, o, second], u_sems, (0, o))
        landed(n_in.at[1, o, second], m_sems, (1, o))
        landed(n_in.at[1, o, first], u_sems, (1, o))
        value = h[y, zo(o)].astype(f32) + n_in[0, o].astype(f32) + n_in[1, o].astype(f32)
        if o == 0:
            r_out[0] = value
        elif o <= half:
            if o < half:
                landed(r_in.at[o], r_sems, (o,))
                value = value + r_in[o]
            r_out[o] = value
            send(r_out.at[o], r_in.at[o - 1], r_sems, (o - 1,), to_z(zo(1)))
        else:
            if nz - o < half - 1:
                landed(r_in.at[o], r_sems, (o,))
                value = value + r_in[o]
            r_out[o] = value
            send(r_out.at[o], r_in.at[o + 1], r_sems, (o + 1,), to_z(zo(-1)))
    for o in range(1, nz):
        landed(zs_in.at[o - 1], zs_sems, (o - 1,))
    mine_small = zs_out[z] + sum(zs_in[o - 1] for o in range(1, nz))
    landed(r_in.at[0], r_sems, (0,))
    mine = r_out[0] + r_in[0]
    if half > 1:
        landed(r_in.at[nz], r_sems, (nz,))
        mine = mine + r_in[nz]
    block_of(y, z)[...] = mine.T.astype(bf16)

    if half > 1:
        reach = [d for k in range(1, half) for d in (k, -k)]
    else:
        reach = [1]
    for d in reversed(reach):
        ref = block_of(y, z)
        send(ref, ref, gz_sems, (d % nz,), to_z(zo(d)))
    squares = jnp.sum(mine * mine) + jnp.sum(mine_small * mine_small)
    small[c, y, z, :, 0:128] = mine_small
    small[c, y, z, :, 128:256] = jnp.full((1, 128), squares, f32)
    for o in range(1, nz):
        ref = small.at[c, y, z]
        send(ref, ref, gzs_sems, (o - 1,), to_z(zo(o)))

    def along_y(o):
        ref = block_of(y, zo(-o))
        send(ref, ref, gy_sems, (0, o), to_y(up))
        send(ref, ref, gy_sems, (1, o), to_y(down))
        send(ref, ref, pair_sems, (0, o), {"dp": partner})

    def from_y(o):
        zz = zo(-o)
        ref = block_of(down, zz)
        landed(ref, gy_sems, (0, o))
        part = half_of(down, zz, 0)
        send(part, part, go_sems, (0, o), to_y(up))
        send(ref, ref, pair_sems, (1, o), {"dp": partner})
        ref = block_of(up, zz)
        landed(ref, gy_sems, (1, o))
        part = half_of(up, zz, 1)
        send(part, part, go_sems, (1, o), to_y(down))
        send(ref, ref, pair_sems, (2, o), {"dp": partner})

    def from_over(o):
        zz = zo(-o)
        landed(half_of(over, zz, 0), go_sems, (0, o))
        landed(half_of(over, zz, 1), go_sems, (1, o))
        ref = block_of(over, zz)
        send(ref, ref, pair_sems, (3, o), {"dp": partner})

    along_y(0)
    for o in range(1, nz):
        landed(small.at[c, y, zo(-o)], gzs_sems, (o - 1,))
    for o in range(1, ny):
        ref = small.at[c, y]
        send(ref, ref, gys_sems, (o - 1,), to_y(yo(o)))
    items = [0]
    lag = 2
    for d in reach + ([half] if half > 1 else []):
        o = d % nz
        if d == half and half > 1:
            landed(half_of(y, zo(-o), 0), tie_sems, (0,))
            landed(half_of(y, zo(-o), 1), tie_sems, (1,))
        else:
            landed(block_of(y, zo(-o)), gz_sems, (o,))
        if half > 1 and d == half - 1:
            part = half_of(y, zo(-o), 0)
            send(part, part, tie_sems, (0,), to_z(zo(1)))
        if half > 1 and d == 1 - half:
            part = half_of(y, zo(-o), 1)
            send(part, part, tie_sems, (1,), to_z(zo(-1)))
        along_y(o)
        items.append(o)
        if len(items) > lag:
            from_y(items[len(items) - 1 - lag])
    for o in range(1, ny):
        landed(small.at[c, yo(-o)], gys_sems, (o - 1,))
    send(small.at[c], small.at[c], pair_small, (0,), {"dp": partner})
    for o in items[max(0, len(items) - lag) :]:
        from_y(o)
    landed(small.at[1 - c], pair_small, (0,))
    x_out[...] = jnp.sum(small[:, :, :, :, 128:256], axis=(0, 1, 2))
    for o in range(1, nx):
        send(x_out, x_in.at[o - 1], x_sems, (o - 1,), {"member": lax.rem(mx + o, nx)})
    for o in items:
        from_over(o)
    for k in range(2):
        for b in range(ny * nz // 2):
            cut = slice(b * 128, (b + 1) * 128)
            at = b // (nz // 2), 2 * (b % (nz // 2))
            shift_out[k : k + 1, cut] = small[k, at[0], at[1], :, 0:128]
            head_out[k : k + 1, cut] = small[k, at[0], at[1] + 1, :, 0:128]
    for o in range(1, nx):
        landed(x_in.at[o - 1], x_sems, (o - 1,))
    total = x_out[...] + sum(x_in[o - 1] for o in range(1, nx))
    root = math.sqrt(2 * nx * (ny * nz // 2 * 128) * 258)
    factor_out[...] = root / jnp.maximum(jnp.sqrt(total), root)
    for o in items:
        for k in range(4):
            zz = zo(-o)
            yy = (y, down, up, over)[k]
            landed(block_of(yy, zz), pair_sems, (k, o))
    for c in started:
        c.wait_send()


def reduce_all(h, hs, ny, nz, nx):
    f32, bf16 = jnp.float32, jnp.bfloat16
    vmem = pl.BlockSpec(memory_space=pltpu.VMEM)
    dma = pltpu.SemaphoreType.DMA
    hidden = ny * nz // 2 * 128
    return pl.pallas_call(
        functools.partial(reduce_kernel, ny, nz, nx),
        out_shape=(
            jax.ShapeDtypeStruct((2, ny * nz // 2, 128, 256), bf16),
            jax.ShapeDtypeStruct((2, hidden), f32),
            jax.ShapeDtypeStruct((2, hidden), f32),
            jax.ShapeDtypeStruct((1, 128), f32),
        ),
        in_specs=[vmem] * 2,
        out_specs=[vmem] * 4,
        scratch_shapes=[
            pltpu.VMEM((2, nz, 64, 128), bf16),
            pltpu.VMEM((2, nz, 64, 128), bf16),
            pltpu.VMEM((2, nz, 128, 128), bf16),
            pltpu.VMEM((nz, 128, 128), f32),
            pltpu.VMEM((nz + 1, 128, 128), f32),
            pltpu.VMEM((2, ny, nz, 1, 256), f32),
            pltpu.VMEM((ny - 1, nz, 1, 128), f32),
            pltpu.VMEM((nz, 1, 128), f32),
            pltpu.VMEM((nz - 1, 1, 128), f32),
            pltpu.VMEM((1, 128), f32),
            pltpu.VMEM((nx - 1, 1, 128), f32),
            dma((2, 2, nz)),
            dma((2, 2, nz)),
            dma((2, 2, nz)),
            dma((2, nz + 1)),
            dma((2, nz)),
            dma((2, 2)),
            dma((2, 2, nz)),
            dma((2, 2, nz)),
            dma((2, 4, nz)),
            dma((2, ny - 1)),
            dma((2, nz - 1)),
            dma((2, nz - 1)),
            dma((2, ny - 1)),
            dma((2, 1)),
            dma((2, nx - 1)),
        ],
        compiler_params=pltpu.CompilerParams(collective_id=0, has_side_effects=True),
        cost_estimate=pl.CostEstimate(flops=10**7, bytes_accessed=4 * 10**6, transcendentals=0),
        name="gradient_sum",
    )(h, hs)


def dot_nt(a, b):
    return lax.dot_general(a, b, (((1,), (1,)), ((), ())), preferred_element_type=jnp.float32)


def dot_nn(a, b):
    return lax.dot_general(a, b, (((1,), (0,)), ((), ())), preferred_element_type=jnp.float32)


def dot_tn(a, b):
    return lax.dot_general(a, b, (((0,), (0,)), ((), ())), preferred_element_type=jnp.float32)


def iota(shape, axis):
    return lax.broadcasted_iota(jnp.int32, shape, axis)


def ones_where(mask):
    return jnp.where(mask, 1.0, 0.0).astype(jnp.bfloat16)


def dispatch_kernel(
    ny,
    nz,
    nx,
    cap,
    features,
    next_features,
    dest_ref,
    terminal,
    source_ids,
    subset,
    reals,
    target_mean,
    target_scale,
    target_shift,
    target_head,
    w_hbm,
    rows,
    notes,
    target_w1,
    sent,
    sent_notes,
    q_all,
    acc,
    w_sem,
    row_send,
    row_recv,
    note_sems,
    x_sems,
    pair_sems,
    pair_note,
    q_sems,
):
    f32, bf16 = jnp.float32, jnp.bfloat16
    shards = 2 * ny * nz
    flat = 2 * ny
    kept = cap // 2
    tokens, width = features.shape
    me = lax.axis_index("dp")
    mx = lax.axis_index("member")
    c = lax.rem(me, 2)
    z = lax.rem(me // 2, nz)
    y = me // (2 * nz)
    partner = me + 1 - 2 * c
    hh = lax.rem(mx, 2)
    neighbor = mx + 1 - 2 * hh
    fetch = pltpu.make_async_copy(w_hbm, target_w1, w_sem)
    fetch.start()

    def remote(src, dst, send, recv, device):
        return pltpu.make_async_remote_copy(
            src_ref=src, dst_ref=dst, send_sem=send, recv_sem=recv, device_id=device, device_id_type=MESH
        )

    def zo(o):
        return lax.rem(z + nz + o, nz)

    def group(oz, skip, act):
        for j in range(flat):
            oy, oc = j // 2, j % 2
            if skip and j == 0:
                continue
            yy = lax.rem(y + oy, ny)
            cc = lax.rem(c + oc, 2)
            zz = zo(oz)
            act(oz, (yy * nz + zz) * 2 + cc, zz * flat + yy * 2 + cc, cc)

    def each(act):
        def step(i, _):
            group(far_first(i, nz), False, act)
            return 0

        lax.fori_loop(0, nz - 1, step, 0)
        group(0, True, act)

    barrier = pltpu.get_barrier_semaphore()

    def greet(oz, to, place, cc):
        pl.semaphore_signal(barrier, inc=1, device_id={"dp": to}, device_id_type=MESH)

    each(greet)
    for o in range(1, nx):
        pl.semaphore_signal(
            barrier, inc=1, device_id={"member": lax.rem(mx + o, nx)}, device_id_type=MESH
        )

    dest = dest_ref[...]
    dest = ((dest >> 1) & (nz - 1)) * flat + (dest // (2 * nz)) * 2 + (dest & 1)
    to_shard = dest == iota((shards, tokens), 0)
    chosen = ones_where(to_shard)
    before = ones_where(iota((tokens, tokens), 0) < iota((tokens, tokens), 1))
    rank = jnp.sum(jnp.where(to_shard, dot_nn(chosen, before), 0.0), axis=0, keepdims=True)
    rank = rank.astype(jnp.int32)
    low = rank - hh * kept
    slot = jnp.where((low >= 0) & (low < kept), dest * kept + low, -1)
    chunk = min(256, shards * kept)
    per = chunk // kept
    for i in range(shards // per):
        pick = ones_where(iota((chunk, tokens), 0) + i * chunk == slot)
        block = dot_nn(pick, features[...]).astype(bf16)
        sent[i * per : (i + 1) * per] = block.reshape(per, kept, width)

    pl.semaphore_wait(barrier, shards + nx - 2)

    def send_rows(oz, to, place, cc):
        remote(
            sent.at[place],
            rows.at[cc, hh, z, y * 2 + c],
            row_send,
            row_recv.at[lax.rem(oz, nz)],
            {"dp": to},
        ).start()

    each(send_rows)
    rows[c, hh, z, y * 2 + c] = sent[z * flat + y * 2 + c]

    weight = jnp.zeros((1, tokens), f32)
    for k in range(reals.shape[1] - 2 * tokens - 120):
        value = reals[:, 2 * tokens + k : 2 * tokens + k + 1]
        weight = jnp.where(source_ids[...] == k, value, weight)

    hidden = target_w1.shape[1]
    wide = min(256, hidden)
    tall = min(128, tokens)
    acc[...] = jnp.zeros(acc.shape, f32)
    fetch.wait()
    for k in range(2):

        def block(i, _, k=k):
            units = pl.ds(pl.multiple_of(i * wide, wide), wide)
            scale = target_scale[k : k + 1, units]
            shift = target_shift[k : k + 1, units] - target_mean[k : k + 1, units] * scale
            head = target_head[k : k + 1, units]
            w = target_w1[k, units, :]
            for t in range(tokens // tall):
                pre = dot_nt(next_features[t * tall : (t + 1) * tall, :], w)
                term = jnp.maximum(pre * scale + shift, 0.0) * head
                total = term[:, 0:128]
                for part in range(1, wide // 128):
                    total = total + term[:, part * 128 : (part + 1) * 128]
                acc[k, t * tall : (t + 1) * tall, :] += total
            return 0

        lax.fori_loop(0, hidden // wide, block, 0)
        q_all[mx, k] = jnp.sum(acc[k].T, axis=0, keepdims=True)

    def q_copy(o):
        ref = q_all.at[mx]
        return remote(ref, ref, q_sems.at[0, o - 1], q_sems.at[1, o - 1], {"member": lax.rem(mx + o, nx)})

    for o in range(1, nx):
        q_copy(o).start()

    half = nz // 2
    arrivals = [0] + [o % nz for k in range(1, half) for o in (k, -k)] + [half]

    def x_copy(o):
        ref = rows.at[c, hh, zo(-o)]
        return remote(ref, ref, x_sems.at[0, o], x_sems.at[1, o], {"member": neighbor})

    def pair_copy(part, o):
        ref = rows.at[c, hh + part - 2 * hh * part, zo(-o)]
        return remote(ref, ref, pair_sems.at[0, part, o], pair_sems.at[1, part, o], {"dp": partner})

    def arrive(o):
        ref = rows.at[c, hh, zo(-o)]
        if o == 0:
            ref = rows.at[c, hh, z, pl.ds(0, flat - 1)]
        remote(ref, ref, row_send, row_recv.at[o], {"dp": partner}).wait_recv()
        x_copy(o).start()
        pair_copy(0, o).start()

    early = nz // 2
    for o in arrivals[:early]:
        arrive(o)

    for o in range(1, nx):
        q_copy(o).wait_recv()
    first = jnp.zeros((1, tokens), f32)
    second = first
    for k in range(2 * nx):
        value = q_all[k // 2, k % 2]
        first = jnp.where(subset[0:1, :] == k, value, first)
        second = jnp.where(subset[1:2, :] == k, value, second)
    lowest = jnp.minimum(first, second)
    carry = 1.0 - terminal[...].astype(f32)
    target = reals[:, 0:tokens] + GAMMA * carry * (lowest - ALPHA * reals[:, tokens : 2 * tokens])

    lane = iota((128, tokens), 0)
    spread = jnp.where(to_shard, target, 0.0).astype(bf16)
    spread_w = jnp.where(to_shard, weight, 0.0).astype(bf16)
    note = dot_nt(spread, ones_where(lane == rank)) + dot_nt(spread_w, ones_where(lane == rank + cap))
    sent_notes[...] = note.reshape(shards, 1, 128)
    mine = z * flat + y * 2 + c

    def send_notes(oz, to, place, cc):
        remote(
            sent_notes.at[place], notes.at[cc, mine], note_sems.at[0], note_sems.at[1], {"dp": to}
        ).start()

    each(send_notes)
    notes[c, mine] = sent_notes[mine]

    for o in arrivals[early:]:
        arrive(o)
    for o in arrivals:
        x_copy(o).wait_recv()
        pair_copy(1, o).start()
    most = notes.at[c, pl.ds(0, shards - 1)]
    all_notes = remote(most, most, note_sems.at[0], note_sems.at[1], {"dp": partner})
    all_notes.wait_recv()
    pair_n = remote(notes.at[c], notes.at[c], pair_note.at[0], pair_note.at[1], {"dp": partner})
    pair_n.start()

    all_notes.wait_send()
    most = sent.at[pl.ds(0, shards - 1)]
    remote(most, most, row_send, row_recv.at[0], {"dp": partner}).wait_send()
    for o in range(1, nx):
        q_copy(o).wait_send()
    for o in arrivals:
        x_copy(o).wait_send()
        pair_copy(0, o).wait()
        pair_copy(1, o).wait()
    pair_n.wait()


def dispatch(features, next_features, dest, terminal, source_ids, subset, reals, targets, ny, nz, nx):
    tokens, width = features.shape
    shards = 2 * ny * nz
    cap = 2 * tokens // shards
    f32, bf16 = jnp.float32, jnp.bfloat16
    vmem = pl.BlockSpec(memory_space=pltpu.VMEM)
    dma = pltpu.SemaphoreType.DMA
    w1 = targets[0]
    return pl.pallas_call(
        functools.partial(dispatch_kernel, ny, nz, nx, cap),
        out_shape=(
            jax.ShapeDtypeStruct((2, 2, nz, 2 * ny, cap // 2, width), bf16),
            jax.ShapeDtypeStruct((2, shards, 1, 128), f32),
        ),
        in_specs=[vmem] * 11 + [pl.BlockSpec(memory_space=pl.ANY)],
        out_specs=[vmem] * 2,
        scratch_shapes=[
            pltpu.VMEM(w1.shape, w1.dtype),
            pltpu.VMEM((shards, cap // 2, width), bf16),
            pltpu.VMEM((shards, 1, 128), f32),
            pltpu.VMEM((nx, 2, 1, tokens), f32),
            pltpu.VMEM((2, tokens, 128), f32),
            dma,
            dma,
            dma((nz,)),
            dma((2,)),
            dma((2, nz)),
            dma((2, 2, nz)),
            dma((2,)),
            dma((2, nx - 1)),
        ],
        compiler_params=pltpu.CompilerParams(collective_id=1, has_side_effects=True),
        cost_estimate=pl.CostEstimate(flops=10**9, bytes_accessed=4 * 10**6, transcendentals=0),
        name="dispatch",
    )(features, next_features, dest, terminal, source_ids, subset, reals, *targets[1:], w1)


def critic_kernel(
    cap,
    tile,
    rows,
    notes,
    shift_all,
    head_all,
    w_hbm,
    h,
    hs,
    w_wide,
    w,
    xc,
    targets,
    weights,
    zbuf,
    gbuf,
    gz,
    gt,
    sq,
    s0,
    s1,
    sem,
):
    f32, bf16 = jnp.float32, jnp.bfloat16
    slots, width = rows.shape[1:]
    hidden = w.shape[0]
    shards = slots // cap
    pieces = slots // 128
    few, many = 3, 6
    wide = min(256, hidden)
    lanes = hidden // 128
    c = lax.rem(lax.axis_index("dp"), 2)
    fetch = pltpu.make_async_copy(w_hbm.at[c], w_wide, sem)
    fetch.start()
    shift = shift_all[pl.ds(c, 1), :]
    head = head_all[pl.ds(c, 1), :]

    kept, part = cap // 2, slots // 2
    at_slot = iota((1, slots), 1)
    owner = ones_where(lax.rem(at_slot, part) // kept == iota((shards, slots), 0))
    my_slot = at_slot // part * kept + lax.rem(at_slot, kept) == iota((cap, slots), 0)
    upto = ones_where(iota((128, 128), 0) <= iota((128, 128), 1))
    counts = []
    for s in range(2):
        by_slot = notes[s, :, 0, :].T[0 : 2 * cap].astype(bf16)
        spread = dot_nn(by_slot, owner)
        y_row = jnp.sum(jnp.where(my_slot, spread[0:cap], 0.0), axis=0, keepdims=True)
        w_row = jnp.sum(jnp.where(my_slot, spread[cap : 2 * cap], 0.0), axis=0, keepdims=True)
        alive = jnp.where(w_row > 0, 1.0, 0.0)
        stacked = jnp.concatenate(
            [alive[:, p * 128 : (p + 1) * 128] for p in range(pieces)]
            + [jnp.zeros((8, 128), f32)] * (1 if pieces < 8 else 0),
            axis=0,
        )
        running = dot_nn(stacked.astype(bf16), upto)
        place = []
        start = jnp.zeros((1, 1), f32)
        for p in range(pieces):
            position = running[p : p + 1] - 1.0 + start
            position = jnp.where(stacked[p : p + 1] > 0, position, -1.0)
            place.append(position.astype(jnp.int32))
            start = start + running[p : p + 1, 127:128]
        number = jnp.sum(alive)
        counts.append(number)
        y_wide = jnp.broadcast_to(y_row, (128, slots)).astype(bf16)
        w_wide_row = jnp.broadcast_to(w_row, (128, slots)).astype(bf16)
        trips = jnp.where(number <= few * tile, few, many)

        def compact(i, _, s=s, place=place, y_wide=y_wide, w_wide_row=w_wide_row):
            at = pl.ds(pl.multiple_of(i * tile, tile), tile)
            row = iota((tile, 128), 0) + i * tile
            pick = jnp.concatenate([ones_where(row == p) for p in place], axis=1)
            xc[s, at, :] = dot_nn(pick, rows[s]).astype(bf16)
            targets[s, at, :] = dot_nt(pick, y_wide)
            weights[s, at, :] = dot_nt(pick, w_wide_row)
            return 0

        lax.fori_loop(0, trips, compact, 0)

    fetch.wait()
    w[...] = w_wide[...].astype(bf16)
    total0 = jnp.zeros((1, hidden), f32)
    total1 = jnp.zeros((1, hidden), f32)
    groups = tile // 8
    for s in range(2):
        number = counts[s]
        whole = jnp.full((1, 1), number, f32)
        trips = jnp.where(number <= few * tile, few, many)
        middle = jnp.sum(rows[s].astype(f32), axis=0, keepdims=True) / whole
        one = middle.astype(bf16)
        rest = middle - one.astype(f32)
        two = rest.astype(bf16)
        three = (rest - two.astype(f32)).astype(bf16)
        parts = jnp.concatenate(
            [one.astype(f32), two.astype(f32), three.astype(f32), jnp.zeros((13, width), f32)], axis=0
        ).astype(bf16)
        mu = jnp.sum(dot_nt(parts, w[...]), axis=0, keepdims=True)
        sq[...] = jnp.zeros(sq.shape, f32)
        s0[...] = jnp.zeros(s0.shape, f32)
        s1[...] = jnp.zeros(s1.shape, f32)

        def forward(i, _, s=s, mu=mu, number=number):
            at = pl.ds(pl.multiple_of(i * tile, tile), tile)
            row = iota((tile, 128), 0) + i * tile
            alive = jnp.where(row < number.astype(jnp.int32), 1.0, 0.0)
            x = xc[s, at, :]
            for j in range(hidden // wide):
                pre = dot_nt(x, w[j * wide : (j + 1) * wide, :])
                for k in range(wide // 128):
                    lo = j * wide + k * 128
                    zc = (pre[:, k * 128 : (k + 1) * 128] - mu[:, lo : lo + 128]) * alive
                    zbuf[at, lo : lo + 128] = zc
                    sq[:, lo : lo + 128] += jnp.sum((zc * zc).reshape(groups, 8, 128), axis=0)
            return 0

        lax.fori_loop(0, trips, forward, 0)
        var = jnp.sum(sq[...], axis=0, keepdims=True) / whole
        inv = 1.0 / jnp.sqrt(var + EPS)

        def slopes(i, _, s=s, inv=inv):
            at = pl.ds(pl.multiple_of(i * tile, tile), tile)
            acc = jnp.zeros((tile, 128), f32)
            for j in range(lanes):
                cut = slice(j * 128, (j + 1) * 128)
                zh = zbuf[at, cut] * inv[:, cut]
                zbuf[at, cut] = zh
                acc = acc + jnp.maximum(zh + shift[:, cut], 0.0) * head[:, cut]
            q = jnp.sum(acc, axis=1, keepdims=True)
            dq = weights[s, at, :] * (q - targets[s, at, :])
            for j in range(lanes):
                cut = slice(j * 128, (j + 1) * 128)
                zh = zbuf[at, cut]
                g = jnp.where(zh > -shift[:, cut], dq, 0.0)
                gbuf[at, cut] = g
                s0[:, cut] += jnp.sum(g.reshape(groups, 8, 128), axis=0)
                s1[:, cut] += jnp.sum((g * zh).reshape(groups, 8, 128), axis=0)
            return 0

        lax.fori_loop(0, trips, slopes, 0)
        sum0 = jnp.sum(s0[...], axis=0, keepdims=True)
        sum1 = jnp.sum(s1[...], axis=0, keepdims=True)
        total0 = total0 + sum0
        total1 = total1 + sum1
        scale = inv * head
        base = -scale * (sum0 / whole)
        tilt = -scale * (sum1 / whole)

        def backward(i, _, scale=scale, base=base, tilt=tilt):
            at = pl.ds(pl.multiple_of(i * tile, tile), tile)
            for j in range(lanes):
                cut = slice(j * 128, (j + 1) * 128)
                value = gbuf[at, cut] * scale[:, cut] + (zbuf[at, cut] * tilt[:, cut] + base[:, cut])
                gz[at, cut] = value.astype(bf16)
            return 0

        lax.fori_loop(0, trips, backward, 0)

        def product(depth, s=s):
            x = xc[s, 0:depth, :]
            for j in range(hidden // wide):
                cut = slice(j * wide, (j + 1) * wide)
                out = dot_tn(x, gz[0:depth, cut])
                gt[:, cut] = out if s == 0 else gt[:, cut] + out

        @pl.when(trips == few)
        def _():
            product(few * tile)

        @pl.when(trips != few)
        def _():
            product(many * tile)

    g_shift = head * total0
    g_head = shift * total0 + total1
    for u in range(lanes):
        cut = slice(u * 128, (u + 1) * 128)
        h[2 * u] = gt[0:128, cut].astype(bf16)
        h[2 * u + 1] = gt[128:256, cut].astype(bf16)
        hs[2 * u] = g_shift[:, cut]
        hs[2 * u + 1] = g_head[:, cut]


def critic_sums(rows, notes, shift, head, w1, cap):
    f32, bf16 = jnp.float32, jnp.bfloat16
    slots, width = rows.shape[1:]
    hidden = w1.shape[1]
    tile = slots * 3 // 16
    tall = 6 * tile
    vmem = pl.BlockSpec(memory_space=pltpu.VMEM)
    blocks = hidden // 128 * (width // 128)
    return pl.pallas_call(
        functools.partial(critic_kernel, cap, tile),
        out_shape=(
            jax.ShapeDtypeStruct((blocks, 128, 128), bf16),
            jax.ShapeDtypeStruct((blocks, 1, 128), f32),
        ),
        in_specs=[vmem] * 4 + [pl.BlockSpec(memory_space=pl.ANY)],
        out_specs=[vmem] * 2,
        scratch_shapes=[
            pltpu.VMEM((hidden, width), f32),
            pltpu.VMEM((hidden, width), bf16),
            pltpu.VMEM((2, tall, width), bf16),
            pltpu.VMEM((2, tall, 128), f32),
            pltpu.VMEM((2, tall, 128), f32),
            pltpu.VMEM((tall, hidden), f32),
            pltpu.VMEM((tall, hidden), f32),
            pltpu.VMEM((tall, hidden), bf16),
            pltpu.VMEM((width, hidden), f32),
            pltpu.VMEM((8, hidden), f32),
            pltpu.VMEM((8, hidden), f32),
            pltpu.VMEM((8, hidden), f32),
            pltpu.SemaphoreType.DMA,
        ],
        compiler_params=pltpu.CompilerParams(vmem_limit_bytes=60 * 2**20),
        cost_estimate=pl.CostEstimate(
            flops=8 * slots * hidden * width, bytes_accessed=4 * 10**6, transcendentals=0
        ),
        name="critic_sums",
    )(rows, notes, shift, head, w1)


def per_device(
    features,
    next_features,
    rewards,
    next_logp,
    terminal,
    source_ids,
    source_weight,
    subset,
    destination,
    critic_w1,
    critic_shift,
    critic_head,
    target_w1,
    target_mean,
    target_scale,
    target_shift,
    target_head,
):
    f32 = jnp.float32
    shards = lax.axis_size("dp")
    nx = lax.axis_size("member")
    nz = NZ
    ny = shards // (2 * nz)
    tokens, width = features.shape
    critics, hidden = critic_w1.shape[:2]
    cap = 2 * tokens // shards
    reals = jnp.concatenate(
        [
            rewards.astype(f32),
            next_logp.astype(f32),
            source_weight.astype(f32),
            jnp.zeros((120,), f32),
        ]
    )
    rows, notes = dispatch(
        features,
        next_features,
        destination.reshape(1, tokens),
        terminal.reshape(1, tokens),
        source_ids.reshape(1, tokens),
        subset.T,
        reals.reshape(1, 2 * tokens + 128),
        (target_w1, target_mean, target_scale, target_shift, target_head),
        ny,
        nz,
        nx,
    )
    h, hs = critic_sums(
        rows.reshape(2, shards * cap, width), notes, critic_shift, critic_head, critic_w1, cap
    )
    h = h.reshape(ny, nz, 128, 128)
    hs = hs.reshape(ny, nz, 1, 128)
    full, shift, head, factor = reduce_all(h, hs, ny, nz, nx)
    factor = factor[0, 0]
    step_w1 = full.reshape(critics, hidden, width).astype(f32) * factor
    return (step_w1, shift * factor, head * factor)


def solution(mesh):
    in_specs = (
        P("dp", None),
        P("dp", None),
        P("dp"),
        P("dp"),
        P("dp"),
        P("dp"),
        P(),
        P("dp", None),
        P("dp"),
        P("member", None, None),
        P("member", None),
        P("member", None),
        P("member", None, None),
        P("member", None),
        P("member", None),
        P("member", None),
        P("member", None),
    )
    out_specs = (P("member", None, None), P("member", None), P("member", None))
    return jax.shard_map(
        per_device, mesh=mesh, in_specs=in_specs, out_specs=out_specs, check_vma=False
    )
```

```python
import functools
import math

import jax
import jax.numpy as jnp
from jax import lax
from jax.experimental import pallas as pl
from jax.experimental.pallas import tpu as pltpu
from jax.sharding import PartitionSpec as P

GAMMA = 0.99
ALPHA = 0.2
EPS = 1e-05
NZ = 8
MESH = pl.DeviceIdType.MESH


def far_first(i, nz):
    half = nz // 2
    return half + ((i + 1) // 2) * (2 * ((i + 1) % 2) - 1)


def near_first(i, nz):
    return far_first(nz - 2 - i, nz)


def reduce_kernel(
    ny,
    nz,
    nx,
    h,
    hs,
    full,
    shift_out,
    head_out,
    factor_out,
    small,
    y_in,
    z_out,
    z_in,
    ys_in,
    zs_out,
    zs_in,
    x_out,
    x_in,
    y_sems,
    z_sems,
    gz_sems,
    gy_sems,
    pair_sems,
    ys_sems,
    zs_sems,
    gzs_sems,
    gys_sems,
    pair_small,
    x_sems,
):
    me = lax.axis_index("dp")
    mx = lax.axis_index("member")
    c = lax.rem(me, 2)
    z = lax.rem(me // 2, nz)
    y = me // (2 * nz)
    partner = me + 1 - 2 * c

    def dp_of(yy, zz):
        return (yy * nz + zz) * 2 + c

    def yo(o):
        return lax.rem(y + o, ny)

    def zo(o):
        return lax.rem(z + o, nz)

    def copy(src, dst, sems, index, dp):
        return pltpu.make_async_remote_copy(
            src_ref=src,
            dst_ref=dst,
            send_sem=sems.at[(0,) + index],
            recv_sem=sems.at[(1,) + index],
            device_id={"dp": dp},
            device_id_type=MESH,
        )

    def block_of(yy, zz):
        return full.at[
            c, yy * (nz // 2) + zz // 2, :, pl.ds(pl.multiple_of(lax.rem(zz, 2) * 128, 128), 128)
        ]

    barrier = pltpu.get_barrier_semaphore()
    for o in range(1, ny):
        pl.semaphore_signal(barrier, inc=1, device_id={"dp": dp_of(yo(o), z)}, device_id_type=MESH)
    for o in range(1, nz):
        pl.semaphore_signal(barrier, inc=1, device_id={"dp": dp_of(y, zo(o))}, device_id_type=MESH)
    pl.semaphore_signal(barrier, inc=1, device_id={"dp": partner}, device_id_type=MESH)
    for o in range(1, nx):
        pl.semaphore_signal(
            barrier, inc=1, device_id={"member": lax.rem(mx + o, nx)}, device_id_type=MESH
        )
    pl.semaphore_wait(barrier, ny + nz + nx - 2)

    def y_small(o):
        return copy(hs.at[yo(o)], ys_in.at[o - 1], ys_sems, (o - 1,), dp_of(yo(o), z))

    def y_block(o, oz):
        return copy(
            h.at[yo(o), zo(oz)],
            y_in.at[o - 1, oz],
            y_sems,
            (o - 1, oz),
            dp_of(yo(o), z),
        )

    for o in range(1, ny):
        y_small(o).start()

    def send_y(i, _):
        oz = lax.rem(far_first(i, nz), nz)
        for o in range(1, ny):
            y_block(o, oz).start()
        return 0

    lax.fori_loop(0, nz - 1, send_y, 0)
    for o in range(1, ny):
        y_block(o, 0).start()

    def z_small(o):
        return copy(zs_out.at[zo(o)], zs_in.at[o - 1], zs_sems, (o - 1,), dp_of(y, zo(o)))

    def z_block(o):
        return copy(z_out.at[o], z_in.at[o], z_sems, (o,), dp_of(y, zo(o)))

    for o in range(1, ny):
        y_small(o).wait_recv()
    zs_out[...] = hs[y] + sum(ys_in[o - 1] for o in range(1, ny))
    for o in range(1, nz):
        z_small(o).start()

    def y_sum(oz):
        for o in range(1, ny):
            y_block(o, oz).wait_recv()
        value = h[y, zo(oz)].astype(jnp.float32)
        for o in range(1, ny):
            value = value + y_in[o - 1, oz].astype(jnp.float32)
        z_out[oz] = value

    def send_z(i, _):
        oz = lax.rem(far_first(i, nz), nz)
        y_sum(oz)
        z_block(oz).start()
        return 0

    lax.fori_loop(0, nz - 1, send_z, 0)
    y_sum(0)

    for o in range(1, nz):
        z_small(o).wait_recv()
    mine_small = zs_out[z] + sum(zs_in[o - 1] for o in range(1, nz))

    def add_z(i, value):
        oz = near_first(i, nz)
        z_block(oz).wait_recv()
        return value + z_in[oz]

    z_out[0] = lax.fori_loop(0, nz - 1, add_z, z_out[0])
    mine = z_out[0]
    squares = jnp.sum(mine * mine) + jnp.sum(mine_small * mine_small)
    small[c, y, z, :, 0:128] = mine_small
    small[c, y, z, :, 128:256] = jnp.full((1, 128), squares, jnp.float32)
    block_of(y, z)[...] = mine.T.astype(jnp.bfloat16)

    def gz_small(o):
        ref = small.at[c, y, z]
        return copy(ref, ref, gzs_sems, (o - 1,), dp_of(y, zo(o)))

    def gz_block(o):
        ref = block_of(y, z)
        return copy(ref, ref, gz_sems, (o,), dp_of(y, zo(o)))

    def gy_small(o):
        ref = small.at[c, y]
        return copy(ref, ref, gys_sems, (o - 1,), dp_of(yo(o), z))

    def gy_block(o, oz):
        ref = block_of(y, zo(nz - oz))
        return copy(ref, ref, gy_sems, (o - 1, oz), dp_of(yo(o), z))

    def pair_block(oy, oz):
        ref = block_of(yo(ny - oy), zo(nz - oz))
        return copy(ref, ref, pair_sems, (oy, oz), partner)

    for o in range(1, nz):
        gz_small(o).start()

    def send_gz(i, _):
        gz_block(near_first(i, nz)).start()
        return 0

    lax.fori_loop(0, nz - 1, send_gz, 0)
    for o in range(1, ny):
        gy_block(o, 0).start()
    pair_block(0, 0).start()

    for o in range(1, nz):
        gz_small(o).wait_recv()
    for o in range(1, ny):
        gy_small(o).start()

    def relay_z(i, _):
        oz = near_first(i, nz)
        gz_block(oz).wait_recv()
        for o in range(1, ny):
            gy_block(o, oz).start()
        pair_block(0, oz).start()
        return 0

    lax.fori_loop(0, nz - 1, relay_z, 0)

    for o in range(1, ny):
        gy_small(o).wait_recv()
    pair_s = copy(small.at[c], small.at[c], pair_small, (0,), partner)
    pair_s.start()

    def relay_y(i, _):
        oz = lax.rem(near_first(lax.rem(i + nz - 2, nz - 1), nz) * lax.min(i, 1), nz)
        for o in range(1, ny):
            gy_block(o, oz).wait_recv()
            pair_block(o, oz).start()
        return 0

    half = nz // 2
    lax.fori_loop(0, half, relay_y, 0)
    pair_s.wait_recv()
    x_out[...] = jnp.sum(small[:, :, :, :, 128:256], axis=(0, 1, 2))

    def x_copy(o):
        return pltpu.make_async_remote_copy(
            src_ref=x_out,
            dst_ref=x_in.at[o - 1],
            send_sem=x_sems.at[0, o - 1],
            recv_sem=x_sems.at[1, o - 1],
            device_id={"member": lax.rem(mx + o, nx)},
            device_id_type=MESH,
        )

    for o in range(1, nx):
        x_copy(o).start()
    lax.fori_loop(half, nz, relay_y, 0)
    for o in range(1, nx):
        x_copy(o).wait_recv()
    total = x_out[...] + sum(x_in[o - 1] for o in range(1, nx))
    root = math.sqrt(2 * nx * (ny * nz // 2 * 128) * 258)
    factor_out[...] = root / jnp.maximum(jnp.sqrt(total), root)
    for k in range(2):
        for b in range(ny * nz // 2):
            cut = slice(b * 128, (b + 1) * 128)
            at = b // (nz // 2), 2 * (b % (nz // 2))
            shift_out[k : k + 1, cut] = small[k, at[0], at[1], :, 0:128]
            head_out[k : k + 1, cut] = small[k, at[0], at[1] + 1, :, 0:128]

    def wait_pair(i, _):
        for o in range(ny):
            pair_block(o, i).wait_recv()
        return 0

    lax.fori_loop(0, nz, wait_pair, 0)

    def drain_y(i, _):
        for o in range(1, ny):
            y_block(o, i).wait_send()
            gy_block(o, i).wait_send()
        for o in range(ny):
            pair_block(o, i).wait_send()
        return 0

    lax.fori_loop(0, nz, drain_y, 0)

    def drain_z(i, _):
        z_block(i).wait_send()
        gz_block(i).wait_send()
        return 0

    lax.fori_loop(1, nz, drain_z, 0)
    for o in range(1, ny):
        y_small(o).wait_send()
        gy_small(o).wait_send()
    for o in range(1, nz):
        z_small(o).wait_send()
        gz_small(o).wait_send()
    for o in range(1, nx):
        x_copy(o).wait_send()
    pair_s.wait_send()


def reduce_all(h, hs, ny, nz, nx):
    rows, width = h.shape[2:]
    f32, bf16 = jnp.float32, jnp.bfloat16
    vmem = pl.BlockSpec(memory_space=pltpu.VMEM)
    dma = pltpu.SemaphoreType.DMA
    return pl.pallas_call(
        functools.partial(reduce_kernel, ny, nz, nx),
        out_shape=(
            pltpu.VMEM((2, ny * nz // 2, 128, 256), bf16),
            pltpu.VMEM((2, ny * nz // 2 * 128), f32),
            pltpu.VMEM((2, ny * nz // 2 * 128), f32),
            pltpu.VMEM((1, 128), f32),
        ),
        in_specs=[vmem] * 2,
        out_specs=[vmem] * 4,
        scratch_shapes=[
            pltpu.VMEM((2, ny, nz, 1, 256), f32),
            pltpu.VMEM((ny - 1, nz, rows, width), bf16),
            pltpu.VMEM((nz, rows, width), f32),
            pltpu.VMEM((nz, rows, width), f32),
            pltpu.VMEM((ny - 1, nz, 1, 128), f32),
            pltpu.VMEM((nz, 1, 128), f32),
            pltpu.VMEM((nz - 1, 1, 128), f32),
            pltpu.VMEM((1, 128), f32),
            pltpu.VMEM((nx - 1, 1, 128), f32),
            dma((2, ny - 1, nz)),
            dma((2, nz)),
            dma((2, nz)),
            dma((2, ny - 1, nz)),
            dma((2, ny, nz)),
            dma((2, ny - 1)),
            dma((2, nz - 1)),
            dma((2, nz - 1)),
            dma((2, ny - 1)),
            dma((2, 1)),
            dma((2, nx - 1)),
        ],
        compiler_params=pltpu.CompilerParams(
            collective_id=0, has_side_effects=True, vmem_limit_bytes=44 * 2**20
        ),
        cost_estimate=pl.CostEstimate(flops=10**7, bytes_accessed=4 * 10**6, transcendentals=0),
        name="gradient_sum",
    )(h, hs)


def dot_nt(a, b):
    return lax.dot_general(a, b, (((1,), (1,)), ((), ())), preferred_element_type=jnp.float32)


def dot_nn(a, b):
    return lax.dot_general(a, b, (((1,), (0,)), ((), ())), preferred_element_type=jnp.float32)


def dot_tn(a, b):
    return lax.dot_general(a, b, (((0,), (0,)), ((), ())), preferred_element_type=jnp.float32)


def iota(shape, axis):
    return lax.broadcasted_iota(jnp.int32, shape, axis)


def ones_where(mask):
    return jnp.where(mask, 1.0, 0.0).astype(jnp.bfloat16)


def dispatch_kernel(
    ny,
    nz,
    nx,
    cap,
    features,
    next_features,
    dest_ref,
    terminal,
    source_ids,
    subset,
    rewards,
    next_logp,
    source_weight,
    critic_shift,
    critic_head,
    target_mean,
    target_scale,
    target_shift,
    target_head,
    w_hbm,
    critic_hbm,
    rows,
    notes,
    shift_out,
    head_out,
    critic_out,
    target_w1,
    critic_w1,
    sent,
    sent_notes,
    q_all,
    acc,
    w_sem,
    critic_sem,
    row_send,
    row_recv,
    note_sems,
    x_sems,
    pair_sems,
    pair_note,
    q_sems,
):
    f32, bf16 = jnp.float32, jnp.bfloat16
    shards = 2 * ny * nz
    flat = 2 * ny
    kept = cap // 2
    tokens, width = features.shape
    me = lax.axis_index("dp")
    mx = lax.axis_index("member")
    c = lax.rem(me, 2)
    z = lax.rem(me // 2, nz)
    y = me // (2 * nz)
    partner = me + 1 - 2 * c
    hh = lax.rem(mx, 2)
    neighbor = mx + 1 - 2 * hh
    fetch = pltpu.make_async_copy(w_hbm, target_w1, w_sem)
    fetch.start()
    fetch_critic = pltpu.make_async_copy(critic_hbm.at[c], critic_w1, critic_sem)
    fetch_critic.start()

    def as_row(ref):
        wide = ref[...].astype(f32)
        return jnp.concatenate([wide[i : i + 1] for i in range(wide.shape[0])], axis=1)

    def remote(src, dst, send, recv, device):
        return pltpu.make_async_remote_copy(
            src_ref=src, dst_ref=dst, send_sem=send, recv_sem=recv, device_id=device, device_id_type=MESH
        )

    def zo(o):
        return lax.rem(z + nz + o, nz)

    def group(oz, skip, act):
        for j in range(flat):
            oy, oc = j // 2, j % 2
            if skip and j == 0:
                continue
            yy = lax.rem(y + oy, ny)
            cc = lax.rem(c + oc, 2)
            zz = zo(oz)
            act(oz, (yy * nz + zz) * 2 + cc, zz * flat + yy * 2 + cc, cc)

    def each(act):
        def step(i, _):
            group(far_first(i, nz), False, act)
            return 0

        lax.fori_loop(0, nz - 1, step, 0)
        group(0, True, act)

    barrier = pltpu.get_barrier_semaphore()

    def greet(oz, to, place, cc):
        pl.semaphore_signal(barrier, inc=1, device_id={"dp": to}, device_id_type=MESH)

    each(greet)
    for o in range(1, nx):
        pl.semaphore_signal(
            barrier, inc=1, device_id={"member": lax.rem(mx + o, nx)}, device_id_type=MESH
        )

    dest = dest_ref[...]
    dest = ((dest >> 1) & (nz - 1)) * flat + (dest // (2 * nz)) * 2 + (dest & 1)
    to_shard = dest == iota((shards, tokens), 0)
    chosen = ones_where(to_shard)
    before = ones_where(iota((tokens, tokens), 0) < iota((tokens, tokens), 1))
    rank = jnp.sum(jnp.where(to_shard, dot_nn(chosen, before), 0.0), axis=0, keepdims=True)
    rank = rank.astype(jnp.int32)
    low = rank - hh * kept
    slot = jnp.where((low >= 0) & (low < kept), dest * kept + low, -1)
    chunk = min(256, shards * kept)
    per = chunk // kept
    for i in range(shards // per):
        pick = ones_where(iota((chunk, tokens), 0) + i * chunk == slot)
        block = dot_nn(pick, features[...]).astype(bf16)
        sent[i * per : (i + 1) * per] = block.reshape(per, kept, width)

    pl.semaphore_wait(barrier, shards + nx - 2)

    def send_rows(oz, to, place, cc):
        remote(
            sent.at[place],
            rows.at[cc, hh, z, y * 2 + c],
            row_send,
            row_recv.at[lax.rem(oz, nz)],
            {"dp": to},
        ).start()

    each(send_rows)
    rows[c, hh, z, y * 2 + c] = sent[z * flat + y * 2 + c]

    weight = jnp.zeros((1, tokens), f32)
    weights = source_weight[...].astype(f32)
    for k in range(weights.shape[1]):
        weight = jnp.where(source_ids[...] == k, weights[:, k : k + 1], weight)

    hidden = target_w1.shape[1]
    wide = min(256, hidden)
    tall = min(128, tokens)
    acc[...] = jnp.zeros(acc.shape, f32)
    fetch.wait()
    for k in range(2):

        def block(i, _, k=k):
            units = pl.ds(pl.multiple_of(i * wide, wide), wide)
            scale = target_scale[k : k + 1, units]
            shift = target_shift[k : k + 1, units] - target_mean[k : k + 1, units] * scale
            head = target_head[k : k + 1, units]
            w = target_w1[k, units, :]
            for t in range(tokens // tall):
                pre = dot_nt(next_features[t * tall : (t + 1) * tall, :], w)
                term = jnp.maximum(pre * scale + shift, 0.0) * head
                total = term[:, 0:128]
                for part in range(1, wide // 128):
                    total = total + term[:, part * 128 : (part + 1) * 128]
                acc[k, t * tall : (t + 1) * tall, :] += total
            return 0

        lax.fori_loop(0, hidden // wide, block, 0)
        q_all[mx, k] = jnp.sum(acc[k].T, axis=0, keepdims=True)

    def q_copy(o):
        ref = q_all.at[mx]
        return remote(ref, ref, q_sems.at[0, o - 1], q_sems.at[1, o - 1], {"member": lax.rem(mx + o, nx)})

    for o in range(1, nx):
        q_copy(o).start()

    half = nz // 2
    arrivals = [0] + [o % nz for k in range(1, half) for o in (k, -k)] + [half]

    def x_copy(o):
        ref = rows.at[c, hh, zo(-o)]
        return remote(ref, ref, x_sems.at[0, o], x_sems.at[1, o], {"member": neighbor})

    def pair_copy(part, o):
        ref = rows.at[c, hh + part - 2 * hh * part, zo(-o)]
        return remote(ref, ref, pair_sems.at[0, part, o], pair_sems.at[1, part, o], {"dp": partner})

    def arrive(o):
        ref = rows.at[c, hh, zo(-o)]
        if o == 0:
            ref = rows.at[c, hh, z, pl.ds(0, flat - 1)]
        remote(ref, ref, row_send, row_recv.at[o], {"dp": partner}).wait_recv()
        x_copy(o).start()
        pair_copy(0, o).start()

    shift_out[...] = critic_shift[pl.ds(c, 1), :]
    head_out[...] = critic_head[pl.ds(c, 1), :]
    fetch_critic.wait()
    critic_out[...] = critic_w1[...].astype(bf16)
    early = nz // 2
    for o in arrivals[:early]:
        arrive(o)

    for o in range(1, nx):
        q_copy(o).wait_recv()
    first = jnp.zeros((1, tokens), f32)
    second = first
    for k in range(2 * nx):
        value = q_all[k // 2, k % 2]
        first = jnp.where(subset[0:1, :] == k, value, first)
        second = jnp.where(subset[1:2, :] == k, value, second)
    lowest = jnp.minimum(first, second)
    carry = 1.0 - terminal[...].astype(f32)
    target = as_row(rewards) + GAMMA * carry * (lowest - ALPHA * as_row(next_logp))

    lane = iota((128, tokens), 0)
    spread = jnp.where(to_shard, target, 0.0).astype(bf16)
    spread_w = jnp.where(to_shard, weight, 0.0).astype(bf16)
    note = dot_nt(spread, ones_where(lane == rank)) + dot_nt(spread_w, ones_where(lane == rank + cap))
    sent_notes[...] = note.reshape(shards, 1, 128)
    mine = z * flat + y * 2 + c

    def send_notes(oz, to, place, cc):
        remote(
            sent_notes.at[place], notes.at[cc, mine], note_sems.at[0], note_sems.at[1], {"dp": to}
        ).start()

    each(send_notes)
    notes[c, mine] = sent_notes[mine]

    for o in arrivals[early:]:
        arrive(o)
    for o in arrivals:
        x_copy(o).wait_recv()
        pair_copy(1, o).start()
    most = notes.at[c, pl.ds(0, shards - 1)]
    all_notes = remote(most, most, note_sems.at[0], note_sems.at[1], {"dp": partner})
    all_notes.wait_recv()
    pair_n = remote(notes.at[c], notes.at[c], pair_note.at[0], pair_note.at[1], {"dp": partner})
    pair_n.start()

    all_notes.wait_send()
    most = sent.at[pl.ds(0, shards - 1)]
    remote(most, most, row_send, row_recv.at[0], {"dp": partner}).wait_send()
    for o in range(1, nx):
        q_copy(o).wait_send()
    for o in arrivals:
        x_copy(o).wait_send()
        pair_copy(0, o).wait()
        pair_copy(1, o).wait()
    pair_n.wait()


def dispatch(features, next_features, small, targets, critics, ny, nz, nx):
    tokens, width = features.shape
    shards = 2 * ny * nz
    cap = 2 * tokens // shards
    f32, bf16 = jnp.float32, jnp.bfloat16
    vmem = pl.BlockSpec(memory_space=pltpu.VMEM)
    dma = pltpu.SemaphoreType.DMA
    w1 = targets[0]
    return pl.pallas_call(
        functools.partial(dispatch_kernel, ny, nz, nx, cap),
        out_shape=(
            pltpu.VMEM((2, 2, nz, 2 * ny, cap // 2, width), bf16),
            pltpu.VMEM((2, shards, 1, 128), f32),
            pltpu.VMEM((1, w1.shape[1]), f32),
            pltpu.VMEM((1, w1.shape[1]), f32),
            pltpu.VMEM(w1.shape[1:], bf16),
        ),
        in_specs=[vmem] * 15 + [pl.BlockSpec(memory_space=pltpu.HBM)] * 2,
        out_specs=[vmem] * 5,
        scratch_shapes=[
            pltpu.VMEM(w1.shape, w1.dtype),
            pltpu.VMEM(w1.shape[1:], f32),
            pltpu.VMEM((shards, cap // 2, width), bf16),
            pltpu.VMEM((shards, 1, 128), f32),
            pltpu.VMEM((nx, 2, 1, tokens), f32),
            pltpu.VMEM((2, tokens, 128), f32),
            dma,
            dma,
            dma,
            dma((nz,)),
            dma((2,)),
            dma((2, nz)),
            dma((2, 2, nz)),
            dma((2,)),
            dma((2, nx - 1)),
        ],
        compiler_params=pltpu.CompilerParams(
            collective_id=1, has_side_effects=True, vmem_limit_bytes=56 * 2**20
        ),
        cost_estimate=pl.CostEstimate(flops=10**9, bytes_accessed=4 * 10**6, transcendentals=0),
        name="dispatch",
    )(features, next_features, *small, *critics[1:], *targets[1:], w1, critics[0])


def critic_kernel(
    cap,
    tile,
    rows,
    notes,
    shift_ref,
    head_ref,
    w,
    h,
    hs,
    xc,
    targets,
    weights,
    zbuf,
    gbuf,
    gz,
    gt,
    sq,
    s0,
    s1,
):
    f32, bf16 = jnp.float32, jnp.bfloat16
    slots, width = rows.shape[1:]
    hidden = w.shape[0]
    shards = slots // cap
    pieces = slots // 128
    few, many = 3, 6
    wide = min(256, hidden)
    lanes = hidden // 128
    shift = shift_ref[...]
    head = head_ref[...]

    kept, part = cap // 2, slots // 2
    at_slot = iota((1, slots), 1)
    owner = ones_where(lax.rem(at_slot, part) // kept == iota((shards, slots), 0))
    my_slot = at_slot // part * kept + lax.rem(at_slot, kept) == iota((cap, slots), 0)
    upto = ones_where(iota((128, 128), 0) <= iota((128, 128), 1))
    counts = []
    for s in range(2):
        by_slot = notes[s, :, 0, :].T[0 : 2 * cap].astype(bf16)
        spread = dot_nn(by_slot, owner)
        y_row = jnp.sum(jnp.where(my_slot, spread[0:cap], 0.0), axis=0, keepdims=True)
        w_row = jnp.sum(jnp.where(my_slot, spread[cap : 2 * cap], 0.0), axis=0, keepdims=True)
        alive = jnp.where(w_row > 0, 1.0, 0.0)
        stacked = jnp.concatenate(
            [alive[:, p * 128 : (p + 1) * 128] for p in range(pieces)]
            + [jnp.zeros((8, 128), f32)] * (1 if pieces < 8 else 0),
            axis=0,
        )
        running = dot_nn(stacked.astype(bf16), upto)
        place = []
        start = jnp.zeros((1, 1), f32)
        for p in range(pieces):
            position = running[p : p + 1] - 1.0 + start
            position = jnp.where(stacked[p : p + 1] > 0, position, -1.0)
            place.append(position.astype(jnp.int32))
            start = start + running[p : p + 1, 127:128]
        number = jnp.sum(alive)
        counts.append(number)
        y_wide = jnp.broadcast_to(y_row, (128, slots)).astype(bf16)
        w_wide_row = jnp.broadcast_to(w_row, (128, slots)).astype(bf16)
        trips = jnp.where(number <= few * tile, few, many)

        def compact(i, _, s=s, place=place, y_wide=y_wide, w_wide_row=w_wide_row):
            at = pl.ds(pl.multiple_of(i * tile, tile), tile)
            row = iota((tile, 128), 0) + i * tile
            pick = jnp.concatenate([ones_where(row == p) for p in place], axis=1)
            xc[s, at, :] = dot_nn(pick, rows[s]).astype(bf16)
            targets[s, at, :] = dot_nt(pick, y_wide)
            weights[s, at, :] = dot_nt(pick, w_wide_row)
            return 0

        lax.fori_loop(0, trips, compact, 0)

    total0 = jnp.zeros((1, hidden), f32)
    total1 = jnp.zeros((1, hidden), f32)
    groups = tile // 8
    for s in range(2):
        number = counts[s]
        whole = jnp.full((1, 1), number, f32)
        trips = jnp.where(number <= few * tile, few, many)
        middle = jnp.sum(rows[s].astype(f32), axis=0, keepdims=True) / whole
        one = middle.astype(bf16)
        rest = middle - one.astype(f32)
        two = rest.astype(bf16)
        three = (rest - two.astype(f32)).astype(bf16)
        parts = jnp.concatenate(
            [one.astype(f32), two.astype(f32), three.astype(f32), jnp.zeros((13, width), f32)], axis=0
        ).astype(bf16)
        mu = jnp.sum(dot_nt(parts, w[...]), axis=0, keepdims=True)
        sq[...] = jnp.zeros(sq.shape, f32)
        s0[...] = jnp.zeros(s0.shape, f32)
        s1[...] = jnp.zeros(s1.shape, f32)

        def forward(i, _, s=s, mu=mu, number=number):
            at = pl.ds(pl.multiple_of(i * tile, tile), tile)
            row = iota((tile, 128), 0) + i * tile
            alive = jnp.where(row < number.astype(jnp.int32), 1.0, 0.0)
            x = xc[s, at, :]
            for j in range(hidden // wide):
                pre = dot_nt(x, w[j * wide : (j + 1) * wide, :])
                for k in range(wide // 128):
                    lo = j * wide + k * 128
                    zc = (pre[:, k * 128 : (k + 1) * 128] - mu[:, lo : lo + 128]) * alive
                    zbuf[at, lo : lo + 128] = zc
                    sq[:, lo : lo + 128] += jnp.sum((zc * zc).reshape(groups, 8, 128), axis=0)
            return 0

        lax.fori_loop(0, trips, forward, 0)
        var = jnp.sum(sq[...], axis=0, keepdims=True) / whole
        inv = 1.0 / jnp.sqrt(var + EPS)

        def slopes(i, _, s=s, inv=inv):
            at = pl.ds(pl.multiple_of(i * tile, tile), tile)
            acc = jnp.zeros((tile, 128), f32)
            for j in range(lanes):
                cut = slice(j * 128, (j + 1) * 128)
                zh = zbuf[at, cut] * inv[:, cut]
                zbuf[at, cut] = zh
                acc = acc + jnp.maximum(zh + shift[:, cut], 0.0) * head[:, cut]
            q = jnp.sum(acc, axis=1, keepdims=True)
            dq = weights[s, at, :] * (q - targets[s, at, :])
            for j in range(lanes):
                cut = slice(j * 128, (j + 1) * 128)
                zh = zbuf[at, cut]
                g = jnp.where(zh > -shift[:, cut], dq, 0.0)
                gbuf[at, cut] = g
                s0[:, cut] += jnp.sum(g.reshape(groups, 8, 128), axis=0)
                s1[:, cut] += jnp.sum((g * zh).reshape(groups, 8, 128), axis=0)
            return 0

        lax.fori_loop(0, trips, slopes, 0)
        sum0 = jnp.sum(s0[...], axis=0, keepdims=True)
        sum1 = jnp.sum(s1[...], axis=0, keepdims=True)
        total0 = total0 + sum0
        total1 = total1 + sum1
        scale = inv * head
        base = -scale * (sum0 / whole)
        tilt = -scale * (sum1 / whole)

        def backward(i, _, scale=scale, base=base, tilt=tilt):
            at = pl.ds(pl.multiple_of(i * tile, tile), tile)
            for j in range(lanes):
                cut = slice(j * 128, (j + 1) * 128)
                value = gbuf[at, cut] * scale[:, cut] + (zbuf[at, cut] * tilt[:, cut] + base[:, cut])
                gz[at, cut] = value.astype(bf16)
            return 0

        lax.fori_loop(0, trips, backward, 0)

        def product(depth, s=s):
            x = xc[s, 0:depth, :]
            for j in range(hidden // wide):
                cut = slice(j * wide, (j + 1) * wide)
                out = dot_tn(x, gz[0:depth, cut])
                gt[:, cut] = out if s == 0 else gt[:, cut] + out

        @pl.when(trips == few)
        def _():
            product(few * tile)

        @pl.when(trips != few)
        def _():
            product(many * tile)

    g_shift = head * total0
    g_head = shift * total0 + total1
    for u in range(lanes):
        cut = slice(u * 128, (u + 1) * 128)
        h[2 * u] = gt[0:128, cut].astype(bf16)
        h[2 * u + 1] = gt[128:256, cut].astype(bf16)
        hs[2 * u] = g_shift[:, cut]
        hs[2 * u + 1] = g_head[:, cut]


def critic_sums(rows, notes, shift, head, w1, cap):
    f32, bf16 = jnp.float32, jnp.bfloat16
    slots, width = rows.shape[1:]
    hidden = w1.shape[0]
    tile = slots * 3 // 16
    tall = 6 * tile
    vmem = pl.BlockSpec(memory_space=pltpu.VMEM)
    blocks = hidden // 128 * (width // 128)
    return pl.pallas_call(
        functools.partial(critic_kernel, cap, tile),
        out_shape=(
            pltpu.VMEM((blocks, 128, 128), bf16),
            pltpu.VMEM((blocks, 1, 128), f32),
        ),
        in_specs=[vmem] * 5,
        out_specs=[vmem] * 2,
        scratch_shapes=[
            pltpu.VMEM((2, tall, width), bf16),
            pltpu.VMEM((2, tall, 128), f32),
            pltpu.VMEM((2, tall, 128), f32),
            pltpu.VMEM((tall, hidden), f32),
            pltpu.VMEM((tall, hidden), f32),
            pltpu.VMEM((tall, hidden), bf16),
            pltpu.VMEM((width, hidden), f32),
            pltpu.VMEM((8, hidden), f32),
            pltpu.VMEM((8, hidden), f32),
            pltpu.VMEM((8, hidden), f32),
        ],
        compiler_params=pltpu.CompilerParams(vmem_limit_bytes=48 * 2**20),
        cost_estimate=pl.CostEstimate(
            flops=8 * slots * hidden * width, bytes_accessed=4 * 10**6, transcendentals=0
        ),
        name="critic_sums",
    )(rows, notes, shift, head, w1)


def per_device(
    features,
    next_features,
    rewards,
    next_logp,
    terminal,
    source_ids,
    source_weight,
    subset,
    destination,
    critic_w1,
    critic_shift,
    critic_head,
    target_w1,
    target_mean,
    target_scale,
    target_shift,
    target_head,
):
    f32 = jnp.float32
    shards = lax.axis_size("dp")
    nx = lax.axis_size("member")
    nz = NZ
    ny = shards // (2 * nz)
    tokens, width = features.shape
    critics, hidden = critic_w1.shape[:2]
    cap = 2 * tokens // shards
    rows, notes, shift, head, w1 = dispatch(
        features,
        next_features,
        (
            destination.reshape(1, tokens),
            terminal.reshape(1, tokens),
            source_ids.reshape(1, tokens),
            subset.T,
            rewards.reshape(tokens // 128, 128),
            next_logp.reshape(tokens // 128, 128),
            source_weight.reshape(1, -1),
        ),
        (target_w1, target_mean, target_scale, target_shift, target_head),
        (critic_w1, critic_shift, critic_head),
        ny,
        nz,
        nx,
    )
    h, hs = critic_sums(rows.reshape(2, shards * cap, width), notes, shift, head, w1, cap)
    h = h.reshape(ny, nz, 128, 128)
    hs = hs.reshape(ny, nz, 1, 128)
    full, shift, head, factor = reduce_all(h, hs, ny, nz, nx)
    factor = factor[0, 0]
    step_w1 = full.reshape(critics, hidden, width).astype(f32) * factor
    return (step_w1, shift * factor, head * factor)


def solution(mesh):
    in_specs = (
        P("dp", None),
        P("dp", None),
        P("dp"),
        P("dp"),
        P("dp"),
        P("dp"),
        P(),
        P("dp", None),
        P("dp"),
        P("member", None, None),
        P("member", None),
        P("member", None),
        P("member", None, None),
        P("member", None),
        P("member", None),
        P("member", None),
        P("member", None),
    )
    out_specs = (P("member", None, None), P("member", None), P("member", None))
    return jax.shard_map(
        per_device, mesh=mesh, in_specs=in_specs, out_specs=out_specs, check_vma=False
    )
```

```python
import functools
import math

import jax
import jax.numpy as jnp
from jax import lax
from jax.experimental import pallas as pl
from jax.experimental.pallas import tpu as pltpu
from jax.sharding import PartitionSpec as P

GAMMA = 0.99
ALPHA = 0.2
EPS = 1e-05
NZ = 8
MESH = pl.DeviceIdType.MESH


def far_first(i, nz):
    half = nz // 2
    return half + ((i + 1) // 2) * (2 * ((i + 1) % 2) - 1)


def near_first(i, nz):
    return far_first(nz - 2 - i, nz)


def reduce_kernel(
    ny,
    nz,
    nx,
    h,
    hs,
    full,
    shift_out,
    head_out,
    factor_out,
    small,
    y_in,
    z_out,
    z_in,
    ys_in,
    zs_out,
    zs_in,
    x_out,
    x_in,
    y_sems,
    z_sems,
    gz_sems,
    gy_sems,
    pair_sems,
    ys_sems,
    zs_sems,
    gzs_sems,
    gys_sems,
    pair_small,
    x_sems,
):
    me = lax.axis_index("dp")
    mx = lax.axis_index("member")
    c = lax.rem(me, 2)
    z = lax.rem(me // 2, nz)
    y = me // (2 * nz)
    partner = me + 1 - 2 * c

    def dp_of(yy, zz):
        return (yy * nz + zz) * 2 + c

    def yo(o):
        return lax.rem(y + o, ny)

    def zo(o):
        return lax.rem(z + o, nz)

    def copy(src, dst, sems, index, dp):
        return pltpu.make_async_remote_copy(
            src_ref=src,
            dst_ref=dst,
            send_sem=sems.at[(0,) + index],
            recv_sem=sems.at[(1,) + index],
            device_id={"dp": dp},
            device_id_type=MESH,
        )

    def block_of(yy, zz):
        return full.at[
            c, yy * (nz // 2) + zz // 2, :, pl.ds(pl.multiple_of(lax.rem(zz, 2) * 128, 128), 128)
        ]

    barrier = pltpu.get_barrier_semaphore()
    for o in range(1, ny):
        pl.semaphore_signal(barrier, inc=1, device_id={"dp": dp_of(yo(o), z)}, device_id_type=MESH)
    for o in range(1, nz):
        pl.semaphore_signal(barrier, inc=1, device_id={"dp": dp_of(y, zo(o))}, device_id_type=MESH)
    pl.semaphore_signal(barrier, inc=1, device_id={"dp": partner}, device_id_type=MESH)
    for o in range(1, nx):
        pl.semaphore_signal(
            barrier, inc=1, device_id={"member": lax.rem(mx + o, nx)}, device_id_type=MESH
        )
    pl.semaphore_wait(barrier, ny + nz + nx - 2)

    def y_small(o):
        return copy(hs.at[yo(o)], ys_in.at[o - 1], ys_sems, (o - 1,), dp_of(yo(o), z))

    def y_block(o, oz):
        return copy(
            h.at[yo(o), zo(oz)],
            y_in.at[o - 1, oz],
            y_sems,
            (o - 1, oz),
            dp_of(yo(o), z),
        )

    for o in range(1, ny):
        y_small(o).start()

    def send_y(i, _):
        oz = lax.rem(far_first(i, nz), nz)
        for o in range(1, ny):
            y_block(o, oz).start()
        return 0

    lax.fori_loop(0, nz - 1, send_y, 0)
    for o in range(1, ny):
        y_block(o, 0).start()

    def z_small(o):
        return copy(zs_out.at[zo(o)], zs_in.at[o - 1], zs_sems, (o - 1,), dp_of(y, zo(o)))

    def z_block(o):
        return copy(z_out.at[o], z_in.at[o], z_sems, (o,), dp_of(y, zo(o)))

    for o in range(1, ny):
        y_small(o).wait_recv()
    zs_out[...] = hs[y] + sum(ys_in[o - 1] for o in range(1, ny))
    for o in range(1, nz):
        z_small(o).start()

    def y_sum(oz):
        for o in range(1, ny):
            y_block(o, oz).wait_recv()
        value = h[y, zo(oz)].astype(jnp.float32)
        for o in range(1, ny):
            value = value + y_in[o - 1, oz].astype(jnp.float32)
        z_out[oz] = value

    def send_z(i, _):
        oz = lax.rem(far_first(i, nz), nz)
        y_sum(oz)
        z_block(oz).start()
        return 0

    lax.fori_loop(0, nz - 1, send_z, 0)
    y_sum(0)

    for o in range(1, nz):
        z_small(o).wait_recv()
    mine_small = zs_out[z] + sum(zs_in[o - 1] for o in range(1, nz))

    def add_z(i, value):
        oz = near_first(i, nz)
        z_block(oz).wait_recv()
        return value + z_in[oz]

    z_out[0] = lax.fori_loop(0, nz - 1, add_z, z_out[0])
    mine = z_out[0]
    squares = jnp.sum(mine * mine) + jnp.sum(mine_small * mine_small)
    small[c, y, z, :, 0:128] = mine_small
    small[c, y, z, :, 128:256] = jnp.full((1, 128), squares, jnp.float32)
    block_of(y, z)[...] = mine.T.astype(jnp.bfloat16)

    def gz_small(o):
        ref = small.at[c, y, z]
        return copy(ref, ref, gzs_sems, (o - 1,), dp_of(y, zo(o)))

    def gz_block(o):
        ref = block_of(y, z)
        return copy(ref, ref, gz_sems, (o,), dp_of(y, zo(o)))

    def gy_small(o):
        ref = small.at[c, y]
        return copy(ref, ref, gys_sems, (o - 1,), dp_of(yo(o), z))

    def gy_block(o, oz):
        ref = block_of(y, zo(nz - oz))
        return copy(ref, ref, gy_sems, (o - 1, oz), dp_of(yo(o), z))

    def pair_block(oy, oz):
        ref = block_of(yo(ny - oy), zo(nz - oz))
        return copy(ref, ref, pair_sems, (oy, oz), partner)

    for o in range(1, nz):
        gz_small(o).start()

    def send_gz(i, _):
        gz_block(near_first(i, nz)).start()
        return 0

    lax.fori_loop(0, nz - 1, send_gz, 0)
    for o in range(1, ny):
        gy_block(o, 0).start()
    pair_block(0, 0).start()

    for o in range(1, nz):
        gz_small(o).wait_recv()
    for o in range(1, ny):
        gy_small(o).start()

    def relay_z(i, _):
        oz = near_first(i, nz)
        gz_block(oz).wait_recv()
        for o in range(1, ny):
            gy_block(o, oz).start()
        pair_block(0, oz).start()
        return 0

    lax.fori_loop(0, nz - 1, relay_z, 0)

    for o in range(1, ny):
        gy_small(o).wait_recv()
    pair_s = copy(small.at[c], small.at[c], pair_small, (0,), partner)
    pair_s.start()

    def relay_y(i, _):
        oz = lax.rem(near_first(lax.rem(i + nz - 2, nz - 1), nz) * lax.min(i, 1), nz)
        for o in range(1, ny):
            gy_block(o, oz).wait_recv()
            pair_block(o, oz).start()
        return 0

    half = nz // 2
    lax.fori_loop(0, half, relay_y, 0)
    pair_s.wait_recv()
    x_out[...] = jnp.sum(small[:, :, :, :, 128:256], axis=(0, 1, 2))

    def x_copy(o):
        return pltpu.make_async_remote_copy(
            src_ref=x_out,
            dst_ref=x_in.at[o - 1],
            send_sem=x_sems.at[0, o - 1],
            recv_sem=x_sems.at[1, o - 1],
            device_id={"member": lax.rem(mx + o, nx)},
            device_id_type=MESH,
        )

    for o in range(1, nx):
        x_copy(o).start()
    lax.fori_loop(half, nz, relay_y, 0)
    for o in range(1, nx):
        x_copy(o).wait_recv()
    total = x_out[...] + sum(x_in[o - 1] for o in range(1, nx))
    root = math.sqrt(2 * nx * (ny * nz // 2 * 128) * 258)
    factor_out[...] = root / jnp.maximum(jnp.sqrt(total), root)
    for k in range(2):
        for b in range(ny * nz // 2):
            cut = slice(b * 128, (b + 1) * 128)
            at = b // (nz // 2), 2 * (b % (nz // 2))
            shift_out[k : k + 1, cut] = small[k, at[0], at[1], :, 0:128]
            head_out[k : k + 1, cut] = small[k, at[0], at[1] + 1, :, 0:128]

    def wait_pair(i, _):
        for o in range(ny):
            pair_block(o, i).wait_recv()
        return 0

    lax.fori_loop(0, nz, wait_pair, 0)

    def drain_y(i, _):
        for o in range(1, ny):
            y_block(o, i).wait_send()
            gy_block(o, i).wait_send()
        for o in range(ny):
            pair_block(o, i).wait_send()
        return 0

    lax.fori_loop(0, nz, drain_y, 0)

    def drain_z(i, _):
        z_block(i).wait_send()
        gz_block(i).wait_send()
        return 0

    lax.fori_loop(1, nz, drain_z, 0)
    for o in range(1, ny):
        y_small(o).wait_send()
        gy_small(o).wait_send()
    for o in range(1, nz):
        z_small(o).wait_send()
        gz_small(o).wait_send()
    for o in range(1, nx):
        x_copy(o).wait_send()
    pair_s.wait_send()


def reduce_all(h, hs, ny, nz, nx):
    rows, width = h.shape[2:]
    f32, bf16 = jnp.float32, jnp.bfloat16
    vmem = pl.BlockSpec(memory_space=pltpu.VMEM)
    dma = pltpu.SemaphoreType.DMA
    return pl.pallas_call(
        functools.partial(reduce_kernel, ny, nz, nx),
        out_shape=(
            pltpu.VMEM((2, ny * nz // 2, 128, 256), bf16),
            pltpu.VMEM((2, ny * nz // 2 * 128), f32),
            pltpu.VMEM((2, ny * nz // 2 * 128), f32),
            pltpu.VMEM((1, 128), f32),
        ),
        in_specs=[vmem] * 2,
        out_specs=[vmem] * 4,
        scratch_shapes=[
            pltpu.VMEM((2, ny, nz, 1, 256), f32),
            pltpu.VMEM((ny - 1, nz, rows, width), bf16),
            pltpu.VMEM((nz, rows, width), f32),
            pltpu.VMEM((nz, rows, width), f32),
            pltpu.VMEM((ny - 1, nz, 1, 128), f32),
            pltpu.VMEM((nz, 1, 128), f32),
            pltpu.VMEM((nz - 1, 1, 128), f32),
            pltpu.VMEM((1, 128), f32),
            pltpu.VMEM((nx - 1, 1, 128), f32),
            dma((2, ny - 1, nz)),
            dma((2, nz)),
            dma((2, nz)),
            dma((2, ny - 1, nz)),
            dma((2, ny, nz)),
            dma((2, ny - 1)),
            dma((2, nz - 1)),
            dma((2, nz - 1)),
            dma((2, ny - 1)),
            dma((2, 1)),
            dma((2, nx - 1)),
        ],
        compiler_params=pltpu.CompilerParams(
            collective_id=0, has_side_effects=True, vmem_limit_bytes=44 * 2**20
        ),
        cost_estimate=pl.CostEstimate(flops=10**7, bytes_accessed=4 * 10**6, transcendentals=0),
        name="gradient_sum",
    )(h, hs)


def dot_nt(a, b):
    return lax.dot_general(a, b, (((1,), (1,)), ((), ())), preferred_element_type=jnp.float32)


def dot_nn(a, b):
    return lax.dot_general(a, b, (((1,), (0,)), ((), ())), preferred_element_type=jnp.float32)


def dot_tn(a, b):
    return lax.dot_general(a, b, (((0,), (0,)), ((), ())), preferred_element_type=jnp.float32)


def iota(shape, axis):
    return lax.broadcasted_iota(jnp.int32, shape, axis)


def ones_where(mask):
    return jnp.where(mask, 1.0, 0.0).astype(jnp.bfloat16)


def dispatch_kernel(
    ny,
    nz,
    nx,
    cap,
    features,
    next_features,
    dest_ref,
    terminal,
    source_ids,
    subset,
    rewards,
    next_logp,
    source_weight,
    critic_shift,
    critic_head,
    target_mean,
    target_scale,
    target_shift,
    target_head,
    w_hbm,
    critic_hbm,
    rows,
    notes,
    shift_out,
    head_out,
    critic_out,
    target_w1,
    critic_w1,
    sent,
    sent_notes,
    q_all,
    acc,
    w_sem,
    critic_sem,
    row_send,
    row_recv,
    note_sems,
    x_sems,
    pair_sems,
    pair_note,
    q_sems,
):
    f32, bf16 = jnp.float32, jnp.bfloat16
    shards = 2 * ny * nz
    flat = 2 * ny
    kept = cap // 2
    tokens, width = features.shape
    me = lax.axis_index("dp")
    mx = lax.axis_index("member")
    c = lax.rem(me, 2)
    z = lax.rem(me // 2, nz)
    y = me // (2 * nz)
    partner = me + 1 - 2 * c
    hh = lax.rem(mx, 2)
    neighbor = mx + 1 - 2 * hh
    fetch = pltpu.make_async_copy(w_hbm, target_w1, w_sem)
    fetch.start()
    fetch_critic = pltpu.make_async_copy(critic_hbm.at[c], critic_w1, critic_sem)
    fetch_critic.start()

    def as_row(ref):
        wide = ref[...].astype(f32)
        return jnp.concatenate([wide[i : i + 1] for i in range(wide.shape[0])], axis=1)

    def remote(src, dst, send, recv, device):
        return pltpu.make_async_remote_copy(
            src_ref=src, dst_ref=dst, send_sem=send, recv_sem=recv, device_id=device, device_id_type=MESH
        )

    def zo(o):
        return lax.rem(z + nz + o, nz)

    def group(oz, skip, act):
        for j in range(flat):
            oy, oc = j // 2, j % 2
            if skip and j == 0:
                continue
            yy = lax.rem(y + oy, ny)
            cc = lax.rem(c + oc, 2)
            zz = zo(oz)
            act(oz, (yy * nz + zz) * 2 + cc, zz * flat + yy * 2 + cc, cc)

    def each(act):
        group(0, True, act)

        def step(i, _):
            group(near_first(i, nz), False, act)
            return 0

        lax.fori_loop(0, nz - 1, step, 0)

    barrier = pltpu.get_barrier_semaphore()

    def greet(oz, to, place, cc):
        pl.semaphore_signal(barrier, inc=1, device_id={"dp": to}, device_id_type=MESH)

    each(greet)
    for o in range(1, nx):
        pl.semaphore_signal(
            barrier, inc=1, device_id={"member": lax.rem(mx + o, nx)}, device_id_type=MESH
        )

    dest = dest_ref[...]
    dest = ((dest >> 1) & (nz - 1)) * flat + (dest // (2 * nz)) * 2 + (dest & 1)
    to_shard = dest == iota((shards, tokens), 0)
    chosen = ones_where(to_shard)
    before = ones_where(iota((tokens, tokens), 0) < iota((tokens, tokens), 1))
    rank = jnp.sum(jnp.where(to_shard, dot_nn(chosen, before), 0.0), axis=0, keepdims=True)
    rank = rank.astype(jnp.int32)
    low = rank - hh * kept
    slot = jnp.where((low >= 0) & (low < kept), dest * kept + low, -1)
    chunk = min(256, shards * kept)
    per = chunk // kept
    for i in range(shards // per):
        pick = ones_where(iota((chunk, tokens), 0) + i * chunk == slot)
        block = dot_nn(pick, features[...]).astype(bf16)
        sent[i * per : (i + 1) * per] = block.reshape(per, kept, width)

    pl.semaphore_wait(barrier, shards + nx - 2)

    def send_rows(oz, to, place, cc):
        remote(
            sent.at[place],
            rows.at[cc, hh, z, y * 2 + c],
            row_send,
            row_recv.at[lax.rem(oz, nz)],
            {"dp": to},
        ).start()

    each(send_rows)
    rows[c, hh, z, y * 2 + c] = sent[z * flat + y * 2 + c]

    weight = jnp.zeros((1, tokens), f32)
    weights = source_weight[...].astype(f32)
    for k in range(weights.shape[1]):
        weight = jnp.where(source_ids[...] == k, weights[:, k : k + 1], weight)

    hidden = target_w1.shape[1]
    wide = min(256, hidden)
    tall = min(512, tokens)
    acc[...] = jnp.zeros(acc.shape, f32)
    fetch.wait()
    for k in range(2):

        def block(i, _, k=k):
            units = pl.ds(pl.multiple_of(i * wide, wide), wide)
            scale = target_scale[k : k + 1, units]
            shift = target_shift[k : k + 1, units] - target_mean[k : k + 1, units] * scale
            head = target_head[k : k + 1, units]
            w = target_w1[k, units, :]
            for t in range(tokens // tall):
                pre = dot_nt(next_features[t * tall : (t + 1) * tall, :], w)
                term = jnp.maximum(pre * scale + shift, 0.0) * head
                total = term[:, 0:128]
                for part in range(1, wide // 128):
                    total = total + term[:, part * 128 : (part + 1) * 128]
                acc[k, t * tall : (t + 1) * tall, :] += total
            return 0

        lax.fori_loop(0, hidden // wide, block, 0)
        q_all[mx, k] = jnp.sum(acc[k].T, axis=0, keepdims=True)

    def q_copy(o):
        ref = q_all.at[mx]
        return remote(ref, ref, q_sems.at[0, o - 1], q_sems.at[1, o - 1], {"member": lax.rem(mx + o, nx)})

    for o in range(1, nx):
        q_copy(o).start()

    half = nz // 2
    arrivals = [0] + [o % nz for k in range(1, half) for o in (k, -k)] + [half]

    def x_copy(o):
        ref = rows.at[c, hh, zo(-o)]
        return remote(ref, ref, x_sems.at[0, o], x_sems.at[1, o], {"member": neighbor})

    def pair_copy(part, o):
        ref = rows.at[c, hh + part - 2 * hh * part, zo(-o)]
        return remote(ref, ref, pair_sems.at[0, part, o], pair_sems.at[1, part, o], {"dp": partner})

    def arrive(o):
        ref = rows.at[c, hh, zo(-o)]
        if o == 0:
            ref = rows.at[c, hh, z, pl.ds(0, flat - 1)]
        remote(ref, ref, row_send, row_recv.at[o], {"dp": partner}).wait_recv()
        x_copy(o).start()
        pair_copy(0, o).start()

    shift_out[...] = critic_shift[pl.ds(c, 1), :]
    head_out[...] = critic_head[pl.ds(c, 1), :]
    fetch_critic.wait()
    step = min(256, critic_w1.shape[0])
    for i in range(critic_w1.shape[0] // step):
        cut = slice(i * step, (i + 1) * step)
        critic_out[:, cut] = critic_w1[cut, :].T.astype(bf16)
    early = nz // 2
    for o in arrivals[:early]:
        arrive(o)

    for o in range(1, nx):
        q_copy(o).wait_recv()
    first = jnp.zeros((1, tokens), f32)
    second = first
    for k in range(2 * nx):
        value = q_all[k // 2, k % 2]
        first = jnp.where(subset[0:1, :] == k, value, first)
        second = jnp.where(subset[1:2, :] == k, value, second)
    lowest = jnp.minimum(first, second)
    carry = 1.0 - terminal[...].astype(f32)
    target = as_row(rewards) + GAMMA * carry * (lowest - ALPHA * as_row(next_logp))

    lane = iota((128, tokens), 0)
    spread = jnp.where(to_shard, target, 0.0).astype(bf16)
    spread_w = jnp.where(to_shard, weight, 0.0).astype(bf16)
    note = dot_nt(spread, ones_where(lane == rank)) + dot_nt(spread_w, ones_where(lane == rank + cap))
    sent_notes[...] = note.reshape(shards, 1, 128)
    mine = z * flat + y * 2 + c

    def send_notes(oz, to, place, cc):
        remote(
            sent_notes.at[place], notes.at[cc, mine], note_sems.at[0], note_sems.at[1], {"dp": to}
        ).start()

    each(send_notes)
    notes[c, mine] = sent_notes[mine]

    for o in arrivals[early:]:
        arrive(o)
    for o in arrivals:
        x_copy(o).wait_recv()
        pair_copy(1, o).start()
    most = notes.at[c, pl.ds(0, shards - 1)]
    all_notes = remote(most, most, note_sems.at[0], note_sems.at[1], {"dp": partner})
    all_notes.wait_recv()
    pair_n = remote(notes.at[c], notes.at[c], pair_note.at[0], pair_note.at[1], {"dp": partner})
    pair_n.start()

    all_notes.wait_send()
    most = sent.at[pl.ds(0, shards - 1)]
    remote(most, most, row_send, row_recv.at[0], {"dp": partner}).wait_send()
    for o in range(1, nx):
        q_copy(o).wait_send()
    for o in arrivals:
        x_copy(o).wait_send()
        pair_copy(0, o).wait()
        pair_copy(1, o).wait()
    pair_n.wait()


def dispatch(features, next_features, small, targets, critics, ny, nz, nx):
    tokens, width = features.shape
    shards = 2 * ny * nz
    cap = 2 * tokens // shards
    f32, bf16 = jnp.float32, jnp.bfloat16
    vmem = pl.BlockSpec(memory_space=pltpu.VMEM)
    dma = pltpu.SemaphoreType.DMA
    w1 = targets[0]
    return pl.pallas_call(
        functools.partial(dispatch_kernel, ny, nz, nx, cap),
        out_shape=(
            pltpu.VMEM((2, 2, nz, 2 * ny, cap // 2, width), bf16),
            pltpu.VMEM((2, shards, 1, 128), f32),
            pltpu.VMEM((1, w1.shape[1]), f32),
            pltpu.VMEM((1, w1.shape[1]), f32),
            pltpu.VMEM(w1.shape[:0:-1], bf16),
        ),
        in_specs=[vmem] * 15 + [pl.BlockSpec(memory_space=pltpu.HBM)] * 2,
        out_specs=[vmem] * 5,
        scratch_shapes=[
            pltpu.VMEM(w1.shape, w1.dtype),
            pltpu.VMEM(w1.shape[1:], f32),
            pltpu.VMEM((shards, cap // 2, width), bf16),
            pltpu.VMEM((shards, 1, 128), f32),
            pltpu.VMEM((nx, 2, 1, tokens), f32),
            pltpu.VMEM((2, tokens, 128), f32),
            dma,
            dma,
            dma,
            dma((nz,)),
            dma((2,)),
            dma((2, nz)),
            dma((2, 2, nz)),
            dma((2,)),
            dma((2, nx - 1)),
        ],
        compiler_params=pltpu.CompilerParams(
            collective_id=1, has_side_effects=True, vmem_limit_bytes=56 * 2**20
        ),
        cost_estimate=pl.CostEstimate(flops=10**9, bytes_accessed=4 * 10**6, transcendentals=0),
        name="dispatch",
    )(features, next_features, *small, *critics[1:], *targets[1:], w1, critics[0])


def critic_kernel(
    cap,
    tile,
    rows,
    notes,
    shift_ref,
    head_ref,
    w,
    h,
    hs,
    xc,
    targets,
    weights,
    zbuf,
    gbuf,
    gt,
    sq,
    s0,
    s1,
):
    f32, bf16 = jnp.float32, jnp.bfloat16
    slots, width = rows.shape[1:]
    hidden = w.shape[1]
    shards = slots // cap
    pieces = slots // 128
    few, many = 3, 6
    big = few * tile
    wide = min(256, hidden)
    lanes = hidden // 128
    shift = shift_ref[...]
    head = head_ref[...]

    kept, part = cap // 2, slots // 2
    at_slot = iota((1, slots), 1)
    owner = ones_where(lax.rem(at_slot, part) // kept == iota((shards, slots), 0))
    my_slot = at_slot // part * kept + lax.rem(at_slot, kept) == iota((cap, slots), 0)
    upto = ones_where(iota((128, 128), 0) <= iota((128, 128), 1))
    counts = []
    for s in range(2):
        by_slot = notes[s, :, 0, :].T[0 : 2 * cap].astype(bf16)
        spread = dot_nn(by_slot, owner)
        y_row = jnp.sum(jnp.where(my_slot, spread[0:cap], 0.0), axis=0, keepdims=True)
        w_row = jnp.sum(jnp.where(my_slot, spread[cap : 2 * cap], 0.0), axis=0, keepdims=True)
        alive = jnp.where(w_row > 0, 1.0, 0.0)
        stacked = jnp.concatenate(
            [alive[:, p * 128 : (p + 1) * 128] for p in range(pieces)]
            + [jnp.zeros((8, 128), f32)] * (1 if pieces < 8 else 0),
            axis=0,
        )
        running = dot_nn(stacked.astype(bf16), upto)
        place = []
        start = jnp.zeros((1, 1), f32)
        for p in range(pieces):
            position = running[p : p + 1] - 1.0 + start
            position = jnp.where(stacked[p : p + 1] > 0, position, -1.0)
            place.append(position.astype(jnp.int32))
            start = start + running[p : p + 1, 127:128]
        number = jnp.sum(alive)
        counts.append(number)
        yw = jnp.concatenate(
            [jnp.broadcast_to(y_row, (128, slots)), jnp.broadcast_to(w_row, (128, slots))], axis=0
        ).astype(bf16)
        trips = jnp.where(number <= few * tile, few, many)

        def compact(i, _, s=s, place=place, yw=yw):
            at = pl.ds(pl.multiple_of(i * big, big), big)
            row = iota((big, 128), 0) + i * big
            pick = jnp.concatenate([ones_where(row == p) for p in place], axis=1)
            xc[s, at, :] = dot_nn(pick, rows[s]).astype(bf16)
            both = dot_nt(pick, yw)
            targets[s, at, :] = both[:, 0:128]
            weights[s, at, :] = both[:, 128:256]
            return 0

        lax.fori_loop(0, trips // few, compact, 0)

    total0 = jnp.zeros((1, hidden), f32)
    total1 = jnp.zeros((1, hidden), f32)
    groups = tile // 8
    for s in range(2):
        number = counts[s]
        whole = jnp.full((1, 1), number, f32)
        trips = jnp.where(number <= few * tile, few, many)
        middle = jnp.sum(rows[s].astype(f32), axis=0, keepdims=True) / whole
        one = middle.astype(bf16)
        rest = middle - one.astype(f32)
        two = rest.astype(bf16)
        three = (rest - two.astype(f32)).astype(bf16)
        parts = jnp.concatenate(
            [one.astype(f32), two.astype(f32), three.astype(f32), jnp.zeros((13, width), f32)], axis=0
        ).astype(bf16)
        mu = jnp.sum(dot_nn(parts, w[...]), axis=0, keepdims=True)
        sq[...] = jnp.zeros(sq.shape, f32)
        s0[...] = jnp.zeros(s0.shape, f32)
        s1[...] = jnp.zeros(s1.shape, f32)

        def forward(i, _, s=s, mu=mu, number=number):
            at = pl.ds(pl.multiple_of(i * tile, tile), tile)
            row = iota((tile, 128), 0) + i * tile
            alive = jnp.where(row < number.astype(jnp.int32), 1.0, 0.0)
            x = xc[s, at, :]
            for j in range(hidden // wide):
                pre = dot_nn(x, w[:, j * wide : (j + 1) * wide])
                for k in range(wide // 128):
                    lo = j * wide + k * 128
                    zc = (pre[:, k * 128 : (k + 1) * 128] - mu[:, lo : lo + 128]) * alive
                    zbuf[at, lo : lo + 128] = zc
                    sq[:, lo : lo + 128] += jnp.sum((zc * zc).reshape(groups, 8, 128), axis=0)
            return 0

        lax.fori_loop(0, trips, forward, 0)
        var = jnp.sum(sq[...], axis=0, keepdims=True) / whole
        inv = 1.0 / jnp.sqrt(var + EPS)

        def slopes(i, _, s=s, inv=inv):
            at = pl.ds(pl.multiple_of(i * tile, tile), tile)
            acc = jnp.zeros((tile, 128), f32)
            for j in range(lanes):
                cut = slice(j * 128, (j + 1) * 128)
                zh = zbuf[at, cut] * inv[:, cut]
                zbuf[at, cut] = zh
                acc = acc + jnp.maximum(zh + shift[:, cut], 0.0) * head[:, cut]
            q = jnp.sum(acc, axis=1, keepdims=True)
            dq = weights[s, at, :] * (q - targets[s, at, :])
            for j in range(lanes):
                cut = slice(j * 128, (j + 1) * 128)
                zh = zbuf[at, cut]
                g = jnp.where(zh > -shift[:, cut], dq, 0.0)
                gbuf[at, cut] = g
                s0[:, cut] += jnp.sum(g.reshape(groups, 8, 128), axis=0)
                s1[:, cut] += jnp.sum((g * zh).reshape(groups, 8, 128), axis=0)
            return 0

        lax.fori_loop(0, trips, slopes, 0)
        sum0 = jnp.sum(s0[...], axis=0, keepdims=True)
        sum1 = jnp.sum(s1[...], axis=0, keepdims=True)
        total0 = total0 + sum0
        total1 = total1 + sum1
        scale = inv * head
        base = -scale * (sum0 / whole)
        tilt = -scale * (sum1 / whole)

        def slope_of(at, cut, scale=scale, base=base, tilt=tilt):
            value = gbuf[at, cut] * scale[:, cut] + (zbuf[at, cut] * tilt[:, cut] + base[:, cut])
            return value.astype(bf16)

        @pl.when(trips == few)
        def _(s=s, slope_of=slope_of):
            xt = xc[s, 0:big, :].T
            for j in range(hidden // wide):
                cut = slice(j * wide, (j + 1) * wide)
                out = dot_nn(xt, slope_of(slice(0, big), cut))
                gt[:, cut] = out if s == 0 else gt[:, cut] + out

        @pl.when(trips != few)
        def _(s=s, slope_of=slope_of):
            if s == 0:
                gt[...] = jnp.zeros(gt.shape, f32)

            def step(i, _):
                at = pl.ds(pl.multiple_of(i * tile, tile), tile)
                for j in range(hidden // wide):
                    cut = slice(j * wide, (j + 1) * wide)
                    gt[:, cut] += dot_tn(xc[s, at, :], slope_of(at, cut))
                return 0

            lax.fori_loop(0, many, step, 0)

    g_shift = head * total0
    g_head = shift * total0 + total1
    for u in range(lanes):
        cut = slice(u * 128, (u + 1) * 128)
        h[2 * u] = gt[0:128, cut].astype(bf16)
        h[2 * u + 1] = gt[128:256, cut].astype(bf16)
        hs[2 * u] = g_shift[:, cut]
        hs[2 * u + 1] = g_head[:, cut]


def critic_sums(rows, notes, shift, head, w1, cap):
    f32, bf16 = jnp.float32, jnp.bfloat16
    slots, width = rows.shape[1:]
    hidden = w1.shape[1]
    tile = slots * 3 // 16
    tall = 6 * tile
    vmem = pl.BlockSpec(memory_space=pltpu.VMEM)
    blocks = hidden // 128 * (width // 128)
    return pl.pallas_call(
        functools.partial(critic_kernel, cap, tile),
        out_shape=(
            pltpu.VMEM((blocks, 128, 128), bf16),
            pltpu.VMEM((blocks, 1, 128), f32),
        ),
        in_specs=[vmem] * 5,
        out_specs=[vmem] * 2,
        scratch_shapes=[
            pltpu.VMEM((2, tall, width), bf16),
            pltpu.VMEM((2, tall, 128), f32),
            pltpu.VMEM((2, tall, 128), f32),
            pltpu.VMEM((tall, hidden), f32),
            pltpu.VMEM((tall, hidden), f32),
            pltpu.VMEM((width, hidden), f32),
            pltpu.VMEM((8, hidden), f32),
            pltpu.VMEM((8, hidden), f32),
            pltpu.VMEM((8, hidden), f32),
        ],
        compiler_params=pltpu.CompilerParams(vmem_limit_bytes=48 * 2**20),
        cost_estimate=pl.CostEstimate(
            flops=8 * slots * hidden * width, bytes_accessed=4 * 10**6, transcendentals=0
        ),
        name="critic_sums",
    )(rows, notes, shift, head, w1)


def per_device(
    features,
    next_features,
    rewards,
    next_logp,
    terminal,
    source_ids,
    source_weight,
    subset,
    destination,
    critic_w1,
    critic_shift,
    critic_head,
    target_w1,
    target_mean,
    target_scale,
    target_shift,
    target_head,
):
    f32 = jnp.float32
    shards = lax.axis_size("dp")
    nx = lax.axis_size("member")
    nz = NZ
    ny = shards // (2 * nz)
    tokens, width = features.shape
    critics, hidden = critic_w1.shape[:2]
    cap = 2 * tokens // shards
    rows, notes, shift, head, w1 = dispatch(
        features,
        next_features,
        (
            destination.reshape(1, tokens),
            terminal.reshape(1, tokens),
            source_ids.reshape(1, tokens),
            subset.T,
            rewards.reshape(tokens // 128, 128),
            next_logp.reshape(tokens // 128, 128),
            source_weight.reshape(1, -1),
        ),
        (target_w1, target_mean, target_scale, target_shift, target_head),
        (critic_w1, critic_shift, critic_head),
        ny,
        nz,
        nx,
    )
    h, hs = critic_sums(rows.reshape(2, shards * cap, width), notes, shift, head, w1, cap)
    h = h.reshape(ny, nz, 128, 128)
    hs = hs.reshape(ny, nz, 1, 128)
    full, shift, head, factor = reduce_all(h, hs, ny, nz, nx)
    factor = factor[0, 0]
    step_w1 = full.reshape(critics, hidden, width).astype(f32) * factor
    return (step_w1, shift * factor, head * factor)


def solution(mesh):
    in_specs = (
        P("dp", None),
        P("dp", None),
        P("dp"),
        P("dp"),
        P("dp"),
        P("dp"),
        P(),
        P("dp", None),
        P("dp"),
        P("member", None, None),
        P("member", None),
        P("member", None),
        P("member", None, None),
        P("member", None),
        P("member", None),
        P("member", None),
        P("member", None),
    )
    out_specs = (P("member", None, None), P("member", None), P("member", None))
    return jax.shard_map(
        per_device, mesh=mesh, in_specs=in_specs, out_specs=out_specs, check_vma=False
    )
```

```python
import functools
import math

import jax
import jax.numpy as jnp
from jax import lax
from jax.experimental import pallas as pl
from jax.experimental.pallas import tpu as pltpu
from jax.sharding import PartitionSpec as P

GAMMA = 0.99
ALPHA = 0.2
EPS = 1e-05
NZ = 8
MESH = pl.DeviceIdType.MESH


def far_first(i, nz):
    half = nz // 2
    return half + ((i + 1) // 2) * (2 * ((i + 1) % 2) - 1)


def near_first(i, nz):
    return far_first(nz - 2 - i, nz)


def reduce_kernel(
    ny,
    nz,
    nx,
    h,
    hs,
    full,
    shift_out,
    head_out,
    factor_out,
    small,
    y_in,
    z_out,
    z_in,
    ys_in,
    zs_out,
    zs_in,
    x_out,
    x_in,
    y_sems,
    z_sems,
    gz_sems,
    gy_sems,
    pair_sems,
    ys_sems,
    zs_sems,
    gzs_sems,
    gys_sems,
    pair_small,
    x_sems,
):
    me = lax.axis_index("dp")
    mx = lax.axis_index("member")
    c = lax.rem(me, 2)
    z = lax.rem(me // 2, nz)
    y = me // (2 * nz)
    partner = me + 1 - 2 * c

    def dp_of(yy, zz):
        return (yy * nz + zz) * 2 + c

    def yo(o):
        return lax.rem(y + o, ny)

    def zo(o):
        return lax.rem(z + o, nz)

    def copy(src, dst, sems, index, dp):
        return pltpu.make_async_remote_copy(
            src_ref=src,
            dst_ref=dst,
            send_sem=sems.at[(0,) + index],
            recv_sem=sems.at[(1,) + index],
            device_id={"dp": dp},
            device_id_type=MESH,
        )

    def block_of(yy, zz):
        return full.at[
            c, yy * (nz // 2) + zz // 2, :, pl.ds(pl.multiple_of(lax.rem(zz, 2) * 128, 128), 128)
        ]

    barrier = pltpu.get_barrier_semaphore()
    for o in range(1, ny):
        pl.semaphore_signal(barrier, inc=1, device_id={"dp": dp_of(yo(o), z)}, device_id_type=MESH)
    for o in range(1, nz):
        pl.semaphore_signal(barrier, inc=1, device_id={"dp": dp_of(y, zo(o))}, device_id_type=MESH)
    pl.semaphore_signal(barrier, inc=1, device_id={"dp": partner}, device_id_type=MESH)
    for o in range(1, nx):
        pl.semaphore_signal(
            barrier, inc=1, device_id={"member": lax.rem(mx + o, nx)}, device_id_type=MESH
        )
    pl.semaphore_wait(barrier, ny + nz + nx - 2)

    def y_small(o):
        return copy(hs.at[yo(o)], ys_in.at[o - 1], ys_sems, (o - 1,), dp_of(yo(o), z))

    def y_block(o, oz):
        return copy(
            h.at[yo(o), zo(oz)],
            y_in.at[o - 1, oz],
            y_sems,
            (o - 1, oz),
            dp_of(yo(o), z),
        )

    for o in range(1, ny):
        y_small(o).start()

    def send_y(i, _):
        oz = lax.rem(far_first(i, nz), nz)
        for o in range(1, ny):
            y_block(o, oz).start()
        return 0

    lax.fori_loop(0, nz - 1, send_y, 0)
    for o in range(1, ny):
        y_block(o, 0).start()

    def z_small(o):
        return copy(zs_out.at[zo(o)], zs_in.at[o - 1], zs_sems, (o - 1,), dp_of(y, zo(o)))

    def z_block(o):
        return copy(z_out.at[o], z_in.at[o], z_sems, (o,), dp_of(y, zo(o)))

    for o in range(1, ny):
        y_small(o).wait_recv()
    zs_out[...] = hs[y] + sum(ys_in[o - 1] for o in range(1, ny))
    for o in range(1, nz):
        z_small(o).start()

    def y_sum(oz):
        for o in range(1, ny):
            y_block(o, oz).wait_recv()
        value = h[y, zo(oz)].astype(jnp.float32)
        for o in range(1, ny):
            value = value + y_in[o - 1, oz].astype(jnp.float32)
        z_out[oz] = value

    def send_z(i, _):
        oz = lax.rem(far_first(i, nz), nz)
        y_sum(oz)
        z_block(oz).start()
        return 0

    lax.fori_loop(0, nz - 1, send_z, 0)
    y_sum(0)

    for o in range(1, nz):
        z_small(o).wait_recv()
    mine_small = zs_out[z] + sum(zs_in[o - 1] for o in range(1, nz))

    def add_z(i, value):
        oz = near_first(i, nz)
        z_block(oz).wait_recv()
        return value + z_in[oz]

    z_out[0] = lax.fori_loop(0, nz - 1, add_z, z_out[0])
    mine = z_out[0]
    squares = jnp.sum(mine * mine) + jnp.sum(mine_small * mine_small)
    small[c, y, z, :, 0:128] = mine_small
    small[c, y, z, :, 128:256] = jnp.full((1, 128), squares, jnp.float32)
    block_of(y, z)[...] = mine.T.astype(jnp.bfloat16)

    def gz_small(o):
        ref = small.at[c, y, z]
        return copy(ref, ref, gzs_sems, (o - 1,), dp_of(y, zo(o)))

    def gz_block(o):
        ref = block_of(y, z)
        return copy(ref, ref, gz_sems, (o,), dp_of(y, zo(o)))

    def gy_small(o):
        ref = small.at[c, y]
        return copy(ref, ref, gys_sems, (o - 1,), dp_of(yo(o), z))

    def gy_block(o, oz):
        ref = block_of(y, zo(nz - oz))
        return copy(ref, ref, gy_sems, (o - 1, oz), dp_of(yo(o), z))

    def pair_block(oy, oz):
        ref = block_of(yo(ny - oy), zo(nz - oz))
        return copy(ref, ref, pair_sems, (oy, oz), partner)

    for o in range(1, nz):
        gz_small(o).start()

    def send_gz(i, _):
        gz_block(near_first(i, nz)).start()
        return 0

    lax.fori_loop(0, nz - 1, send_gz, 0)
    for o in range(1, ny):
        gy_block(o, 0).start()
    pair_block(0, 0).start()

    for o in range(1, nz):
        gz_small(o).wait_recv()
    for o in range(1, ny):
        gy_small(o).start()

    def relay_z(i, _):
        oz = near_first(i, nz)
        gz_block(oz).wait_recv()
        for o in range(1, ny):
            gy_block(o, oz).start()
        pair_block(0, oz).start()
        return 0

    lax.fori_loop(0, nz - 1, relay_z, 0)

    for o in range(1, ny):
        gy_small(o).wait_recv()
    pair_s = copy(small.at[c], small.at[c], pair_small, (0,), partner)
    pair_s.start()

    def relay_y(i, _):
        oz = lax.rem(near_first(lax.rem(i + nz - 2, nz - 1), nz) * lax.min(i, 1), nz)
        for o in range(1, ny):
            gy_block(o, oz).wait_recv()
            pair_block(o, oz).start()
        return 0

    half = nz // 2
    lax.fori_loop(0, half, relay_y, 0)
    pair_s.wait_recv()
    x_out[...] = jnp.sum(small[:, :, :, :, 128:256], axis=(0, 1, 2))

    def x_copy(o):
        return pltpu.make_async_remote_copy(
            src_ref=x_out,
            dst_ref=x_in.at[o - 1],
            send_sem=x_sems.at[0, o - 1],
            recv_sem=x_sems.at[1, o - 1],
            device_id={"member": lax.rem(mx + o, nx)},
            device_id_type=MESH,
        )

    for o in range(1, nx):
        x_copy(o).start()
    lax.fori_loop(half, nz, relay_y, 0)
    for o in range(1, nx):
        x_copy(o).wait_recv()
    total = x_out[...] + sum(x_in[o - 1] for o in range(1, nx))
    root = math.sqrt(2 * nx * (ny * nz // 2 * 128) * 258)
    factor_out[...] = root / jnp.maximum(jnp.sqrt(total), root)
    for k in range(2):
        for b in range(ny * nz // 2):
            cut = slice(b * 128, (b + 1) * 128)
            at = b // (nz // 2), 2 * (b % (nz // 2))
            shift_out[k : k + 1, cut] = small[k, at[0], at[1], :, 0:128]
            head_out[k : k + 1, cut] = small[k, at[0], at[1] + 1, :, 0:128]

    def wait_pair(i, _):
        for o in range(ny):
            pair_block(o, i).wait_recv()
        return 0

    lax.fori_loop(0, nz, wait_pair, 0)

    def drain_y(i, _):
        for o in range(1, ny):
            y_block(o, i).wait_send()
            gy_block(o, i).wait_send()
        for o in range(ny):
            pair_block(o, i).wait_send()
        return 0

    lax.fori_loop(0, nz, drain_y, 0)

    def drain_z(i, _):
        z_block(i).wait_send()
        gz_block(i).wait_send()
        return 0

    lax.fori_loop(1, nz, drain_z, 0)
    for o in range(1, ny):
        y_small(o).wait_send()
        gy_small(o).wait_send()
    for o in range(1, nz):
        z_small(o).wait_send()
        gz_small(o).wait_send()
    for o in range(1, nx):
        x_copy(o).wait_send()
    pair_s.wait_send()


def reduce_all(h, hs, ny, nz, nx):
    rows, width = h.shape[2:]
    f32, bf16 = jnp.float32, jnp.bfloat16
    vmem = pl.BlockSpec(memory_space=pltpu.VMEM)
    dma = pltpu.SemaphoreType.DMA
    return pl.pallas_call(
        functools.partial(reduce_kernel, ny, nz, nx),
        out_shape=(
            pltpu.VMEM((2, ny * nz // 2, 128, 256), bf16),
            pltpu.VMEM((2, ny * nz // 2 * 128), f32),
            pltpu.VMEM((2, ny * nz // 2 * 128), f32),
            pltpu.VMEM((1, 128), f32),
        ),
        in_specs=[vmem] * 2,
        out_specs=[vmem] * 4,
        scratch_shapes=[
            pltpu.VMEM((2, ny, nz, 1, 256), f32),
            pltpu.VMEM((ny - 1, nz, rows, width), bf16),
            pltpu.VMEM((nz, rows, width), f32),
            pltpu.VMEM((nz, rows, width), f32),
            pltpu.VMEM((ny - 1, nz, 1, 128), f32),
            pltpu.VMEM((nz, 1, 128), f32),
            pltpu.VMEM((nz - 1, 1, 128), f32),
            pltpu.VMEM((1, 128), f32),
            pltpu.VMEM((nx - 1, 1, 128), f32),
            dma((2, ny - 1, nz)),
            dma((2, nz)),
            dma((2, nz)),
            dma((2, ny - 1, nz)),
            dma((2, ny, nz)),
            dma((2, ny - 1)),
            dma((2, nz - 1)),
            dma((2, nz - 1)),
            dma((2, ny - 1)),
            dma((2, 1)),
            dma((2, nx - 1)),
        ],
        compiler_params=pltpu.CompilerParams(
            collective_id=0, has_side_effects=True, vmem_limit_bytes=44 * 2**20
        ),
        cost_estimate=pl.CostEstimate(flops=10**7, bytes_accessed=4 * 10**6, transcendentals=0),
        name="gradient_sum",
    )(h, hs)


def dot_nt(a, b):
    return lax.dot_general(a, b, (((1,), (1,)), ((), ())), preferred_element_type=jnp.float32)


def dot_nn(a, b):
    return lax.dot_general(a, b, (((1,), (0,)), ((), ())), preferred_element_type=jnp.float32)


def dot_tn(a, b):
    return lax.dot_general(a, b, (((0,), (0,)), ((), ())), preferred_element_type=jnp.float32)


def iota(shape, axis):
    return lax.broadcasted_iota(jnp.int32, shape, axis)


def ones_where(mask):
    return jnp.where(mask, 1.0, 0.0).astype(jnp.bfloat16)


def dispatch_kernel(
    ny,
    nz,
    nx,
    cap,
    features,
    next_features,
    dest_ref,
    terminal,
    source_ids,
    subset,
    rewards,
    next_logp,
    source_weight,
    critic_shift,
    critic_head,
    target_mean,
    target_scale,
    target_shift,
    target_head,
    w_hbm,
    critic_hbm,
    rows,
    notes,
    shift_out,
    head_out,
    critic_out,
    target_w1,
    critic_w1,
    sent,
    sent_notes,
    q_all,
    acc,
    w_sem,
    critic_sem,
    row_send,
    row_recv,
    note_sems,
    x_sems,
    pair_sems,
    pair_note,
    q_sems,
):
    f32, bf16 = jnp.float32, jnp.bfloat16
    shards = 2 * ny * nz
    flat = 2 * ny
    kept = cap // 2
    tokens, width = features.shape
    me = lax.axis_index("dp")
    mx = lax.axis_index("member")
    c = lax.rem(me, 2)
    z = lax.rem(me // 2, nz)
    y = me // (2 * nz)
    partner = me + 1 - 2 * c
    hh = lax.rem(mx, 2)
    neighbor = mx + 1 - 2 * hh
    fetch = pltpu.make_async_copy(w_hbm, target_w1, w_sem)
    fetch.start()
    fetch_critic = pltpu.make_async_copy(critic_hbm.at[c], critic_w1, critic_sem)
    fetch_critic.start()

    def as_row(ref):
        wide = ref[...].astype(f32)
        return jnp.concatenate([wide[i : i + 1] for i in range(wide.shape[0])], axis=1)

    def remote(src, dst, send, recv, device):
        return pltpu.make_async_remote_copy(
            src_ref=src, dst_ref=dst, send_sem=send, recv_sem=recv, device_id=device, device_id_type=MESH
        )

    def zo(o):
        return lax.rem(z + nz + o, nz)

    def group(oz, skip, act):
        for j in range(flat):
            oy, oc = j // 2, j % 2
            if skip and j == 0:
                continue
            yy = lax.rem(y + oy, ny)
            cc = lax.rem(c + oc, 2)
            zz = zo(oz)
            act(oz, (yy * nz + zz) * 2 + cc, zz * flat + yy * 2 + cc, cc)

    def each(act):
        group(0, True, act)

        def step(i, _):
            group(near_first(i, nz), False, act)
            return 0

        lax.fori_loop(0, nz - 1, step, 0)

    barrier = pltpu.get_barrier_semaphore()

    def greet(oz, to, place, cc):
        pl.semaphore_signal(barrier, inc=1, device_id={"dp": to}, device_id_type=MESH)

    each(greet)
    for o in range(1, nx):
        pl.semaphore_signal(
            barrier, inc=1, device_id={"member": lax.rem(mx + o, nx)}, device_id_type=MESH
        )

    dest = dest_ref[...]
    dest = ((dest >> 1) & (nz - 1)) * flat + (dest // (2 * nz)) * 2 + (dest & 1)
    to_shard = dest == iota((shards, tokens), 0)
    chosen = ones_where(to_shard)
    before = ones_where(iota((tokens, tokens), 0) < iota((tokens, tokens), 1))
    rank = jnp.sum(jnp.where(to_shard, dot_nn(chosen, before), 0.0), axis=0, keepdims=True)
    rank = rank.astype(jnp.int32)
    low = rank - hh * kept
    slot = jnp.where((low >= 0) & (low < kept), dest * kept + low, -1)
    chunk = min(256, shards * kept)
    per = chunk // kept
    for i in range(shards // per):
        pick = ones_where(iota((chunk, tokens), 0) + i * chunk == slot)
        block = dot_nn(pick, features[...]).astype(bf16)
        sent[i * per : (i + 1) * per] = block.reshape(per, kept, width)

    pl.semaphore_wait(barrier, shards + nx - 2)

    def send_rows(oz, to, place, cc):
        remote(
            sent.at[place],
            rows.at[cc, hh, z, y * 2 + c],
            row_send,
            row_recv.at[lax.rem(oz, nz)],
            {"dp": to},
        ).start()

    each(send_rows)
    rows[c, hh, z, y * 2 + c] = sent[z * flat + y * 2 + c]

    weight = jnp.zeros((1, tokens), f32)
    weights = source_weight[...].astype(f32)
    for k in range(weights.shape[1]):
        weight = jnp.where(source_ids[...] == k, weights[:, k : k + 1], weight)

    hidden = target_w1.shape[1]
    wide = min(256, hidden)
    tall = min(512, tokens)
    acc[...] = jnp.zeros(acc.shape, f32)
    fetch.wait()
    for k in range(2):

        def block(i, _, k=k):
            units = pl.ds(pl.multiple_of(i * wide, wide), wide)
            scale = target_scale[k : k + 1, units]
            shift = target_shift[k : k + 1, units] - target_mean[k : k + 1, units] * scale
            head = target_head[k : k + 1, units]
            w = target_w1[k, units, :]
            for t in range(tokens // tall):
                pre = dot_nt(next_features[t * tall : (t + 1) * tall, :], w)
                term = jnp.maximum(pre * scale + shift, 0.0) * head
                total = term[:, 0:128]
                for part in range(1, wide // 128):
                    total = total + term[:, part * 128 : (part + 1) * 128]
                acc[k, t * tall : (t + 1) * tall, :] += total
            return 0

        lax.fori_loop(0, hidden // wide, block, 0, unroll=min(4, hidden // wide))
        q_all[mx, k] = jnp.sum(acc[k].T, axis=0, keepdims=True)

    def q_copy(o):
        ref = q_all.at[mx]
        return remote(ref, ref, q_sems.at[0, o - 1], q_sems.at[1, o - 1], {"member": lax.rem(mx + o, nx)})

    for o in range(1, nx):
        q_copy(o).start()

    half = nz // 2
    arrivals = [0] + [o % nz for k in range(1, half) for o in (k, -k)] + [half]

    def x_copy(o):
        ref = rows.at[c, hh, zo(-o)]
        return remote(ref, ref, x_sems.at[0, o], x_sems.at[1, o], {"member": neighbor})

    def pair_copy(part, o):
        ref = rows.at[c, hh + part - 2 * hh * part, zo(-o)]
        return remote(ref, ref, pair_sems.at[0, part, o], pair_sems.at[1, part, o], {"dp": partner})

    def arrive(o):
        ref = rows.at[c, hh, zo(-o)]
        if o == 0:
            ref = rows.at[c, hh, z, pl.ds(0, flat - 1)]
        remote(ref, ref, row_send, row_recv.at[o], {"dp": partner}).wait_recv()
        x_copy(o).start()
        pair_copy(0, o).start()

    shift_out[...] = critic_shift[pl.ds(c, 1), :]
    head_out[...] = critic_head[pl.ds(c, 1), :]
    fetch_critic.wait()
    step = min(256, critic_w1.shape[0])
    for i in range(critic_w1.shape[0] // step):
        cut = slice(i * step, (i + 1) * step)
        critic_out[:, cut] = critic_w1[cut, :].T.astype(bf16)
    early = nz // 2
    for o in arrivals[:early]:
        arrive(o)

    for o in range(1, nx):
        q_copy(o).wait_recv()
    first = jnp.zeros((1, tokens), f32)
    second = first
    for k in range(2 * nx):
        value = q_all[k // 2, k % 2]
        first = jnp.where(subset[0:1, :] == k, value, first)
        second = jnp.where(subset[1:2, :] == k, value, second)
    lowest = jnp.minimum(first, second)
    carry = 1.0 - terminal[...].astype(f32)
    target = as_row(rewards) + GAMMA * carry * (lowest - ALPHA * as_row(next_logp))

    lane = iota((128, tokens), 0)
    spread = jnp.where(to_shard, target, 0.0).astype(bf16)
    spread_w = jnp.where(to_shard, weight, 0.0).astype(bf16)
    note = dot_nt(spread, ones_where(lane == rank)) + dot_nt(spread_w, ones_where(lane == rank + cap))
    sent_notes[...] = note.reshape(shards, 1, 128)
    mine = z * flat + y * 2 + c

    def send_notes(oz, to, place, cc):
        remote(
            sent_notes.at[place], notes.at[cc, mine], note_sems.at[0], note_sems.at[1], {"dp": to}
        ).start()

    each(send_notes)
    notes[c, mine] = sent_notes[mine]

    for o in arrivals[early:]:
        arrive(o)
    for o in arrivals:
        x_copy(o).wait_recv()
        pair_copy(1, o).start()
    most = notes.at[c, pl.ds(0, shards - 1)]
    all_notes = remote(most, most, note_sems.at[0], note_sems.at[1], {"dp": partner})
    all_notes.wait_recv()
    pair_n = remote(notes.at[c], notes.at[c], pair_note.at[0], pair_note.at[1], {"dp": partner})
    pair_n.start()

    all_notes.wait_send()
    most = sent.at[pl.ds(0, shards - 1)]
    remote(most, most, row_send, row_recv.at[0], {"dp": partner}).wait_send()
    for o in range(1, nx):
        q_copy(o).wait_send()
    for o in arrivals:
        x_copy(o).wait_send()
        pair_copy(0, o).wait()
        pair_copy(1, o).wait()
    pair_n.wait()


def dispatch(features, next_features, small, targets, critics, ny, nz, nx):
    tokens, width = features.shape
    shards = 2 * ny * nz
    cap = 2 * tokens // shards
    f32, bf16 = jnp.float32, jnp.bfloat16
    vmem = pl.BlockSpec(memory_space=pltpu.VMEM)
    dma = pltpu.SemaphoreType.DMA
    w1 = targets[0]
    return pl.pallas_call(
        functools.partial(dispatch_kernel, ny, nz, nx, cap),
        out_shape=(
            pltpu.VMEM((2, 2, nz, 2 * ny, cap // 2, width), bf16),
            pltpu.VMEM((2, shards, 1, 128), f32),
            pltpu.VMEM((1, w1.shape[1]), f32),
            pltpu.VMEM((1, w1.shape[1]), f32),
            pltpu.VMEM(w1.shape[:0:-1], bf16),
        ),
        in_specs=[vmem] * 15 + [pl.BlockSpec(memory_space=pltpu.HBM)] * 2,
        out_specs=[vmem] * 5,
        scratch_shapes=[
            pltpu.VMEM(w1.shape, w1.dtype),
            pltpu.VMEM(w1.shape[1:], f32),
            pltpu.VMEM((shards, cap // 2, width), bf16),
            pltpu.VMEM((shards, 1, 128), f32),
            pltpu.VMEM((nx, 2, 1, tokens), f32),
            pltpu.VMEM((2, tokens, 128), f32),
            dma,
            dma,
            dma,
            dma((nz,)),
            dma((2,)),
            dma((2, nz)),
            dma((2, 2, nz)),
            dma((2,)),
            dma((2, nx - 1)),
        ],
        compiler_params=pltpu.CompilerParams(
            collective_id=1, has_side_effects=True, vmem_limit_bytes=56 * 2**20
        ),
        cost_estimate=pl.CostEstimate(flops=10**9, bytes_accessed=4 * 10**6, transcendentals=0),
        name="dispatch",
    )(features, next_features, *small, *critics[1:], *targets[1:], w1, critics[0])


def critic_kernel(
    cap,
    tile,
    rows,
    notes,
    shift_ref,
    head_ref,
    w,
    h,
    hs,
    xc,
    targets,
    weights,
    zbuf,
    gbuf,
    gt,
    sq,
    s0,
    s1,
):
    f32, bf16 = jnp.float32, jnp.bfloat16
    slots, width = rows.shape[1:]
    hidden = w.shape[1]
    shards = slots // cap
    pieces = slots // 128
    few, many = 3, 6
    big = few * tile
    wide = min(256, hidden)
    lanes = hidden // 128
    shift = shift_ref[...]
    head = head_ref[...]

    kept, part = cap // 2, slots // 2
    at_slot = iota((1, slots), 1)
    owner = ones_where(lax.rem(at_slot, part) // kept == iota((shards, slots), 0))
    my_slot = at_slot // part * kept + lax.rem(at_slot, kept) == iota((cap, slots), 0)
    upto = ones_where(iota((128, 128), 0) <= iota((128, 128), 1))
    counts = []
    for s in range(2):
        by_slot = notes[s, :, 0, :].T[0 : 2 * cap].astype(bf16)
        spread = dot_nn(by_slot, owner)
        y_row = jnp.sum(jnp.where(my_slot, spread[0:cap], 0.0), axis=0, keepdims=True)
        w_row = jnp.sum(jnp.where(my_slot, spread[cap : 2 * cap], 0.0), axis=0, keepdims=True)
        alive = jnp.where(w_row > 0, 1.0, 0.0)
        stacked = jnp.concatenate(
            [alive[:, p * 128 : (p + 1) * 128] for p in range(pieces)]
            + [jnp.zeros((8, 128), f32)] * (1 if pieces < 8 else 0),
            axis=0,
        )
        running = dot_nn(stacked.astype(bf16), upto)
        place = []
        start = jnp.zeros((1, 1), f32)
        for p in range(pieces):
            position = running[p : p + 1] - 1.0 + start
            position = jnp.where(stacked[p : p + 1] > 0, position, -1.0)
            place.append(position.astype(jnp.int32))
            start = start + running[p : p + 1, 127:128]
        number = jnp.sum(alive)
        counts.append(number)
        yw = jnp.concatenate(
            [jnp.broadcast_to(y_row, (128, slots)), jnp.broadcast_to(w_row, (128, slots))], axis=0
        ).astype(bf16)
        trips = jnp.where(number <= few * tile, few, many)

        def compact(i, _, s=s, place=place, yw=yw):
            at = pl.ds(pl.multiple_of(i * big, big), big)
            row = iota((big, 128), 0) + i * big
            pick = jnp.concatenate([ones_where(row == p) for p in place], axis=1)
            xc[s, at, :] = dot_nn(pick, rows[s]).astype(bf16)
            both = dot_nt(pick, yw)
            targets[s, at, :] = both[:, 0:128]
            weights[s, at, :] = both[:, 128:256]
            return 0

        lax.fori_loop(0, trips // few, compact, 0)

    total0 = jnp.zeros((1, hidden), f32)
    total1 = jnp.zeros((1, hidden), f32)
    groups = tile // 8
    for s in range(2):
        number = counts[s]
        whole = jnp.full((1, 1), number, f32)
        trips = jnp.where(number <= few * tile, few, many)
        middle = jnp.sum(rows[s].astype(f32), axis=0, keepdims=True) / whole
        one = middle.astype(bf16)
        rest = middle - one.astype(f32)
        two = rest.astype(bf16)
        three = (rest - two.astype(f32)).astype(bf16)
        parts = jnp.concatenate(
            [one.astype(f32), two.astype(f32), three.astype(f32), jnp.zeros((13, width), f32)], axis=0
        ).astype(bf16)
        mu = jnp.sum(dot_nn(parts, w[...]), axis=0, keepdims=True)
        sq[...] = jnp.zeros(sq.shape, f32)
        s0[...] = jnp.zeros(s0.shape, f32)
        s1[...] = jnp.zeros(s1.shape, f32)

        def forward(i, _, s=s, mu=mu, number=number):
            at = pl.ds(pl.multiple_of(i * tile, tile), tile)
            row = iota((tile, 128), 0) + i * tile
            alive = jnp.where(row < number.astype(jnp.int32), 1.0, 0.0)
            x = xc[s, at, :]
            for j in range(hidden // wide):
                pre = dot_nn(x, w[:, j * wide : (j + 1) * wide])
                for k in range(wide // 128):
                    lo = j * wide + k * 128
                    zc = (pre[:, k * 128 : (k + 1) * 128] - mu[:, lo : lo + 128]) * alive
                    zbuf[at, lo : lo + 128] = zc
                    sq[:, lo : lo + 128] += jnp.sum((zc * zc).reshape(groups, 8, 128), axis=0)
            return 0

        lax.fori_loop(0, trips, forward, 0)
        var = jnp.sum(sq[...], axis=0, keepdims=True) / whole
        inv = 1.0 / jnp.sqrt(var + EPS)

        def slopes(i, _, s=s, inv=inv):
            at = pl.ds(pl.multiple_of(i * tile, tile), tile)
            acc = jnp.zeros((tile, 128), f32)
            for j in range(lanes):
                cut = slice(j * 128, (j + 1) * 128)
                zh = zbuf[at, cut] * inv[:, cut]
                zbuf[at, cut] = zh
                acc = acc + jnp.maximum(zh + shift[:, cut], 0.0) * head[:, cut]
            q = jnp.sum(acc, axis=1, keepdims=True)
            dq = weights[s, at, :] * (q - targets[s, at, :])
            for j in range(lanes):
                cut = slice(j * 128, (j + 1) * 128)
                zh = zbuf[at, cut]
                g = jnp.where(zh > -shift[:, cut], dq, 0.0)
                gbuf[at, cut] = g
                s0[:, cut] += jnp.sum(g.reshape(groups, 8, 128), axis=0)
                s1[:, cut] += jnp.sum((g * zh).reshape(groups, 8, 128), axis=0)
            return 0

        lax.fori_loop(0, trips, slopes, 0)
        sum0 = jnp.sum(s0[...], axis=0, keepdims=True)
        sum1 = jnp.sum(s1[...], axis=0, keepdims=True)
        total0 = total0 + sum0
        total1 = total1 + sum1
        scale = inv * head
        base = -scale * (sum0 / whole)
        tilt = -scale * (sum1 / whole)

        def slope_of(at, cut, scale=scale, base=base, tilt=tilt):
            value = gbuf[at, cut] * scale[:, cut] + (zbuf[at, cut] * tilt[:, cut] + base[:, cut])
            return value.astype(bf16)

        @pl.when(trips == few)
        def _(s=s, slope_of=slope_of):
            xt = xc[s, 0:big, :].T
            for j in range(hidden // wide):
                cut = slice(j * wide, (j + 1) * wide)
                out = dot_nn(xt, slope_of(slice(0, big), cut))
                gt[:, cut] = out if s == 0 else gt[:, cut] + out

        @pl.when(trips != few)
        def _(s=s, slope_of=slope_of):
            if s == 0:
                gt[...] = jnp.zeros(gt.shape, f32)

            def step(i, _):
                at = pl.ds(pl.multiple_of(i * tile, tile), tile)
                for j in range(hidden // wide):
                    cut = slice(j * wide, (j + 1) * wide)
                    gt[:, cut] += dot_tn(xc[s, at, :], slope_of(at, cut))
                return 0

            lax.fori_loop(0, many, step, 0)

    g_shift = head * total0
    g_head = shift * total0 + total1
    for u in range(lanes):
        cut = slice(u * 128, (u + 1) * 128)
        h[2 * u] = gt[0:128, cut].astype(bf16)
        h[2 * u + 1] = gt[128:256, cut].astype(bf16)
        hs[2 * u] = g_shift[:, cut]
        hs[2 * u + 1] = g_head[:, cut]


def critic_sums(rows, notes, shift, head, w1, cap):
    f32, bf16 = jnp.float32, jnp.bfloat16
    slots, width = rows.shape[1:]
    hidden = w1.shape[1]
    tile = slots * 3 // 16
    tall = 6 * tile
    vmem = pl.BlockSpec(memory_space=pltpu.VMEM)
    blocks = hidden // 128 * (width // 128)
    return pl.pallas_call(
        functools.partial(critic_kernel, cap, tile),
        out_shape=(
            pltpu.VMEM((blocks, 128, 128), bf16),
            pltpu.VMEM((blocks, 1, 128), f32),
        ),
        in_specs=[vmem] * 5,
        out_specs=[vmem] * 2,
        scratch_shapes=[
            pltpu.VMEM((2, tall, width), bf16),
            pltpu.VMEM((2, tall, 128), f32),
            pltpu.VMEM((2, tall, 128), f32),
            pltpu.VMEM((tall, hidden), f32),
            pltpu.VMEM((tall, hidden), f32),
            pltpu.VMEM((width, hidden), f32),
            pltpu.VMEM((8, hidden), f32),
            pltpu.VMEM((8, hidden), f32),
            pltpu.VMEM((8, hidden), f32),
        ],
        compiler_params=pltpu.CompilerParams(vmem_limit_bytes=48 * 2**20),
        cost_estimate=pl.CostEstimate(
            flops=8 * slots * hidden * width, bytes_accessed=4 * 10**6, transcendentals=0
        ),
        name="critic_sums",
    )(rows, notes, shift, head, w1)


def per_device(
    features,
    next_features,
    rewards,
    next_logp,
    terminal,
    source_ids,
    source_weight,
    subset,
    destination,
    critic_w1,
    critic_shift,
    critic_head,
    target_w1,
    target_mean,
    target_scale,
    target_shift,
    target_head,
):
    f32 = jnp.float32
    shards = lax.axis_size("dp")
    nx = lax.axis_size("member")
    nz = NZ
    ny = shards // (2 * nz)
    tokens, width = features.shape
    critics, hidden = critic_w1.shape[:2]
    cap = 2 * tokens // shards
    rows, notes, shift, head, w1 = dispatch(
        features,
        next_features,
        (
            destination.reshape(1, tokens),
            terminal.reshape(1, tokens),
            source_ids.reshape(1, tokens),
            subset.T,
            rewards.reshape(tokens // 128, 128),
            next_logp.reshape(tokens // 128, 128),
            source_weight.reshape(1, -1),
        ),
        (target_w1, target_mean, target_scale, target_shift, target_head),
        (critic_w1, critic_shift, critic_head),
        ny,
        nz,
        nx,
    )
    h, hs = critic_sums(rows.reshape(2, shards * cap, width), notes, shift, head, w1, cap)
    h = h.reshape(ny, nz, 128, 128)
    hs = hs.reshape(ny, nz, 1, 128)
    full, shift, head, factor = reduce_all(h, hs, ny, nz, nx)
    factor = factor[0, 0]
    step_w1 = full.reshape(critics, hidden, width).astype(f32) * factor
    return (step_w1, shift * factor, head * factor)


def solution(mesh):
    in_specs = (
        P("dp", None),
        P("dp", None),
        P("dp"),
        P("dp"),
        P("dp"),
        P("dp"),
        P(),
        P("dp", None),
        P("dp"),
        P("member", None, None),
        P("member", None),
        P("member", None),
        P("member", None, None),
        P("member", None),
        P("member", None),
        P("member", None),
        P("member", None),
    )
    out_specs = (P("member", None, None), P("member", None), P("member", None))
    return jax.shard_map(
        per_device, mesh=mesh, in_specs=in_specs, out_specs=out_specs, check_vma=False
    )
```

```python
import functools
import math

import jax
import jax.numpy as jnp
from jax import lax
from jax.experimental import pallas as pl
from jax.experimental.pallas import tpu as pltpu
from jax.sharding import PartitionSpec as P

GAMMA = 0.99
ALPHA = 0.2
EPS = 1e-05
NZ = 8
MESH = pl.DeviceIdType.MESH


def far_first(i, nz):
    half = nz // 2
    return half + ((i + 1) // 2) * (2 * ((i + 1) % 2) - 1)


def near_first(i, nz):
    return far_first(nz - 2 - i, nz)


def reduce_kernel(
    ny,
    nz,
    nx,
    h,
    hs,
    full,
    shift_out,
    head_out,
    factor_out,
    small,
    y_in,
    z_out,
    z_in,
    ys_in,
    zs_out,
    zs_in,
    x_out,
    x_in,
    y_sems,
    z_sems,
    gz_sems,
    gy_sems,
    pair_sems,
    ys_sems,
    zs_sems,
    gzs_sems,
    gys_sems,
    pair_small,
    x_sems,
):
    me = lax.axis_index("dp")
    mx = lax.axis_index("member")
    c = lax.rem(me, 2)
    z = lax.rem(me // 2, nz)
    y = me // (2 * nz)
    partner = me + 1 - 2 * c

    def dp_of(yy, zz):
        return (yy * nz + zz) * 2 + c

    def yo(o):
        return lax.rem(y + o, ny)

    def zo(o):
        return lax.rem(z + o, nz)

    def copy(src, dst, sems, index, dp):
        return pltpu.make_async_remote_copy(
            src_ref=src,
            dst_ref=dst,
            send_sem=sems.at[(0,) + index],
            recv_sem=sems.at[(1,) + index],
            device_id={"dp": dp},
            device_id_type=MESH,
        )

    def block_of(yy, zz):
        return full.at[
            c, yy * (nz // 2) + zz // 2, :, pl.ds(pl.multiple_of(lax.rem(zz, 2) * 128, 128), 128)
        ]

    barrier = pltpu.get_barrier_semaphore()
    for o in range(1, ny):
        pl.semaphore_signal(barrier, inc=1, device_id={"dp": dp_of(yo(o), z)}, device_id_type=MESH)
    for o in range(1, nz):
        pl.semaphore_signal(barrier, inc=1, device_id={"dp": dp_of(y, zo(o))}, device_id_type=MESH)
    pl.semaphore_signal(barrier, inc=1, device_id={"dp": partner}, device_id_type=MESH)
    for o in range(1, nx):
        pl.semaphore_signal(
            barrier, inc=1, device_id={"member": lax.rem(mx + o, nx)}, device_id_type=MESH
        )
    pl.semaphore_wait(barrier, ny + nz + nx - 2)

    def y_small(o):
        return copy(hs.at[yo(o)], ys_in.at[o - 1], ys_sems, (o - 1,), dp_of(yo(o), z))

    def y_block(o, oz):
        return copy(
            h.at[yo(o), zo(oz)],
            y_in.at[o - 1, oz],
            y_sems,
            (o - 1, oz),
            dp_of(yo(o), z),
        )

    for o in range(1, ny):
        y_small(o).start()

    def send_y(i, _):
        oz = lax.rem(far_first(i, nz), nz)
        for o in range(1, ny):
            y_block(o, oz).start()
        return 0

    lax.fori_loop(0, nz - 1, send_y, 0)
    for o in range(1, ny):
        y_block(o, 0).start()

    def z_small(o):
        return copy(zs_out.at[zo(o)], zs_in.at[o - 1], zs_sems, (o - 1,), dp_of(y, zo(o)))

    def z_block(o):
        return copy(z_out.at[o], z_in.at[o], z_sems, (o,), dp_of(y, zo(o)))

    for o in range(1, ny):
        y_small(o).wait_recv()
    zs_out[...] = hs[y] + sum(ys_in[o - 1] for o in range(1, ny))
    for o in range(1, nz):
        z_small(o).start()

    def y_sum(oz):
        for o in range(1, ny):
            y_block(o, oz).wait_recv()
        value = h[y, zo(oz)].astype(jnp.float32)
        for o in range(1, ny):
            value = value + y_in[o - 1, oz].astype(jnp.float32)
        z_out[oz] = value

    def send_z(i, _):
        oz = lax.rem(far_first(i, nz), nz)
        y_sum(oz)
        z_block(oz).start()
        return 0

    lax.fori_loop(0, nz - 1, send_z, 0)
    y_sum(0)

    for o in range(1, nz):
        z_small(o).wait_recv()
    mine_small = zs_out[z] + sum(zs_in[o - 1] for o in range(1, nz))

    def add_z(i, value):
        oz = near_first(i, nz)
        z_block(oz).wait_recv()
        return value + z_in[oz]

    z_out[0] = lax.fori_loop(0, nz - 1, add_z, z_out[0])
    mine = z_out[0]
    squares = jnp.sum(mine * mine) + jnp.sum(mine_small * mine_small)
    small[c, y, z, :, 0:128] = mine_small
    small[c, y, z, :, 128:256] = jnp.full((1, 128), squares, jnp.float32)
    block_of(y, z)[...] = mine.T.astype(jnp.bfloat16)

    def gz_small(o):
        ref = small.at[c, y, z]
        return copy(ref, ref, gzs_sems, (o - 1,), dp_of(y, zo(o)))

    def gz_block(o):
        ref = block_of(y, z)
        return copy(ref, ref, gz_sems, (o,), dp_of(y, zo(o)))

    def gy_small(o):
        ref = small.at[c, y]
        return copy(ref, ref, gys_sems, (o - 1,), dp_of(yo(o), z))

    def gy_block(o, oz):
        ref = block_of(y, zo(nz - oz))
        return copy(ref, ref, gy_sems, (o - 1, oz), dp_of(yo(o), z))

    def pair_block(oy, oz):
        ref = block_of(yo(ny - oy), zo(nz - oz))
        return copy(ref, ref, pair_sems, (oy, oz), partner)

    for o in range(1, nz):
        gz_small(o).start()

    def send_gz(i, _):
        gz_block(near_first(i, nz)).start()
        return 0

    lax.fori_loop(0, nz - 1, send_gz, 0)
    for o in range(1, ny):
        gy_block(o, 0).start()
    pair_block(0, 0).start()

    for o in range(1, nz):
        gz_small(o).wait_recv()
    for o in range(1, ny):
        gy_small(o).start()

    def relay_z(i, _):
        oz = near_first(i, nz)
        gz_block(oz).wait_recv()
        for o in range(1, ny):
            gy_block(o, oz).start()
        pair_block(0, oz).start()
        return 0

    lax.fori_loop(0, nz - 1, relay_z, 0)

    for o in range(1, ny):
        gy_small(o).wait_recv()
    pair_s = copy(small.at[c], small.at[c], pair_small, (0,), partner)
    pair_s.start()

    def relay_y(i, _):
        oz = lax.rem(near_first(lax.rem(i + nz - 2, nz - 1), nz) * lax.min(i, 1), nz)
        for o in range(1, ny):
            gy_block(o, oz).wait_recv()
            pair_block(o, oz).start()
        return 0

    half = nz // 2
    lax.fori_loop(0, half, relay_y, 0)
    pair_s.wait_recv()
    x_out[...] = jnp.sum(small[:, :, :, :, 128:256], axis=(0, 1, 2))

    def x_copy(o):
        return pltpu.make_async_remote_copy(
            src_ref=x_out,
            dst_ref=x_in.at[o - 1],
            send_sem=x_sems.at[0, o - 1],
            recv_sem=x_sems.at[1, o - 1],
            device_id={"member": lax.rem(mx + o, nx)},
            device_id_type=MESH,
        )

    for o in range(1, nx):
        x_copy(o).start()
    lax.fori_loop(half, nz, relay_y, 0)
    for o in range(1, nx):
        x_copy(o).wait_recv()
    total = x_out[...] + sum(x_in[o - 1] for o in range(1, nx))
    root = math.sqrt(2 * nx * (ny * nz // 2 * 128) * 258)
    factor_out[...] = root / jnp.maximum(jnp.sqrt(total), root)
    for k in range(2):
        for b in range(ny * nz // 2):
            cut = slice(b * 128, (b + 1) * 128)
            at = b // (nz // 2), 2 * (b % (nz // 2))
            shift_out[k : k + 1, cut] = small[k, at[0], at[1], :, 0:128]
            head_out[k : k + 1, cut] = small[k, at[0], at[1] + 1, :, 0:128]

    def wait_pair(i, _):
        for o in range(ny):
            pair_block(o, i).wait_recv()
        return 0

    lax.fori_loop(0, nz, wait_pair, 0)

    def drain_y(i, _):
        for o in range(1, ny):
            y_block(o, i).wait_send()
            gy_block(o, i).wait_send()
        for o in range(ny):
            pair_block(o, i).wait_send()
        return 0

    lax.fori_loop(0, nz, drain_y, 0)

    def drain_z(i, _):
        z_block(i).wait_send()
        gz_block(i).wait_send()
        return 0

    lax.fori_loop(1, nz, drain_z, 0)
    for o in range(1, ny):
        y_small(o).wait_send()
        gy_small(o).wait_send()
    for o in range(1, nz):
        z_small(o).wait_send()
        gz_small(o).wait_send()
    for o in range(1, nx):
        x_copy(o).wait_send()
    pair_s.wait_send()


def reduce_all(h, hs, ny, nz, nx):
    rows, width = h.shape[2:]
    f32, bf16 = jnp.float32, jnp.bfloat16
    vmem = pl.BlockSpec(memory_space=pltpu.VMEM)
    dma = pltpu.SemaphoreType.DMA
    return pl.pallas_call(
        functools.partial(reduce_kernel, ny, nz, nx),
        out_shape=(
            pltpu.VMEM((2, ny * nz // 2, 128, 256), bf16),
            pltpu.VMEM((2, ny * nz // 2 * 128), f32),
            pltpu.VMEM((2, ny * nz // 2 * 128), f32),
            pltpu.VMEM((1, 128), f32),
        ),
        in_specs=[vmem] * 2,
        out_specs=[vmem] * 4,
        scratch_shapes=[
            pltpu.VMEM((2, ny, nz, 1, 256), f32),
            pltpu.VMEM((ny - 1, nz, rows, width), bf16),
            pltpu.VMEM((nz, rows, width), f32),
            pltpu.VMEM((nz, rows, width), f32),
            pltpu.VMEM((ny - 1, nz, 1, 128), f32),
            pltpu.VMEM((nz, 1, 128), f32),
            pltpu.VMEM((nz - 1, 1, 128), f32),
            pltpu.VMEM((1, 128), f32),
            pltpu.VMEM((nx - 1, 1, 128), f32),
            dma((2, ny - 1, nz)),
            dma((2, nz)),
            dma((2, nz)),
            dma((2, ny - 1, nz)),
            dma((2, ny, nz)),
            dma((2, ny - 1)),
            dma((2, nz - 1)),
            dma((2, nz - 1)),
            dma((2, ny - 1)),
            dma((2, 1)),
            dma((2, nx - 1)),
        ],
        compiler_params=pltpu.CompilerParams(
            collective_id=0, has_side_effects=True, vmem_limit_bytes=44 * 2**20
        ),
        cost_estimate=pl.CostEstimate(flops=10**7, bytes_accessed=4 * 10**6, transcendentals=0),
        name="gradient_sum",
    )(h, hs)


def dot_nt(a, b):
    return lax.dot_general(a, b, (((1,), (1,)), ((), ())), preferred_element_type=jnp.float32)


def dot_nn(a, b):
    return lax.dot_general(a, b, (((1,), (0,)), ((), ())), preferred_element_type=jnp.float32)


def dot_tn(a, b):
    return lax.dot_general(a, b, (((0,), (0,)), ((), ())), preferred_element_type=jnp.float32)


def iota(shape, axis):
    return lax.broadcasted_iota(jnp.int32, shape, axis)


def ones_where(mask):
    return jnp.where(mask, 1.0, 0.0).astype(jnp.bfloat16)


def dispatch_kernel(
    ny,
    nz,
    nx,
    cap,
    features,
    next_features,
    dest_ref,
    terminal,
    source_ids,
    subset,
    rewards,
    next_logp,
    source_weight,
    critic_shift,
    critic_head,
    target_mean,
    target_scale,
    target_shift,
    target_head,
    w_hbm,
    critic_hbm,
    rows,
    notes,
    shift_out,
    head_out,
    critic_out,
    target_w1,
    critic_w1,
    sent,
    sent_notes,
    q_all,
    acc,
    w_sem,
    critic_sem,
    row_send,
    row_recv,
    note_sems,
    x_sems,
    pair_sems,
    pair_note,
    q_sems,
):
    f32, bf16 = jnp.float32, jnp.bfloat16
    shards = 2 * ny * nz
    flat = 2 * ny
    kept = cap // 2
    tokens, width = features.shape
    me = lax.axis_index("dp")
    mx = lax.axis_index("member")
    c = lax.rem(me, 2)
    z = lax.rem(me // 2, nz)
    y = me // (2 * nz)
    partner = me + 1 - 2 * c
    hh = lax.rem(mx, 2)
    neighbor = mx + 1 - 2 * hh
    fetch = pltpu.make_async_copy(w_hbm, target_w1, w_sem)
    fetch.start()
    fetch_critic = pltpu.make_async_copy(critic_hbm.at[c], critic_w1, critic_sem)
    fetch_critic.start()

    def as_row(ref):
        wide = ref[...].astype(f32)
        return jnp.concatenate([wide[i : i + 1] for i in range(wide.shape[0])], axis=1)

    def remote(src, dst, send, recv, device):
        return pltpu.make_async_remote_copy(
            src_ref=src, dst_ref=dst, send_sem=send, recv_sem=recv, device_id=device, device_id_type=MESH
        )

    def zo(o):
        return lax.rem(z + nz + o, nz)

    def group(oz, skip, act):
        for j in range(flat):
            oy, oc = j // 2, j % 2
            if skip and j == 0:
                continue
            yy = lax.rem(y + oy, ny)
            cc = lax.rem(c + oc, 2)
            zz = zo(oz)
            act(oz, (yy * nz + zz) * 2 + cc, zz * flat + yy * 2 + cc, cc)

    def each(act):
        group(0, True, act)

        def step(i, _):
            group(near_first(i, nz), False, act)
            return 0

        lax.fori_loop(0, nz - 1, step, 0)

    barrier = pltpu.get_barrier_semaphore()

    def greet(oz, to, place, cc):
        pl.semaphore_signal(barrier, inc=1, device_id={"dp": to}, device_id_type=MESH)

    each(greet)
    for o in range(1, nx):
        pl.semaphore_signal(
            barrier, inc=1, device_id={"member": lax.rem(mx + o, nx)}, device_id_type=MESH
        )

    dest = dest_ref[...]
    dest = ((dest >> 1) & (nz - 1)) * flat + (dest // (2 * nz)) * 2 + (dest & 1)
    to_shard = dest == iota((shards, tokens), 0)
    chosen = ones_where(to_shard)
    before = ones_where(iota((tokens, tokens), 0) < iota((tokens, tokens), 1))
    rank = jnp.sum(jnp.where(to_shard, dot_nn(chosen, before), 0.0), axis=0, keepdims=True)
    rank = rank.astype(jnp.int32)
    low = rank - hh * kept
    slot = jnp.where((low >= 0) & (low < kept), dest * kept + low, -1)
    chunk = min(256, shards * kept)
    per = chunk // kept
    for i in range(shards // per):
        pick = ones_where(iota((chunk, tokens), 0) + i * chunk == slot)
        block = dot_nn(pick, features[...]).astype(bf16)
        sent[i * per : (i + 1) * per] = block.reshape(per, kept, width)

    pl.semaphore_wait(barrier, shards + nx - 2)

    def send_rows(oz, to, place, cc):
        remote(
            sent.at[place],
            rows.at[cc, hh, z, y * 2 + c],
            row_send,
            row_recv.at[lax.rem(oz, nz)],
            {"dp": to},
        ).start()

    each(send_rows)
    rows[c, hh, z, y * 2 + c] = sent[z * flat + y * 2 + c]

    weight = jnp.zeros((1, tokens), f32)
    weights = source_weight[...].astype(f32)
    for k in range(weights.shape[1]):
        weight = jnp.where(source_ids[...] == k, weights[:, k : k + 1], weight)

    hidden = target_w1.shape[1]
    wide = min(256, hidden)
    tall = min(512, tokens)
    acc[...] = jnp.zeros(acc.shape, f32)
    fetch.wait()
    for k in range(2):

        def block(i, _, k=k):
            units = pl.ds(pl.multiple_of(i * wide, wide), wide)
            scale = target_scale[k : k + 1, units]
            shift = target_shift[k : k + 1, units] - target_mean[k : k + 1, units] * scale
            head = target_head[k : k + 1, units]
            w = target_w1[k, units, :]
            for t in range(tokens // tall):
                pre = dot_nt(next_features[t * tall : (t + 1) * tall, :], w)
                term = jnp.maximum(pre * scale + shift, 0.0) * head
                total = term[:, 0:128]
                for part in range(1, wide // 128):
                    total = total + term[:, part * 128 : (part + 1) * 128]
                acc[k, t * tall : (t + 1) * tall, :] += total
            return 0

        lax.fori_loop(0, hidden // wide, block, 0, unroll=min(8, hidden // wide))
        q_all[mx, k] = jnp.sum(acc[k].T, axis=0, keepdims=True)

    def q_copy(o):
        ref = q_all.at[mx]
        return remote(ref, ref, q_sems.at[0, o - 1], q_sems.at[1, o - 1], {"member": lax.rem(mx + o, nx)})

    for o in range(1, nx):
        q_copy(o).start()

    half = nz // 2
    arrivals = [0] + [o % nz for k in range(1, half) for o in (k, -k)] + [half]

    def x_copy(o):
        ref = rows.at[c, hh, zo(-o)]
        return remote(ref, ref, x_sems.at[0, o], x_sems.at[1, o], {"member": neighbor})

    def pair_copy(part, o):
        ref = rows.at[c, hh + part - 2 * hh * part, zo(-o)]
        return remote(ref, ref, pair_sems.at[0, part, o], pair_sems.at[1, part, o], {"dp": partner})

    def arrive(o):
        ref = rows.at[c, hh, zo(-o)]
        if o == 0:
            ref = rows.at[c, hh, z, pl.ds(0, flat - 1)]
        remote(ref, ref, row_send, row_recv.at[o], {"dp": partner}).wait_recv()
        x_copy(o).start()
        pair_copy(0, o).start()

    shift_out[...] = critic_shift[pl.ds(c, 1), :]
    head_out[...] = critic_head[pl.ds(c, 1), :]
    fetch_critic.wait()
    step = min(256, critic_w1.shape[0])
    for i in range(critic_w1.shape[0] // step):
        cut = slice(i * step, (i + 1) * step)
        critic_out[:, cut] = critic_w1[cut, :].T.astype(bf16)
    early = nz // 2
    for o in arrivals[:early]:
        arrive(o)

    for o in range(1, nx):
        q_copy(o).wait_recv()
    first = jnp.zeros((1, tokens), f32)
    second = first
    for k in range(2 * nx):
        value = q_all[k // 2, k % 2]
        first = jnp.where(subset[0:1, :] == k, value, first)
        second = jnp.where(subset[1:2, :] == k, value, second)
    lowest = jnp.minimum(first, second)
    carry = 1.0 - terminal[...].astype(f32)
    target = as_row(rewards) + GAMMA * carry * (lowest - ALPHA * as_row(next_logp))

    lane = iota((128, tokens), 0)
    spread = jnp.where(to_shard, target, 0.0).astype(bf16)
    spread_w = jnp.where(to_shard, weight, 0.0).astype(bf16)
    note = dot_nt(spread, ones_where(lane == rank)) + dot_nt(spread_w, ones_where(lane == rank + cap))
    sent_notes[...] = note.reshape(shards, 1, 128)
    mine = z * flat + y * 2 + c

    def send_notes(oz, to, place, cc):
        remote(
            sent_notes.at[place], notes.at[cc, mine], note_sems.at[0], note_sems.at[1], {"dp": to}
        ).start()

    each(send_notes)
    notes[c, mine] = sent_notes[mine]

    for o in arrivals[early:]:
        arrive(o)
    for o in arrivals:
        x_copy(o).wait_recv()
        pair_copy(1, o).start()
    most = notes.at[c, pl.ds(0, shards - 1)]
    all_notes = remote(most, most, note_sems.at[0], note_sems.at[1], {"dp": partner})
    all_notes.wait_recv()
    pair_n = remote(notes.at[c], notes.at[c], pair_note.at[0], pair_note.at[1], {"dp": partner})
    pair_n.start()

    all_notes.wait_send()
    most = sent.at[pl.ds(0, shards - 1)]
    remote(most, most, row_send, row_recv.at[0], {"dp": partner}).wait_send()
    for o in range(1, nx):
        q_copy(o).wait_send()
    for o in arrivals:
        x_copy(o).wait_send()
        pair_copy(0, o).wait()
        pair_copy(1, o).wait()
    pair_n.wait()


def dispatch(features, next_features, small, targets, critics, ny, nz, nx):
    tokens, width = features.shape
    shards = 2 * ny * nz
    cap = 2 * tokens // shards
    f32, bf16 = jnp.float32, jnp.bfloat16
    vmem = pl.BlockSpec(memory_space=pltpu.VMEM)
    dma = pltpu.SemaphoreType.DMA
    w1 = targets[0]
    return pl.pallas_call(
        functools.partial(dispatch_kernel, ny, nz, nx, cap),
        out_shape=(
            pltpu.VMEM((2, 2, nz, 2 * ny, cap // 2, width), bf16),
            pltpu.VMEM((2, shards, 1, 128), f32),
            pltpu.VMEM((1, w1.shape[1]), f32),
            pltpu.VMEM((1, w1.shape[1]), f32),
            pltpu.VMEM(w1.shape[:0:-1], bf16),
        ),
        in_specs=[vmem] * 15 + [pl.BlockSpec(memory_space=pltpu.HBM)] * 2,
        out_specs=[vmem] * 5,
        scratch_shapes=[
            pltpu.VMEM(w1.shape, w1.dtype),
            pltpu.VMEM(w1.shape[1:], f32),
            pltpu.VMEM((shards, cap // 2, width), bf16),
            pltpu.VMEM((shards, 1, 128), f32),
            pltpu.VMEM((nx, 2, 1, tokens), f32),
            pltpu.VMEM((2, tokens, 128), f32),
            dma,
            dma,
            dma,
            dma((nz,)),
            dma((2,)),
            dma((2, nz)),
            dma((2, 2, nz)),
            dma((2,)),
            dma((2, nx - 1)),
        ],
        compiler_params=pltpu.CompilerParams(
            collective_id=1, has_side_effects=True, vmem_limit_bytes=56 * 2**20
        ),
        cost_estimate=pl.CostEstimate(flops=10**9, bytes_accessed=4 * 10**6, transcendentals=0),
        name="dispatch",
    )(features, next_features, *small, *critics[1:], *targets[1:], w1, critics[0])


def critic_kernel(
    cap,
    tile,
    rows,
    notes,
    shift_ref,
    head_ref,
    w,
    h,
    hs,
    xc,
    targets,
    weights,
    zbuf,
    gbuf,
    gt,
    sq,
    s0,
    s1,
):
    f32, bf16 = jnp.float32, jnp.bfloat16
    slots, width = rows.shape[1:]
    hidden = w.shape[1]
    shards = slots // cap
    pieces = slots // 128
    few, many = 3, 6
    big = few * tile
    wide = min(256, hidden)
    lanes = hidden // 128
    shift = shift_ref[...]
    head = head_ref[...]

    kept, part = cap // 2, slots // 2
    at_slot = iota((1, slots), 1)
    owner = ones_where(lax.rem(at_slot, part) // kept == iota((shards, slots), 0))
    my_slot = at_slot // part * kept + lax.rem(at_slot, kept) == iota((cap, slots), 0)
    upto = ones_where(iota((128, 128), 0) <= iota((128, 128), 1))
    counts = []
    for s in range(2):
        by_slot = notes[s, :, 0, :].T[0 : 2 * cap].astype(bf16)
        spread = dot_nn(by_slot, owner)
        y_row = jnp.sum(jnp.where(my_slot, spread[0:cap], 0.0), axis=0, keepdims=True)
        w_row = jnp.sum(jnp.where(my_slot, spread[cap : 2 * cap], 0.0), axis=0, keepdims=True)
        alive = jnp.where(w_row > 0, 1.0, 0.0)
        stacked = jnp.concatenate(
            [alive[:, p * 128 : (p + 1) * 128] for p in range(pieces)]
            + [jnp.zeros((8, 128), f32)] * (1 if pieces < 8 else 0),
            axis=0,
        )
        running = dot_nn(stacked.astype(bf16), upto)
        place = []
        start = jnp.zeros((1, 1), f32)
        for p in range(pieces):
            position = running[p : p + 1] - 1.0 + start
            position = jnp.where(stacked[p : p + 1] > 0, position, -1.0)
            place.append(position.astype(jnp.int32))
            start = start + running[p : p + 1, 127:128]
        number = jnp.sum(alive)
        counts.append(number)
        yw = jnp.concatenate(
            [jnp.broadcast_to(y_row, (128, slots)), jnp.broadcast_to(w_row, (128, slots))], axis=0
        ).astype(bf16)
        trips = jnp.where(number <= few * tile, few, many)

        def compact(i, _, s=s, place=place, yw=yw):
            at = pl.ds(pl.multiple_of(i * big, big), big)
            row = iota((big, 128), 0) + i * big
            pick = jnp.concatenate([ones_where(row == p) for p in place], axis=1)
            xc[s, at, :] = dot_nn(pick, rows[s]).astype(bf16)
            both = dot_nt(pick, yw)
            targets[s, at, :] = both[:, 0:128]
            weights[s, at, :] = both[:, 128:256]
            return 0

        lax.fori_loop(0, trips // few, compact, 0)

    total0 = jnp.zeros((1, hidden), f32)
    total1 = jnp.zeros((1, hidden), f32)
    groups = tile // 8
    for s in range(2):
        number = counts[s]
        whole = jnp.full((1, 1), number, f32)
        trips = jnp.where(number <= few * tile, few, many)
        middle = jnp.sum(rows[s].astype(f32), axis=0, keepdims=True) / whole
        one = middle.astype(bf16)
        rest = middle - one.astype(f32)
        two = rest.astype(bf16)
        three = (rest - two.astype(f32)).astype(bf16)
        parts = jnp.concatenate(
            [one.astype(f32), two.astype(f32), three.astype(f32), jnp.zeros((13, width), f32)], axis=0
        ).astype(bf16)
        mu = jnp.sum(dot_nn(parts, w[...]), axis=0, keepdims=True)
        sq[...] = jnp.zeros(sq.shape, f32)
        s0[...] = jnp.zeros(s0.shape, f32)
        s1[...] = jnp.zeros(s1.shape, f32)

        def forward(i, _, s=s, mu=mu, number=number):
            at = pl.ds(pl.multiple_of(i * tile, tile), tile)
            row = iota((tile, 128), 0) + i * tile
            alive = jnp.where(row < number.astype(jnp.int32), 1.0, 0.0)
            x = xc[s, at, :]
            for j in range(hidden // wide):
                pre = dot_nn(x, w[:, j * wide : (j + 1) * wide])
                for k in range(wide // 128):
                    lo = j * wide + k * 128
                    zc = (pre[:, k * 128 : (k + 1) * 128] - mu[:, lo : lo + 128]) * alive
                    zbuf[at, lo : lo + 128] = zc
                    sq[:, lo : lo + 128] += jnp.sum((zc * zc).reshape(groups, 8, 128), axis=0)
            return 0

        lax.fori_loop(0, trips, forward, 0)
        var = jnp.sum(sq[...], axis=0, keepdims=True) / whole
        inv = 1.0 / jnp.sqrt(var + EPS)

        short = tile // 2

        def slopes(i, _, s=s, inv=inv):
            at = pl.ds(pl.multiple_of(i * short, short), short)
            acc = jnp.zeros((short, 128), f32)
            for j in range(lanes):
                cut = slice(j * 128, (j + 1) * 128)
                zh = zbuf[at, cut] * inv[:, cut]
                zbuf[at, cut] = zh
                acc = acc + jnp.maximum(zh + shift[:, cut], 0.0) * head[:, cut]
            q = jnp.sum(acc, axis=1, keepdims=True)
            dq = weights[s, at, :] * (q - targets[s, at, :])
            for j in range(lanes):
                cut = slice(j * 128, (j + 1) * 128)
                zh = zbuf[at, cut]
                g = jnp.where(zh > -shift[:, cut], dq, 0.0)
                gbuf[at, cut] = g
                s0[:, cut] += jnp.sum(g.reshape(short // 8, 8, 128), axis=0)
                s1[:, cut] += jnp.sum((g * zh).reshape(short // 8, 8, 128), axis=0)
            return 0

        lax.fori_loop(0, trips * (tile // short), slopes, 0)
        sum0 = jnp.sum(s0[...], axis=0, keepdims=True)
        sum1 = jnp.sum(s1[...], axis=0, keepdims=True)
        total0 = total0 + sum0
        total1 = total1 + sum1
        scale = inv * head
        base = -scale * (sum0 / whole)
        tilt = -scale * (sum1 / whole)

        def slope_of(at, cut, scale=scale, base=base, tilt=tilt):
            value = gbuf[at, cut] * scale[:, cut] + (zbuf[at, cut] * tilt[:, cut] + base[:, cut])
            return value.astype(bf16)

        @pl.when(trips == few)
        def _(s=s, slope_of=slope_of):
            xt = xc[s, 0:big, :].T
            for j in range(hidden // wide):
                cut = slice(j * wide, (j + 1) * wide)
                out = dot_nn(xt, slope_of(slice(0, big), cut))
                gt[:, cut] = out if s == 0 else gt[:, cut] + out

        @pl.when(trips != few)
        def _(s=s, slope_of=slope_of):
            if s == 0:
                gt[...] = jnp.zeros(gt.shape, f32)

            def step(i, _):
                at = pl.ds(pl.multiple_of(i * tile, tile), tile)
                for j in range(hidden // wide):
                    cut = slice(j * wide, (j + 1) * wide)
                    gt[:, cut] += dot_tn(xc[s, at, :], slope_of(at, cut))
                return 0

            lax.fori_loop(0, many, step, 0)

    g_shift = head * total0
    g_head = shift * total0 + total1
    for u in range(lanes):
        cut = slice(u * 128, (u + 1) * 128)
        h[2 * u] = gt[0:128, cut].astype(bf16)
        h[2 * u + 1] = gt[128:256, cut].astype(bf16)
        hs[2 * u] = g_shift[:, cut]
        hs[2 * u + 1] = g_head[:, cut]


def critic_sums(rows, notes, shift, head, w1, cap):
    f32, bf16 = jnp.float32, jnp.bfloat16
    slots, width = rows.shape[1:]
    hidden = w1.shape[1]
    tile = slots * 3 // 16
    tall = 6 * tile
    vmem = pl.BlockSpec(memory_space=pltpu.VMEM)
    blocks = hidden // 128 * (width // 128)
    return pl.pallas_call(
        functools.partial(critic_kernel, cap, tile),
        out_shape=(
            pltpu.VMEM((blocks, 128, 128), bf16),
            pltpu.VMEM((blocks, 1, 128), f32),
        ),
        in_specs=[vmem] * 5,
        out_specs=[vmem] * 2,
        scratch_shapes=[
            pltpu.VMEM((2, tall, width), bf16),
            pltpu.VMEM((2, tall, 128), f32),
            pltpu.VMEM((2, tall, 128), f32),
            pltpu.VMEM((tall, hidden), f32),
            pltpu.VMEM((tall, hidden), f32),
            pltpu.VMEM((width, hidden), f32),
            pltpu.VMEM((8, hidden), f32),
            pltpu.VMEM((8, hidden), f32),
            pltpu.VMEM((8, hidden), f32),
        ],
        compiler_params=pltpu.CompilerParams(vmem_limit_bytes=48 * 2**20),
        cost_estimate=pl.CostEstimate(
            flops=8 * slots * hidden * width, bytes_accessed=4 * 10**6, transcendentals=0
        ),
        name="critic_sums",
    )(rows, notes, shift, head, w1)


def per_device(
    features,
    next_features,
    rewards,
    next_logp,
    terminal,
    source_ids,
    source_weight,
    subset,
    destination,
    critic_w1,
    critic_shift,
    critic_head,
    target_w1,
    target_mean,
    target_scale,
    target_shift,
    target_head,
):
    f32 = jnp.float32
    shards = lax.axis_size("dp")
    nx = lax.axis_size("member")
    nz = NZ
    ny = shards // (2 * nz)
    tokens, width = features.shape
    critics, hidden = critic_w1.shape[:2]
    cap = 2 * tokens // shards
    rows, notes, shift, head, w1 = dispatch(
        features,
        next_features,
        (
            destination.reshape(1, tokens),
            terminal.reshape(1, tokens),
            source_ids.reshape(1, tokens),
            subset.T,
            rewards.reshape(tokens // 128, 128),
            next_logp.reshape(tokens // 128, 128),
            source_weight.reshape(1, -1),
        ),
        (target_w1, target_mean, target_scale, target_shift, target_head),
        (critic_w1, critic_shift, critic_head),
        ny,
        nz,
        nx,
    )
    h, hs = critic_sums(rows.reshape(2, shards * cap, width), notes, shift, head, w1, cap)
    h = h.reshape(ny, nz, 128, 128)
    hs = hs.reshape(ny, nz, 1, 128)
    full, shift, head, factor = reduce_all(h, hs, ny, nz, nx)
    factor = factor[0, 0]
    step_w1 = full.reshape(critics, hidden, width).astype(f32) * factor
    return (step_w1, shift * factor, head * factor)


def solution(mesh):
    in_specs = (
        P("dp", None),
        P("dp", None),
        P("dp"),
        P("dp"),
        P("dp"),
        P("dp"),
        P(),
        P("dp", None),
        P("dp"),
        P("member", None, None),
        P("member", None),
        P("member", None),
        P("member", None, None),
        P("member", None),
        P("member", None),
        P("member", None),
        P("member", None),
    )
    out_specs = (P("member", None, None), P("member", None), P("member", None))
    return jax.shard_map(
        per_device, mesh=mesh, in_specs=in_specs, out_specs=out_specs, check_vma=False
    )
```
